256 devices in a mesh: row: 32 (over y, z), col: 8 (over x, core).
Axes of the slice: x: 4, y: 4, z: 8, core: 2. Of those that a mesh axis runs over, the one named last changes fastest.
Arguments:
- points: float32 [16, 32768], P(None, ('col', 'row')), may hold values from -5 to 5
- inv_scales: float32 [16], replicated, may hold values from 0.1 to 0.4
- amplitude: float32 [1], replicated, may hold values from 0.5 to 2
- noise_var: float32 [1], replicated, may hold values from 0.3 to 1
- targets: float32 [8, 32768], P(None, ('col', 'row')), may hold values from -6 to 6
- initial: float32 [8, 32768], P(None, ('col', 'row')), may hold values from -3 to 3
- ritz_basis: float32 [64, 32768], P(None, ('col', 'row')), may hold values from -0.03125 to 0.03125
Outputs:
- solution: float32 [8, 32768], P(None, ('col', 'row'))
- residual: float32 [8, 32768], P(None, ('col', 'row'))
The draws below stay inside these ranges and needn't reach their ends.
All inputs are finite; a program needn't handle non-finite values.
Results may differ from the reference program's by a relative error of at most 0.00065.
Values sent between devices are 32-bit elements; how exact they have to be, the bound alone decides.
No kernel may reach another device: no remote copies, remote signals or barrier semaphores. Data moves between devices by JAX's collectives and lax.ppermute only.
A program may use at most 128 MiB of HBM per device.

```python
import math
import jax
import jax.numpy as jnp
from jax import lax

FEAT = 16
RITZ = 64
ITERS = 1
RHS = 8
POINTS = 32768


def level_of(key, dims, cuts, low, largest):
    level = 1.0
    for axis_at, parts in cuts:
        draws = jax.random.uniform(jax.random.fold_in(jax.random.fold_in(key, 6), axis_at), (parts,), jnp.float32, low / len(cuts), largest / len(cuts))
        level = level * jnp.repeat(jnp.exp(draws), dims[axis_at] // parts).reshape((-1,) + (1,) * (len(dims) - 1 - axis_at))
    return level


def normal_values(key, extent, deviation, reach, split=(), kind=jnp.bfloat16):
    level = level_of(key, extent, split, -0.22, 0.18) if split else 1.0
    drawn = jax.random.normal(key, extent, jnp.float32) * deviation * level
    return jnp.minimum(jnp.maximum(drawn, -reach), reach).astype(kind)


def setup_inputs(seed: int = 0) -> dict:
    key_list = jax.random.split(jax.random.key(seed), 8)
    points = normal_values(key_list[0], (FEAT, POINTS), 1.0, 5.0, ((1, 256),), jnp.float32)
    inv_scales = jnp.clip(jnp.exp(jax.random.uniform(key_list[1], (FEAT,), jnp.float32, math.log(0.1), math.log(0.4))), 0.1, 0.4)
    amplitude = jnp.clip(jnp.exp(jax.random.uniform(key_list[2], (1,), jnp.float32, math.log(0.5), math.log(2.0))), 0.5, 2.0)
    noise_var = jnp.clip(jnp.exp(jax.random.uniform(key_list[3], (1,), jnp.float32, math.log(0.3), math.log(1.0))), 0.3, 1.0)
    targets = normal_values(key_list[4], (RHS, POINTS), 1.0, 6.0, ((1, 256),), jnp.float32)
    initial = normal_values(key_list[5], (RHS, POINTS), 0.5, 3.0, ((1, 256),), jnp.float32)
    ritz_basis = normal_values(key_list[6], (RITZ, POINTS), POINTS ** -0.5, 0.03125, ((1, 256),), jnp.float32)
    return dict(points=points, inv_scales=inv_scales, amplitude=amplitude, noise_var=noise_var, targets=targets, initial=initial, ritz_basis=ritz_basis)


HIGH = lax.Precision.HIGHEST

def kernel_tile(col_x, col_sq, row_x, row_sq, gain):
    cross_term = jnp.dot(col_x.T.astype(jnp.float32), row_x.astype(jnp.float32), precision=HIGH, preferred_element_type=jnp.float32)
    distance = jnp.maximum(col_sq[:, None] + row_sq[None, :] - 2.0 * cross_term, 0.0)
    return gain * jnp.exp(-0.5 * distance)

def coarse_solve(factor, rhs_block):
    middle = lax.linalg.triangular_solve(factor, rhs_block, left_side=True, lower=True)
    return lax.linalg.triangular_solve(factor, middle, left_side=True, lower=True, transpose_a=True)

def matmul(left, right):
    return jnp.dot(left.astype(jnp.float32), right.astype(jnp.float32), precision=HIGH, preferred_element_type=jnp.float32)

def apply_operator(vectors, scaled, sq_norms, gain, nugget):
    length = scaled.shape[1]
    block_size = math.gcd(length, 2048)
    num_blocks = length // block_size

    def one_block(block_index):
        offset = (block_index * block_size).astype(jnp.int32)
        row_x = lax.dynamic_slice_in_dim(scaled, offset, block_size, 1)
        row_sq = lax.dynamic_slice_in_dim(sq_norms, offset, block_size, 0)
        kernel_block = kernel_tile(scaled, sq_norms, row_x, row_sq, gain)
        return jnp.dot(vectors.astype(jnp.float32), kernel_block.astype(jnp.float32), precision=HIGH, preferred_element_type=jnp.float32)
    results = lax.map(one_block, jnp.arange(num_blocks, dtype=jnp.int32))
    results = jnp.transpose(results, (1, 0, 2)).reshape(vectors.shape[0], length)
    return results + nugget * vectors

def reference(points, inv_scales, amplitude, noise_var, targets, initial, ritz_basis):
    gain = amplitude[0]
    nugget = noise_var[0]
    scaled = points * inv_scales[:, None]
    sq_norms = jnp.sum(scaled * scaled, axis=0)
    rhs_count = initial.shape[0]
    applied_all = apply_operator(jnp.concatenate([initial, ritz_basis], 0), scaled, sq_norms, gain, nugget)
    ritz_image = applied_all[rhs_count:]
    first_residual = targets - applied_all[:rhs_count]
    coarse = matmul(ritz_basis, ritz_image.T)
    coarse = 0.5 * (coarse + coarse.T)
    projected = matmul(ritz_basis, first_residual.T)
    factor = jnp.linalg.cholesky(coarse)
    coarse_inverse = coarse_solve(factor, jnp.eye(coarse.shape[0], dtype=coarse.dtype))
    amounts = matmul(coarse_inverse, projected)
    solution = initial + matmul(amounts.T, ritz_basis)
    residual = first_residual - matmul(amounts.T, ritz_image)
    against = matmul(ritz_image, residual.T)
    sq_norm = jnp.sum(residual * residual, axis=1)
    direction = residual - matmul(matmul(coarse_inverse, against).T, ritz_basis)
    for step in range(ITERS):
        applied = apply_operator(direction, scaled, sq_norms, gain, nugget)
        step_size = sq_norm / jnp.sum(direction * applied, axis=1)
        solution = solution + step_size[:, None] * direction
        residual = residual - step_size[:, None] * applied
        against = matmul(ritz_image, residual.T)
        new_norm = jnp.sum(residual * residual, axis=1)
        correction = matmul(matmul(coarse_inverse, against).T, ritz_basis)
        direction = residual + (new_norm / sq_norm)[:, None] * direction - correction
        sq_norm = new_norm
    return (solution, residual)
```

```python
import math

import jax
import jax.numpy as jnp
from jax import lax
from jax.experimental import pallas as pl
from jax.experimental.pallas import tpu as pltpu
from jax.sharding import Mesh
from jax.sharding import PartitionSpec as P

CORE = "col_1"
Z = "row_1"
XY = ("col_0", "row_0")
CZ = ("col_1", "row_1")
EVERY = ("col_0", "col_1", "row_0", "row_1")
COL_ROW = EVERY

FEAT = 16
RITZ = 64
RHS = 8
VEC = RHS + RITZ
BLK = 128
NB = 16
PTS = NB * BLK
STEP = 256
CHUNK = 512

HIGH = lax.Precision.HIGHEST
F32 = jnp.float32
BF16 = jnp.bfloat16
NT = (((1,), (1,)), ((), ()))


def split2(x):
    hi = x.astype(BF16)
    return hi, (x - hi.astype(F32)).astype(BF16)


def split3(x):
    hi = x.astype(BF16).astype(F32)
    rest = x - hi
    mid = rest.astype(BF16).astype(F32)
    return hi, mid, rest - mid


def features(x, swap):
    a, b, c = split3(x)
    n1, n2, n3 = split3(-0.5 * jnp.sum(x * x, axis=0, keepdims=True))
    row = lax.broadcasted_iota(jnp.int32, x.shape, 0)
    base = 3 if swap else 0
    norm = jnp.where(row == base, n1, jnp.where(row == base + 1, n2, jnp.where(row == base + 2, n3, 0.0)))
    one = 0 if swap else 3
    norm = jnp.where((row >= one) & (row < one + 3), 1.0, norm)
    zero = jnp.zeros_like(x)
    if swap:
        parts = [a, b, a, b, c, a, norm, zero]
    else:
        parts = [a, a, b, b, a, c, norm, zero]
    return jnp.concatenate(parts, axis=0)


def tile_kernel(near_ref, far_ref, out_ref, scale_ref, hi_ref, lo_ref, part_ref, cols_ref, rows_ref, vec_ref):
    step = pl.program_id(0)

    @pl.when(step == 0)
    def _():
        scale = scale_ref[...] * math.sqrt(math.log2(math.e))
        vec_ref[...] = jnp.zeros_like(vec_ref)
        for b in range(NB):
            src = near_ref if b < NB // 2 else far_ref
            at = b % (NB // 2)
            lanes = pl.ds(b * BLK, BLK)
            cols_ref[:, lanes] = features(src[at, :FEAT, :] * scale, False).astype(BF16)
            hi, lo = split2(src[at, FEAT:, :])
            vec_ref[pl.ds(0, VEC), lanes] = hi
            vec_ref[pl.ds(BLK, VEC), lanes] = lo
            rows_ref[lanes, :] = features(out_ref[b, :FEAT, :] * scale, True).T.astype(BF16)

    mine = rows_ref[pl.ds(pl.multiple_of(step * STEP, STEP), STEP), :]
    total = jnp.zeros((STEP, 2 * BLK), F32)
    for c in range(PTS // CHUNK):
        lanes = pl.ds(c * CHUNK, CHUNK)
        power = jnp.dot(mine, cols_ref[:, lanes], preferred_element_type=F32)
        value = jnp.exp2(jnp.minimum(power, 0.0))
        hi, lo = split2(value)
        hi_ref[:, lanes] = hi
        lo_ref[:, lanes] = lo
        vec = vec_ref[:, lanes]
        total += lax.dot_general(hi, vec, NT, preferred_element_type=F32)
        total += lax.dot_general(lo, vec, NT, preferred_element_type=F32)
    both = total[:, :BLK] + total[:, BLK:]
    for h in range(STEP // BLK):
        part_ref[h] = both[h * BLK : (h + 1) * BLK].T[:VEC]


def make_tile(near, far, out, scales):
    full = lambda shape: pl.BlockSpec(shape, lambda i: (0,) * len(shape))
    return pl.pallas_call(
        tile_kernel,
        grid=(PTS // STEP,),
        in_specs=[full(near.shape), full(far.shape), full(out.shape), full(scales.shape)],
        out_specs=[
            pl.BlockSpec((STEP, PTS), lambda i: (i, 0)),
            pl.BlockSpec((STEP, PTS), lambda i: (i, 0)),
            pl.BlockSpec((STEP // BLK, VEC, BLK), lambda i: (i, 0, 0)),
        ],
        out_shape=[
            jax.ShapeDtypeStruct((PTS, PTS), BF16),
            jax.ShapeDtypeStruct((PTS, PTS), BF16),
            jax.ShapeDtypeStruct((NB, VEC, BLK), F32),
        ],
        scratch_shapes=[
            pltpu.VMEM((BLK, PTS), BF16),
            pltpu.VMEM((PTS, BLK), BF16),
            pltpu.VMEM((2 * BLK, PTS), BF16),
        ],
        name="kernel_tile",
    )(near, far, out, scales)


def gram_kernel(vec_ref, pts_ref, out_ref, left_ref, right_ref):
    for b in range(NB):
        lanes = pl.ds(b * BLK, BLK)
        left_ref[:, lanes] = vec_ref[b]
        right_ref[pl.ds(0, RITZ), lanes] = pts_ref[b, FEAT:, :]
        right_ref[pl.ds(RITZ, RITZ), lanes] = vec_ref[b, RHS:, :]
    out_ref[...] = lax.dot_general(left_ref[...], right_ref[...], NT, precision=HIGH, preferred_element_type=F32)


def make_gram(vec, pts):
    return pl.pallas_call(
        gram_kernel,
        out_shape=jax.ShapeDtypeStruct((VEC, 2 * RITZ), F32),
        scratch_shapes=[pltpu.VMEM((VEC, PTS), F32), pltpu.VMEM((2 * RITZ, PTS), F32)],
        name="gram",
    )(vec, pts)


def apply_kernel(hi_ref, lo_ref, vec_ref, pts_ref, coef_ref, part_ref, sum_ref):
    step = pl.program_id(0)

    @pl.when(step == 0)
    def _():
        sum_ref[...] = jnp.zeros_like(sum_ref)

    for h in range(STEP // BLK):
        basis = jnp.concatenate([pts_ref[h, FEAT:, :], vec_ref[h, RHS:, :]], axis=0)
        direction = vec_ref[h, :RHS, :] - jnp.dot(
            coef_ref[...], basis, precision=HIGH, preferred_element_type=F32
        )
        hi = direction.astype(BF16).astype(F32)
        both = jnp.concatenate([hi, direction - hi], axis=0).astype(BF16)
        rows = pl.ds(h * BLK, BLK)
        sum_ref[...] += jnp.dot(both, hi_ref[rows, :], preferred_element_type=F32)
        sum_ref[...] += jnp.dot(both, lo_ref[rows, :], preferred_element_type=F32)

    @pl.when(step == pl.num_programs(0) - 1)
    def _():
        for b in range(NB):
            lanes = pl.ds(b * BLK, BLK)
            part_ref[b] = sum_ref[pl.ds(0, RHS), lanes] + sum_ref[pl.ds(RHS, RHS), lanes]


def apply_tile(hi, lo, vec, pts, coef):
    return pl.pallas_call(
        apply_kernel,
        grid=(PTS // STEP,),
        in_specs=[
            pl.BlockSpec((STEP, PTS), lambda i: (i, 0)),
            pl.BlockSpec((STEP, PTS), lambda i: (i, 0)),
            pl.BlockSpec((STEP // BLK, VEC, BLK), lambda i: (i, 0, 0)),
            pl.BlockSpec((STEP // BLK, FEAT + RITZ, BLK), lambda i: (i, 0, 0)),
            pl.BlockSpec(coef.shape, lambda i: (0, 0)),
        ],
        out_specs=pl.BlockSpec((NB, RHS, BLK), lambda i: (0, 0, 0)),
        out_shape=jax.ShapeDtypeStruct((NB, RHS, BLK), F32),
        scratch_shapes=[pltpu.VMEM((2 * RHS, PTS), F32)],
        name="apply_tile",
    )(hi, lo, vec, pts, coef)


def exchange(pieces, axis):
    return lax.all_to_all(pieces, axis, split_axis=0, concat_axis=0, tiled=True)


def from_everyone(array, axis):
    return exchange(jnp.broadcast_to(array, (lax.axis_size(axis), *array.shape)), axis)


def other_core(array):
    return lax.ppermute(array, CORE, [(0, 1), (1, 0)])


def matmul(left, right):
    return jnp.dot(left, right, precision=HIGH, preferred_element_type=F32)


def coarse_solve(factor, rhs_block):
    middle = lax.linalg.triangular_solve(factor, rhs_block, left_side=True, lower=True)
    return lax.linalg.triangular_solve(factor, middle, left_side=True, lower=True, transpose_a=True)


def local(points, inv_scales, amplitude, noise_var, targets, initial, ritz_basis):
    gain = amplitude[0]
    nugget = noise_var[0]
    pts = from_everyone(jnp.concatenate([points, ritz_basis], 0), XY)
    vectors = jnp.concatenate([initial, ritz_basis], 0)
    near = from_everyone(jnp.concatenate([points, vectors], 0), Z)
    far = other_core(near)
    hi, lo, part = make_tile(near, far, pts, inv_scales[:, None])

    applied = gain * exchange(part, XY).sum(axis=0) + nugget * vectors
    own = jnp.concatenate([targets - applied[:RHS], applied[RHS:]], 0)
    vec = from_everyone(own, XY)

    gram = make_gram(vec, pts)
    gram = gram + other_core(gram)
    gram = from_everyone(gram, Z).sum(axis=0)
    projected = gram[:RHS, :RITZ].T
    image_first = gram[:RHS, RITZ:].T
    coarse = gram[RHS:, :RITZ]
    image_image = gram[RHS:, RITZ:]
    coarse = 0.5 * (coarse + coarse.T)
    factor = jnp.linalg.cholesky(coarse)
    coarse_inverse = coarse_solve(factor, jnp.eye(RITZ, dtype=F32))
    amounts = matmul(coarse_inverse, projected)
    against = image_first - matmul(image_image, amounts)
    turned = matmul(coarse_inverse, against)
    coef = jnp.concatenate([turned.T, amounts.T], axis=1)

    part = apply_tile(hi, lo, vec, pts, coef)
    own_first = lax.axis_index(CORE) == 0
    part = jnp.where(own_first, part, jnp.concatenate([part[NB // 2 :], part[: NB // 2]], 0))

    solution = initial + matmul(amounts.T, ritz_basis)
    residual = own[:RHS] - matmul(amounts.T, own[RHS:])
    direction = residual - matmul(turned.T, ritz_basis)
    applied = gain * exchange(part, CZ).sum(axis=0) + nugget * direction
    stats = jnp.concatenate([jnp.sum(direction * applied, axis=1), jnp.sum(residual * residual, axis=1)])
    stats = from_everyone(stats[None, :], EVERY).sum(axis=(0, 1))
    size = (stats[RHS:] / stats[:RHS])[:, None]
    return (solution + size * direction, residual - size * applied)


def solution(mesh):
    torus = Mesh(mesh.devices.reshape(4, 8, 4, 2), ("row_0", "row_1", "col_0", "col_1"))
    in_specs = (
        P(None, COL_ROW),
        P(),
        P(),
        P(),
        P(None, COL_ROW),
        P(None, COL_ROW),
        P(None, COL_ROW),
    )
    out_specs = (P(None, COL_ROW), P(None, COL_ROW))
    return jax.shard_map(local, mesh=torus, in_specs=in_specs, out_specs=out_specs, check_vma=False)
```

```python
import math

import jax
import jax.numpy as jnp
from jax import lax
from jax.experimental import pallas as pl
from jax.experimental.pallas import tpu as pltpu
from jax.sharding import Mesh
from jax.sharding import PartitionSpec as P

CORE = "col_1"
Z = "row_1"
XY = ("col_0", "row_0")
CZ = ("col_1", "row_1")
EVERY = ("col_0", "col_1", "row_0", "row_1")
COL_ROW = EVERY

FEAT = 16
RITZ = 64
RHS = 8
VEC = RHS + RITZ
BLK = 128
NB = 16
PTS = NB * BLK
STEP = 256
CHUNK = 512
PACKED = RHS + RITZ // 2 + 1
WORLD = 256
TILE_MIB = 12
APPLY_MIB = 8

HIGH = lax.Precision.HIGHEST
F32 = jnp.float32
BF16 = jnp.bfloat16
NT = (((1,), (1,)), ((), ()))


def split2(x):
    hi = x.astype(BF16)
    return hi, (x - hi.astype(F32)).astype(BF16)


def split3(x):
    hi = x.astype(BF16).astype(F32)
    rest = x - hi
    mid = rest.astype(BF16).astype(F32)
    return hi, mid, rest - mid


def features(x, swap):
    a, b, c = split3(x)
    n1, n2, n3 = split3(-0.5 * jnp.sum(x * x, axis=0, keepdims=True))
    row = lax.broadcasted_iota(jnp.int32, x.shape, 0)
    base = 3 if swap else 0
    norm = jnp.where(row == base, n1, jnp.where(row == base + 1, n2, jnp.where(row == base + 2, n3, 0.0)))
    one = 0 if swap else 3
    norm = jnp.where((row >= one) & (row < one + 3), 1.0, norm)
    zero = jnp.zeros_like(x)
    if swap:
        parts = [a, b, a, b, c, a, norm, zero]
    else:
        parts = [a, a, b, b, a, c, norm, zero]
    return jnp.concatenate(parts, axis=0)


def vmem():
    return pl.BlockSpec(memory_space=pltpu.VMEM)


def smem():
    return pl.BlockSpec(memory_space=pltpu.SMEM)


def shape(*dims):
    return jax.ShapeDtypeStruct(dims, F32)


def limit(mib):
    return pltpu.CompilerParams(vmem_limit_bytes=mib << 20)


def spread_kernel(points_ref, scale_ref, initial_ref, ritz_ref, near_ref, pts_ref):
    scaled = points_ref[...] * (scale_ref[...].T * math.sqrt(math.log2(math.e)))
    for b in range(NB // 2):
        near_ref[b, pl.ds(0, FEAT), :] = scaled
        near_ref[b, pl.ds(FEAT, RHS), :] = initial_ref[...]
        near_ref[b, pl.ds(FEAT + RHS, RITZ), :] = ritz_ref[...]
    for b in range(NB):
        pts_ref[b, pl.ds(0, FEAT), :] = scaled
        pts_ref[b, pl.ds(FEAT, RITZ), :] = ritz_ref[...]


def spread(points, scales, initial, ritz):
    return pl.pallas_call(
        spread_kernel,
        out_shape=[shape(NB // 2, FEAT + VEC, BLK), shape(NB, FEAT + RITZ, BLK)],
        compiler_params=limit(8),
        name="spread",
    )(points, scales, initial, ritz)


def tile_kernel(near_ref, far_ref, out_ref, hi_ref, lo_ref, part_ref, cols_ref, rows_ref, vec_ref):
    vec_ref[...] = jnp.zeros_like(vec_ref)
    for b in range(NB):
        src = near_ref if b < NB // 2 else far_ref
        at = b % (NB // 2)
        lanes = pl.ds(b * BLK, BLK)
        cols_ref[:, lanes] = features(src[at, :FEAT, :], False).astype(BF16)
        hi, lo = split2(src[at, FEAT:, :])
        vec_ref[pl.ds(0, VEC), lanes] = hi
        vec_ref[pl.ds(BLK, VEC), lanes] = lo
        rows_ref[lanes, :] = features(out_ref[b, :FEAT, :], True).T.astype(BF16)

    def one_step(step, carry):
        rows = pl.ds(pl.multiple_of(step * STEP, STEP), STEP)
        mine = rows_ref[rows, :]
        total = jnp.zeros((STEP, 2 * BLK), F32)
        for c in range(PTS // CHUNK):
            lanes = pl.ds(c * CHUNK, CHUNK)
            power = jnp.dot(mine, cols_ref[:, lanes], preferred_element_type=F32)
            value = jnp.exp2(jnp.minimum(power, 0.0))
            hi, lo = split2(value)
            hi_ref[rows, lanes] = hi
            lo_ref[rows, lanes] = lo
            vec = vec_ref[:, lanes]
            total += lax.dot_general(hi, vec, NT, preferred_element_type=F32)
            total += lax.dot_general(lo, vec, NT, preferred_element_type=F32)
        both = total[:, :BLK] + total[:, BLK:]
        for h in range(STEP // BLK):
            part_ref[step * (STEP // BLK) + h] = both[h * BLK : (h + 1) * BLK].T[:VEC]
        return carry

    lax.fori_loop(0, PTS // STEP, one_step, 0)


def make_tile(near, far, out):
    return pl.pallas_call(
        tile_kernel,
        in_specs=[vmem(), vmem(), vmem()],
        out_specs=[vmem(), vmem(), vmem()],
        out_shape=[
            pltpu.VMEM((PTS, PTS), BF16),
            pltpu.VMEM((PTS, PTS), BF16),
            shape(NB, VEC, BLK),
        ],
        scratch_shapes=[
            pltpu.VMEM((BLK, PTS), BF16),
            pltpu.VMEM((PTS, BLK), BF16),
            pltpu.VMEM((2 * BLK, PTS), BF16),
        ],
        compiler_params=limit(TILE_MIB),
        name="kernel_tile",
    )(near, far, out)


def owner_kernel(got_ref, initial_ref, ritz_ref, targets_ref, gain_ref, nugget_ref, out_ref):
    total = got_ref[0]
    for b in range(1, NB):
        total += got_ref[b]
    first = targets_ref[...] - (gain_ref[0] * total[:RHS] + nugget_ref[0] * initial_ref[...])
    image = gain_ref[0] * total[RHS:] + nugget_ref[0] * ritz_ref[...]
    for b in range(NB):
        out_ref[b, pl.ds(0, RHS), :] = first
        out_ref[b, pl.ds(RHS, RITZ), :] = image


def at_owner(got, initial, ritz, targets, gain, nugget):
    return pl.pallas_call(
        owner_kernel,
        in_specs=[vmem(), vmem(), vmem(), vmem(), smem(), smem()],
        out_shape=shape(NB, VEC, BLK),
        compiler_params=limit(8),
        name="at_owner",
    )(got, initial, ritz, targets, gain, nugget)


def square_iota():
    return lax.broadcasted_iota(jnp.int32, (RITZ, RITZ), 0), lax.broadcasted_iota(jnp.int32, (RITZ, RITZ), 1)


def gram_kernel(vec_ref, pts_ref, out_ref, left_ref, right_ref):
    for b in range(NB):
        lanes = pl.ds(b * BLK, BLK)
        left_ref[:, lanes] = vec_ref[b]
        right_ref[pl.ds(0, RITZ), lanes] = pts_ref[b, FEAT:, :]
        right_ref[pl.ds(RITZ, RITZ), lanes] = vec_ref[b, RHS:, :]
    gram = lax.dot_general(left_ref[...], right_ref[...], NT, precision=HIGH, preferred_element_type=F32)
    coarse = gram[RHS:, :RITZ]
    coarse = 0.5 * (coarse + coarse.T)
    image = gram[RHS:, RITZ:]
    i, j = square_iota()
    packed = jnp.where(j >= i, coarse, image)
    diagonal = jnp.sum(jnp.where(i == j, image, 0.0), axis=0, keepdims=True)
    for b in range(NB // 2):
        out_ref[b, pl.ds(0, RHS), :] = gram[:RHS]
        out_ref[b, pl.ds(RHS, RITZ // 2), :] = jnp.concatenate([packed[: RITZ // 2], packed[RITZ // 2 :]], axis=1)
        out_ref[b, pl.ds(RHS + RITZ // 2, 1), :] = jnp.concatenate([diagonal, diagonal], axis=1)


def make_gram(vec, pts):
    return pl.pallas_call(
        gram_kernel,
        out_shape=shape(NB // 2, PACKED, BLK),
        scratch_shapes=[pltpu.VMEM((VEC, PTS), F32), pltpu.VMEM((2 * RITZ, PTS), F32)],
        compiler_params=limit(12),
        name="gram",
    )(vec, pts)


def inverse(matrix):
    i, j = square_iota()
    work = jnp.concatenate([matrix, jnp.where(i == j, 1.0, 0.0)], axis=1)
    row = lax.broadcasted_iota(jnp.int32, work.shape, 0)
    for k in range(0, RITZ, 2):
        col0 = jnp.broadcast_to(work[:, k : k + 1], work.shape)
        col1 = jnp.broadcast_to(work[:, k + 1 : k + 2], work.shape)
        a, b = col0[k : k + 1], col1[k : k + 1]
        c, d = col0[k + 1 : k + 2], col1[k + 1 : k + 2]
        top, low = work[k : k + 1], work[k + 1 : k + 2]
        scale = 1.0 / (a * d - b * c)
        new_top = (d * top - b * low) * scale
        new_low = (a * low - c * top) * scale
        work = work - (col0 * new_top + col1 * new_low)
        work = jnp.where(row == k, new_top, jnp.where(row == k + 1, new_low, work))
    return work[:, RITZ:]


def apply_kernel(
    gram_ref, more_ref, hi_ref, lo_ref, vec_ref, pts_ref, initial_ref, place_ref, part_ref, own_ref, both_ref
):
    gram = gram_ref[...] + more_ref[...]
    projected = gram[:RHS, :RITZ]
    first = gram[:RHS, RITZ:]
    square = jnp.concatenate([gram[RHS : RHS + RITZ // 2, :RITZ], gram[RHS : RHS + RITZ // 2, RITZ:]], axis=0)
    turned = square.T
    i, j = square_iota()
    coarse = jnp.where(j >= i, square, turned)
    image = jnp.where(j < i, square, jnp.where(j > i, turned, gram[RHS + RITZ // 2 :, :RITZ]))
    solve = inverse(coarse)
    amounts = lax.dot_general(projected, solve, NT, precision=HIGH, preferred_element_type=F32)
    against = first - jnp.dot(amounts, image, precision=HIGH, preferred_element_type=F32)
    turns = lax.dot_general(against, solve, NT, precision=HIGH, preferred_element_type=F32)
    zero = jnp.zeros_like(turns)
    coef = jnp.concatenate([turns, amounts], axis=1)
    for b in range(NB):
        basis = jnp.concatenate([pts_ref[b, FEAT:, :], vec_ref[b, RHS:, :]], axis=0)
        direction = vec_ref[b, :RHS, :] - jnp.dot(coef, basis, precision=HIGH, preferred_element_type=F32)
        hi = direction.astype(BF16).astype(F32)
        both_ref[:, pl.ds(b * BLK, BLK)] = jnp.concatenate([hi, direction - hi], axis=0).astype(BF16)
    both = both_ref[...]
    for c in range(PTS // CHUNK):
        lanes = pl.ds(c * CHUNK, CHUNK)
        total = jnp.dot(both, hi_ref[:, lanes], preferred_element_type=F32)
        total += jnp.dot(both, lo_ref[:, lanes], preferred_element_type=F32)
        value = total[:RHS] + total[RHS:]
        for h in range(CHUNK // BLK):
            at = c * (CHUNK // BLK) + h
            half = (at // (NB // 2) + place_ref[1]) % 2
            part_ref[half * (NB // 2) + at % (NB // 2)] = value[:, h * BLK : (h + 1) * BLK]
    mine = place_ref[0]
    basis = jnp.concatenate([pts_ref[mine, FEAT:, :], vec_ref[mine, RHS:, :]], axis=0)
    wanted = jnp.concatenate(
        [coef, jnp.concatenate([zero, amounts], axis=1), jnp.concatenate([-amounts, zero], axis=1)], axis=0
    )
    base = vec_ref[mine, :RHS, :]
    base = jnp.concatenate([base, base, initial_ref[...]], axis=0)
    own_ref[...] = base - jnp.dot(wanted, basis, precision=HIGH, preferred_element_type=F32)


def apply_tile(gram, more, hi, lo, vec, pts, initial, place):
    return pl.pallas_call(
        apply_kernel,
        in_specs=[vmem()] * 7 + [smem()],
        out_shape=[shape(NB, RHS, BLK), shape(3 * RHS, BLK)],
        scratch_shapes=[pltpu.VMEM((2 * RHS, PTS), BF16)],
        compiler_params=limit(APPLY_MIB),
        name="apply_tile",
    )(gram, more, hi, lo, vec, pts, initial, place)


def stats_kernel(got_ref, own_ref, gain_ref, nugget_ref, applied_ref, out_ref):
    total = got_ref[0]
    for b in range(1, NB):
        total += got_ref[b]
    direction = own_ref[pl.ds(0, RHS), :]
    residual = own_ref[pl.ds(RHS, RHS), :]
    applied = gain_ref[0] * total + nugget_ref[0] * direction
    applied_ref[...] = applied
    sums = jnp.concatenate(
        [
            jnp.sum(direction * applied, axis=1, keepdims=True),
            jnp.sum(residual * residual, axis=1, keepdims=True),
        ],
        axis=0,
    )
    sums = jnp.broadcast_to(sums, (2 * RHS, BLK)).T[:RHS]
    for b in range(WORLD // RHS):
        out_ref[pl.ds(b * RHS, RHS), :] = sums


def make_stats(got, own, gain, nugget):
    return pl.pallas_call(
        stats_kernel,
        in_specs=[vmem(), vmem(), smem(), smem()],
        out_shape=[shape(RHS, BLK), shape(WORLD, 2 * RHS)],
        compiler_params=limit(8),
        name="stats",
    )(got, own, gain, nugget)


def finish_kernel(got_ref, own_ref, applied_ref, solution_ref, residual_ref):
    sums = jnp.sum(got_ref[...], axis=0, keepdims=True)
    i = lax.broadcasted_iota(jnp.int32, (2 * RHS, 2 * RHS), 0)
    j = lax.broadcasted_iota(jnp.int32, (2 * RHS, 2 * RHS), 1)
    sums = jnp.sum(jnp.where(i == j, sums, 0.0), axis=1, keepdims=True)
    size = sums[RHS:] / sums[:RHS]
    solution_ref[...] = own_ref[pl.ds(2 * RHS, RHS), :] + size * own_ref[pl.ds(0, RHS), :]
    residual_ref[...] = own_ref[pl.ds(RHS, RHS), :] - size * applied_ref[...]


def finish(got, own, applied):
    return pl.pallas_call(
        finish_kernel,
        out_shape=[shape(RHS, BLK), shape(RHS, BLK)],
        compiler_params=limit(8),
        name="finish",
    )(got, own, applied)


def exchange(pieces, axis):
    return lax.all_to_all(pieces, axis, split_axis=0, concat_axis=0, tiled=True)


def other_core(array):
    return lax.ppermute(array, CORE, [(0, 1), (1, 0)])


def local(points, inv_scales, amplitude, noise_var, targets, initial, ritz_basis):
    near, pts = spread(points, inv_scales[None, :], initial, ritz_basis)
    near = exchange(near, Z)
    near, pts = lax.optimization_barrier((near, pts))
    far = other_core(near)
    pts = exchange(pts, XY)
    hi, lo, part = make_tile(near, far, pts)

    vec = exchange(at_owner(exchange(part, XY), initial, ritz_basis, targets, amplitude, noise_var), XY)
    gram = jnp.sum(exchange(make_gram(vec, pts), Z), axis=0)
    place = jnp.stack([lax.axis_index(XY), lax.axis_index(CORE)]).astype(jnp.int32)
    part, own = apply_tile(gram, other_core(gram), hi, lo, vec, pts, initial, place)
    applied, stats = make_stats(exchange(part, CZ), own, amplitude, noise_var)
    return tuple(finish(exchange(stats, EVERY), own, applied))


def solution(mesh):
    torus = Mesh(mesh.devices.reshape(4, 8, 4, 2), ("row_0", "row_1", "col_0", "col_1"))
    in_specs = (
        P(None, COL_ROW),
        P(),
        P(),
        P(),
        P(None, COL_ROW),
        P(None, COL_ROW),
        P(None, COL_ROW),
    )
    out_specs = (P(None, COL_ROW), P(None, COL_ROW))
    return jax.shard_map(local, mesh=torus, in_specs=in_specs, out_specs=out_specs, check_vma=False)
```

```python
import math

import jax
import jax.numpy as jnp
from jax import lax
from jax.experimental import pallas as pl
from jax.experimental.pallas import tpu as pltpu
from jax.sharding import Mesh
from jax.sharding import PartitionSpec as P

CORE = "col_1"
Z = "row_1"
XY = ("col_0", "row_0")
CZ = ("col_1", "row_1")
EVERY = ("col_0", "col_1", "row_0", "row_1")
COL_ROW = EVERY

FEAT = 16
RITZ = 64
RHS = 8
VEC = RHS + RITZ
BLK = 128
NB = 16
PTS = NB * BLK
STEP = 512
CHUNK = 256
PACKED = RHS + RITZ // 2 + 1
WORLD = 256

HIGH = lax.Precision.HIGHEST
F32 = jnp.float32
BF16 = jnp.bfloat16
NT = (((1,), (1,)), ((), ()))


def split2(x):
    hi = x.astype(BF16)
    return hi, (x - hi.astype(F32)).astype(BF16)


def split3(x):
    hi = x.astype(BF16).astype(F32)
    rest = x - hi
    mid = rest.astype(BF16).astype(F32)
    return hi, mid, rest - mid


def features(x, swap):
    a, b, c = split3(x)
    n1, n2, n3 = split3(-0.5 * jnp.sum(x * x, axis=0, keepdims=True))
    row = lax.broadcasted_iota(jnp.int32, x.shape, 0)
    base = 3 if swap else 0
    norm = jnp.where(row == base, n1, jnp.where(row == base + 1, n2, jnp.where(row == base + 2, n3, 0.0)))
    one = 0 if swap else 3
    norm = jnp.where((row >= one) & (row < one + 3), 1.0, norm)
    zero = jnp.zeros_like(x)
    if swap:
        parts = [a, b, a, b, c, a, norm, zero]
    else:
        parts = [a, a, b, b, a, c, norm, zero]
    return jnp.concatenate(parts, axis=0)


def vmem():
    return pl.BlockSpec(memory_space=pltpu.VMEM)


def in_hbm(array):
    return pltpu.with_memory_space_constraint(array, pltpu.HBM)


def smem():
    return pl.BlockSpec(memory_space=pltpu.SMEM)


def shape(*dims):
    return jax.ShapeDtypeStruct(dims, F32)


def limit(mib):
    return pltpu.CompilerParams(vmem_limit_bytes=mib << 20)


def hbm():
    return pl.BlockSpec(memory_space=pltpu.HBM)


def spread_kernel(
    points_hbm, scale_hbm, initial_hbm, ritz_hbm, targets_hbm, near_ref, pts_ref, held_ref, points_ref, scale_ref, sem
):
    copies = [
        pltpu.make_async_copy(points_hbm, points_ref, sem.at[0]),
        pltpu.make_async_copy(scale_hbm, scale_ref, sem.at[1]),
        pltpu.make_async_copy(targets_hbm, held_ref.at[pl.ds(0, RHS)], sem.at[2]),
        pltpu.make_async_copy(initial_hbm, held_ref.at[pl.ds(RHS, RHS)], sem.at[3]),
        pltpu.make_async_copy(ritz_hbm, held_ref.at[pl.ds(2 * RHS, RITZ)], sem.at[4]),
    ]
    for copy in copies:
        copy.start()
    for copy in copies:
        copy.wait()
    scaled = points_ref[...] * (scale_ref[...].T * math.sqrt(math.log2(math.e)))
    for b in range(NB // 2):
        near_ref[b, pl.ds(0, FEAT), :] = scaled
        near_ref[b, pl.ds(FEAT, VEC), :] = held_ref[pl.ds(RHS, VEC), :]
    for b in range(NB):
        pts_ref[b, pl.ds(0, FEAT), :] = scaled
        pts_ref[b, pl.ds(FEAT, RITZ), :] = held_ref[pl.ds(2 * RHS, RITZ), :]


def spread(points, scales, initial, ritz, targets):
    return pl.pallas_call(
        spread_kernel,
        in_specs=[hbm()] * 5,
        out_specs=[vmem()] * 3,
        out_shape=[shape(NB // 2, FEAT + VEC, BLK), shape(NB, FEAT + RITZ, BLK), shape(RHS + VEC, BLK)],
        scratch_shapes=[
            pltpu.VMEM((FEAT, BLK), F32),
            pltpu.VMEM((1, FEAT), F32),
            pltpu.SemaphoreType.DMA((5,)),
        ],
        compiler_params=limit(8),
        name="spread",
    )(*map(in_hbm, (points, scales, initial, ritz, targets)))


def tile_kernel(
    near_ref, far_ref, out_ref, hi_hbm, lo_hbm, part_ref, hi_ref, lo_ref, cols_ref, rows_ref, vec_ref, sem
):
    for b in range(NB):
        src = near_ref if b < NB // 2 else far_ref
        at = b % (NB // 2)
        lanes = pl.ds(b * BLK, BLK)
        cols_ref[:, lanes] = features(src[at, :FEAT, :], False).astype(BF16)
        tall = jnp.concatenate([src[at, FEAT:, :], jnp.zeros((BLK - VEC, BLK), F32)], axis=0).T
        hi, lo = split2(tall)
        vec_ref[lanes, pl.ds(0, BLK)] = hi
        vec_ref[lanes, pl.ds(BLK, BLK)] = lo
        rows_ref[lanes, :] = features(out_ref[b, :FEAT, :], True).T.astype(BF16)

    def copies(step):
        rows = pl.ds(pl.multiple_of(step * STEP, STEP), STEP)
        return (
            pltpu.make_async_copy(hi_ref.at[rows], hi_hbm.at[rows], sem.at[0, step]),
            pltpu.make_async_copy(lo_ref.at[rows], lo_hbm.at[rows], sem.at[1, step]),
        )

    def one_step(step, carry):
        rows = pl.ds(pl.multiple_of(step * STEP, STEP), STEP)
        mine = rows_ref[rows, :]
        for c in range(PTS // CHUNK):
            lanes = pl.ds(c * CHUNK, CHUNK)
            power = jnp.dot(mine, cols_ref[:, lanes], preferred_element_type=F32)
            hi, lo = split2(jnp.exp2(jnp.minimum(power, 0.0)))
            hi_ref[rows, lanes] = hi
            lo_ref[rows, lanes] = lo
        for copy in copies(step):
            copy.start()
        total = jnp.dot(hi_ref[rows, :], vec_ref[...], preferred_element_type=F32)
        total += jnp.dot(lo_ref[rows, :], vec_ref[...], preferred_element_type=F32)
        both = total[:, :BLK] + total[:, BLK:]
        for h in range(STEP // BLK):
            part_ref[step * (STEP // BLK) + h] = both[h * BLK : (h + 1) * BLK].T[:VEC]
        return carry

    lax.fori_loop(0, PTS // STEP, one_step, 0)
    for step in range(PTS // STEP):
        for copy in copies(step):
            copy.wait()


def make_tile(near, far, out):
    return pl.pallas_call(
        tile_kernel,
        in_specs=[vmem(), vmem(), vmem()],
        out_specs=[hbm(), hbm(), vmem()],
        out_shape=[
            pltpu.HBM((PTS, PTS), BF16),
            pltpu.HBM((PTS, PTS), BF16),
            shape(NB, VEC, BLK),
        ],
        scratch_shapes=[
            pltpu.VMEM((PTS, PTS), BF16),
            pltpu.VMEM((PTS, PTS), BF16),
            pltpu.VMEM((BLK, PTS), BF16),
            pltpu.VMEM((PTS, BLK), BF16),
            pltpu.VMEM((PTS, 2 * BLK), BF16),
            pltpu.SemaphoreType.DMA((2, PTS // STEP)),
        ],
        compiler_params=limit(40),
        name="kernel_tile",
    )(near, far, out)


def owner_kernel(got_ref, held_ref, gain_ref, nugget_ref, out_ref):
    total = got_ref[0]
    for b in range(1, NB):
        total += got_ref[b]
    applied = gain_ref[0] * total + nugget_ref[0] * held_ref[pl.ds(RHS, VEC), :]
    first = held_ref[pl.ds(0, RHS), :] - applied[:RHS]
    image = applied[RHS:]
    for b in range(NB):
        out_ref[b, pl.ds(0, RHS), :] = first
        out_ref[b, pl.ds(RHS, RITZ), :] = image


def at_owner(got, held, gain, nugget):
    return pl.pallas_call(
        owner_kernel,
        in_specs=[vmem(), vmem(), smem(), smem()],
        out_shape=shape(NB, VEC, BLK),
        compiler_params=limit(8),
        name="at_owner",
    )(got, held, gain, nugget)


def square_iota():
    return lax.broadcasted_iota(jnp.int32, (RITZ, RITZ), 0), lax.broadcasted_iota(jnp.int32, (RITZ, RITZ), 1)


def gram_kernel(vec_ref, pts_ref, out_ref, left_ref, right_ref):
    for b in range(NB):
        lanes = pl.ds(b * BLK, BLK)
        left_ref[:, lanes] = vec_ref[b]
        right_ref[pl.ds(0, RITZ), lanes] = pts_ref[b, FEAT:, :]
        right_ref[pl.ds(RITZ, RITZ), lanes] = vec_ref[b, RHS:, :]
    gram = lax.dot_general(left_ref[...], right_ref[...], NT, precision=HIGH, preferred_element_type=F32)
    coarse = gram[RHS:, :RITZ]
    coarse = 0.5 * (coarse + coarse.T)
    image = gram[RHS:, RITZ:]
    i, j = square_iota()
    packed = jnp.where(j >= i, coarse, image)
    diagonal = jnp.sum(jnp.where(i == j, image, 0.0), axis=0, keepdims=True)
    for b in range(NB // 2):
        out_ref[b, pl.ds(0, RHS), :] = gram[:RHS]
        out_ref[b, pl.ds(RHS, RITZ // 2), :] = jnp.concatenate([packed[: RITZ // 2], packed[RITZ // 2 :]], axis=1)
        out_ref[b, pl.ds(RHS + RITZ // 2, 1), :] = jnp.concatenate([diagonal, diagonal], axis=1)


def make_gram(vec, pts):
    return pl.pallas_call(
        gram_kernel,
        out_shape=shape(NB // 2, PACKED, BLK),
        scratch_shapes=[pltpu.VMEM((VEC, PTS), F32), pltpu.VMEM((2 * RITZ, PTS), F32)],
        compiler_params=limit(12),
        name="gram",
    )(vec, pts)


def inverse(matrix):
    i, j = square_iota()
    work = jnp.concatenate([matrix, jnp.where(i == j, 1.0, 0.0)], axis=1)
    row = lax.broadcasted_iota(jnp.int32, work.shape, 0)
    for k in range(0, RITZ, 2):
        col0 = jnp.broadcast_to(work[:, k : k + 1], work.shape)
        col1 = jnp.broadcast_to(work[:, k + 1 : k + 2], work.shape)
        a, b = col0[k : k + 1], col1[k : k + 1]
        c, d = col0[k + 1 : k + 2], col1[k + 1 : k + 2]
        top, low = work[k : k + 1], work[k + 1 : k + 2]
        scale = 1.0 / (a * d - b * c)
        new_top = (d * top - b * low) * scale
        new_low = (a * low - c * top) * scale
        work = work - (col0 * new_top + col1 * new_low)
        work = jnp.where(row == k, new_top, jnp.where(row == k + 1, new_low, work))
    return work[:, RITZ:]


def apply_kernel(
    gram_ref,
    more_ref,
    hi_hbm,
    lo_hbm,
    vec_ref,
    pts_ref,
    held_ref,
    place_ref,
    part_ref,
    own_ref,
    both_ref,
    hi_ref,
    lo_ref,
    sum_ref,
    sem,
):
    copies = []
    for step in range(PTS // STEP):
        rows = pl.ds(step * STEP, STEP)
        copies.append(
            (
                pltpu.make_async_copy(hi_hbm.at[rows], hi_ref.at[rows], sem.at[0, step]),
                pltpu.make_async_copy(lo_hbm.at[rows], lo_ref.at[rows], sem.at[1, step]),
            )
        )
        for copy in copies[-1]:
            copy.start()
    gram = gram_ref[...] + more_ref[...]
    projected = gram[:RHS, :RITZ]
    first = gram[:RHS, RITZ:]
    square = jnp.concatenate([gram[RHS : RHS + RITZ // 2, :RITZ], gram[RHS : RHS + RITZ // 2, RITZ:]], axis=0)
    turned = square.T
    i, j = square_iota()
    coarse = jnp.where(j >= i, square, turned)
    image = jnp.where(j < i, square, jnp.where(j > i, turned, gram[RHS + RITZ // 2 :, :RITZ]))
    solve = inverse(coarse)
    amounts = lax.dot_general(projected, solve, NT, precision=HIGH, preferred_element_type=F32)
    against = first - jnp.dot(amounts, image, precision=HIGH, preferred_element_type=F32)
    turns = lax.dot_general(against, solve, NT, precision=HIGH, preferred_element_type=F32)
    zero = jnp.zeros_like(turns)
    coef = jnp.concatenate([turns, amounts], axis=1)
    for b in range(NB):
        basis = jnp.concatenate([pts_ref[b, FEAT:, :], vec_ref[b, RHS:, :]], axis=0)
        direction = vec_ref[b, :RHS, :] - jnp.dot(coef, basis, precision=HIGH, preferred_element_type=F32)
        hi = direction.astype(BF16).astype(F32)
        both_ref[:, pl.ds(b * BLK, BLK)] = jnp.concatenate([hi, direction - hi], axis=0).astype(BF16)
    for step in range(PTS // STEP):
        rows = pl.ds(step * STEP, STEP)
        both = both_ref[:, rows]
        for copy in copies[step]:
            copy.wait()
        total = jnp.dot(both, hi_ref[rows, :], preferred_element_type=F32)
        total += jnp.dot(both, lo_ref[rows, :], preferred_element_type=F32)
        if step == 0:
            sum_ref[...] = total
        else:
            sum_ref[...] += total
    for at in range(NB):
        lanes = pl.ds(at * BLK, BLK)
        half = (at // (NB // 2) + place_ref[1]) % 2
        part_ref[half * (NB // 2) + at % (NB // 2)] = sum_ref[pl.ds(0, RHS), lanes] + sum_ref[pl.ds(RHS, RHS), lanes]
    mine = place_ref[0]
    basis = jnp.concatenate([pts_ref[mine, FEAT:, :], vec_ref[mine, RHS:, :]], axis=0)
    wanted = jnp.concatenate(
        [coef, jnp.concatenate([zero, amounts], axis=1), jnp.concatenate([-amounts, zero], axis=1)], axis=0
    )
    base = vec_ref[mine, :RHS, :]
    base = jnp.concatenate([base, base, held_ref[pl.ds(RHS, RHS), :]], axis=0)
    own_ref[...] = base - jnp.dot(wanted, basis, precision=HIGH, preferred_element_type=F32)


def apply_tile(gram, more, hi, lo, vec, pts, held, place):
    return pl.pallas_call(
        apply_kernel,
        in_specs=[vmem(), vmem(), hbm(), hbm(), vmem(), vmem(), vmem(), smem()],
        out_shape=[shape(NB, RHS, BLK), shape(3 * RHS, BLK)],
        scratch_shapes=[
            pltpu.VMEM((2 * RHS, PTS), BF16),
            pltpu.VMEM((PTS, PTS), BF16),
            pltpu.VMEM((PTS, PTS), BF16),
            pltpu.VMEM((2 * RHS, PTS), F32),
            pltpu.SemaphoreType.DMA((2, PTS // STEP)),
        ],
        compiler_params=limit(32),
        name="apply_tile",
    )(gram, more, in_hbm(hi), in_hbm(lo), vec, pts, held, place)


def stats_kernel(got_ref, own_ref, gain_ref, nugget_ref, applied_ref, out_ref):
    total = got_ref[0]
    for b in range(1, NB):
        total += got_ref[b]
    direction = own_ref[pl.ds(0, RHS), :]
    residual = own_ref[pl.ds(RHS, RHS), :]
    applied = gain_ref[0] * total + nugget_ref[0] * direction
    applied_ref[...] = applied
    sums = jnp.concatenate(
        [
            jnp.sum(direction * applied, axis=1, keepdims=True),
            jnp.sum(residual * residual, axis=1, keepdims=True),
        ],
        axis=0,
    )
    sums = jnp.broadcast_to(sums, (2 * RHS, BLK)).T[:RHS]
    for b in range(WORLD // RHS):
        out_ref[pl.ds(b * RHS, RHS), :] = sums


def make_stats(got, own, gain, nugget):
    return pl.pallas_call(
        stats_kernel,
        in_specs=[vmem(), vmem(), smem(), smem()],
        out_shape=[shape(RHS, BLK), shape(WORLD, 2 * RHS)],
        compiler_params=limit(8),
        name="stats",
    )(got, own, gain, nugget)


def finish_kernel(got_ref, own_ref, applied_ref, solution_ref, residual_ref):
    sums = jnp.sum(got_ref[...], axis=0, keepdims=True)
    i = lax.broadcasted_iota(jnp.int32, (2 * RHS, 2 * RHS), 0)
    j = lax.broadcasted_iota(jnp.int32, (2 * RHS, 2 * RHS), 1)
    sums = jnp.sum(jnp.where(i == j, sums, 0.0), axis=1, keepdims=True)
    size = sums[RHS:] / sums[:RHS]
    solution_ref[...] = own_ref[pl.ds(2 * RHS, RHS), :] + size * own_ref[pl.ds(0, RHS), :]
    residual_ref[...] = own_ref[pl.ds(RHS, RHS), :] - size * applied_ref[...]


def finish(got, own, applied):
    return pl.pallas_call(
        finish_kernel,
        out_shape=[shape(RHS, BLK), shape(RHS, BLK)],
        compiler_params=limit(8),
        name="finish",
    )(got, own, applied)


def exchange(pieces, axis):
    return lax.all_to_all(pieces, axis, split_axis=0, concat_axis=0, tiled=True)


def other_core(array):
    return lax.ppermute(array, CORE, [(0, 1), (1, 0)])


def local(points, inv_scales, amplitude, noise_var, targets, initial, ritz_basis):
    near, pts, held = spread(points, inv_scales[None, :], initial, ritz_basis, targets)
    near = exchange(near, Z)
    near, pts = lax.optimization_barrier((near, pts))
    far = other_core(near)
    pts = exchange(pts, XY)
    hi, lo, part = make_tile(near, far, pts)

    vec = exchange(at_owner(exchange(part, XY), held, amplitude, noise_var), XY)
    gram = jnp.sum(exchange(make_gram(vec, pts), Z), axis=0)
    place = jnp.stack([lax.axis_index(XY), lax.axis_index(CORE)]).astype(jnp.int32)
    part, own = apply_tile(gram, other_core(gram), hi, lo, vec, pts, held, place)
    applied, stats = make_stats(exchange(part, CZ), own, amplitude, noise_var)
    return tuple(finish(exchange(stats, EVERY), own, applied))


def solution(mesh):
    torus = Mesh(mesh.devices.reshape(4, 8, 4, 2), ("row_0", "row_1", "col_0", "col_1"))
    in_specs = (
        P(None, COL_ROW),
        P(),
        P(),
        P(),
        P(None, COL_ROW),
        P(None, COL_ROW),
        P(None, COL_ROW),
    )
    out_specs = (P(None, COL_ROW), P(None, COL_ROW))
    return jax.shard_map(local, mesh=torus, in_specs=in_specs, out_specs=out_specs, check_vma=False)
```

```python
import math

import jax
import jax.numpy as jnp
from jax import lax
from jax.experimental import pallas as pl
from jax.experimental.pallas import tpu as pltpu
from jax.sharding import Mesh
from jax.sharding import PartitionSpec as P

CORE = "col_1"
Z = "row_1"
XY = ("col_0", "row_0")
CZ = ("col_1", "row_1")
EVERY = ("col_0", "col_1", "row_0", "row_1")
COL_ROW = EVERY

FEAT = 16
RITZ = 64
RHS = 8
VEC = RHS + RITZ
BLK = 128
NB = 16
PTS = NB * BLK
STEP = 256
CHUNK = 256
READ = 512
HALF = 2 * RHS + 2 * RITZ
PACKED = RHS + RITZ // 2 + 1
WORLD = 256

HIGH = lax.Precision.HIGHEST
F32 = jnp.float32
BF16 = jnp.bfloat16
NT = (((1,), (1,)), ((), ()))


def split2(x):
    hi = x.astype(BF16)
    return hi, (x - hi.astype(F32)).astype(BF16)


def split3(x):
    hi = x.astype(BF16).astype(F32)
    rest = x - hi
    mid = rest.astype(BF16).astype(F32)
    return hi, mid, rest - mid


def features(x, swap):
    a, b, c = split3(x)
    n1, n2, n3 = split3(-0.5 * jnp.sum(x * x, axis=0, keepdims=True))
    row = lax.broadcasted_iota(jnp.int32, x.shape, 0)
    base = 3 if swap else 0
    norm = jnp.where(row == base, n1, jnp.where(row == base + 1, n2, jnp.where(row == base + 2, n3, 0.0)))
    one = 0 if swap else 3
    norm = jnp.where((row >= one) & (row < one + 3), 1.0, norm)
    zero = jnp.zeros_like(x)
    if swap:
        parts = [a, b, a, b, c, a, norm, zero]
    else:
        parts = [a, a, b, b, a, c, norm, zero]
    return jnp.concatenate(parts, axis=0)


def vmem():
    return pl.BlockSpec(memory_space=pltpu.VMEM)


def in_hbm(array):
    return pltpu.with_memory_space_constraint(array, pltpu.HBM)


def smem():
    return pl.BlockSpec(memory_space=pltpu.SMEM)


def shape(*dims):
    return jax.ShapeDtypeStruct(dims, F32)


def limit(mib):
    return pltpu.CompilerParams(vmem_limit_bytes=mib << 20)


def hbm():
    return pl.BlockSpec(memory_space=pltpu.HBM)


def spread_kernel(
    points_hbm, scale_hbm, initial_hbm, ritz_hbm, targets_hbm, near_ref, pts_ref, held_ref, points_ref, scale_ref, sem
):
    copies = [
        pltpu.make_async_copy(points_hbm, points_ref, sem.at[0]),
        pltpu.make_async_copy(scale_hbm, scale_ref, sem.at[1]),
        pltpu.make_async_copy(targets_hbm, held_ref.at[pl.ds(0, RHS)], sem.at[2]),
        pltpu.make_async_copy(initial_hbm, held_ref.at[pl.ds(RHS, RHS)], sem.at[3]),
        pltpu.make_async_copy(ritz_hbm, held_ref.at[pl.ds(2 * RHS, RITZ)], sem.at[4]),
    ]
    for copy in copies:
        copy.start()
    for copy in copies:
        copy.wait()
    scaled = points_ref[...] * (scale_ref[...].T * math.sqrt(math.log2(math.e)))
    for b in range(NB // 2):
        near_ref[b, pl.ds(0, FEAT), :] = scaled
        near_ref[b, pl.ds(FEAT, VEC), :] = held_ref[pl.ds(RHS, VEC), :]
    for b in range(NB):
        pts_ref[b, pl.ds(0, FEAT), :] = scaled
        pts_ref[b, pl.ds(FEAT, RITZ), :] = held_ref[pl.ds(2 * RHS, RITZ), :]


def spread(points, scales, initial, ritz, targets):
    return pl.pallas_call(
        spread_kernel,
        in_specs=[hbm()] * 5,
        out_specs=[vmem()] * 3,
        out_shape=[shape(NB // 2, FEAT + VEC, BLK), shape(NB, FEAT + RITZ, BLK), shape(RHS + VEC, BLK)],
        scratch_shapes=[
            pltpu.VMEM((FEAT, BLK), F32),
            pltpu.VMEM((1, FEAT), F32),
            pltpu.SemaphoreType.DMA((5,)),
        ],
        compiler_params=limit(8),
        name="spread",
    )(*map(in_hbm, (points, scales, initial, ritz, targets)))


def tile_kernel(
    near_ref, far_ref, out_ref, hi_hbm, lo_hbm, part_ref, hi_ref, lo_ref, cols_ref, rows_ref, vec_ref, sem
):
    for b in range(NB):
        src = near_ref if b < NB // 2 else far_ref
        at = b % (NB // 2)
        lanes = pl.ds(b * BLK, BLK)
        cols_ref[:, lanes] = features(src[at, :FEAT, :], False).astype(BF16)
        tall = jnp.concatenate([src[at, FEAT:, :], jnp.zeros((BLK - VEC, BLK), F32)], axis=0).T
        hi, lo = split2(tall)
        vec_ref[lanes, pl.ds(0, BLK)] = hi
        vec_ref[lanes, pl.ds(BLK, BLK)] = lo
        rows_ref[lanes, :] = features(out_ref[b, :FEAT, :], True).T.astype(BF16)

    def copies(step):
        rows = pl.ds(step * STEP, STEP)
        return (
            pltpu.make_async_copy(hi_ref.at[rows], hi_hbm.at[rows], sem.at[0, step]),
            pltpu.make_async_copy(lo_ref.at[rows], lo_hbm.at[rows], sem.at[1, step]),
        )

    steps = PTS // STEP
    for step in range(steps + 1):
        rows, before = pl.ds(step * STEP, STEP), pl.ds((step - 1) * STEP, STEP)
        if step > 0:
            for copy in copies(step - 1):
                copy.start()
        total = jnp.zeros((STEP, 2 * BLK), F32)
        for c in range(PTS // CHUNK):
            lanes = pl.ds(c * CHUNK, CHUNK)
            if step > 0:
                vec = vec_ref[lanes, :]
                total += jnp.dot(hi_ref[before, lanes], vec, preferred_element_type=F32)
                total += jnp.dot(lo_ref[before, lanes], vec, preferred_element_type=F32)
            if step < steps:
                power = jnp.dot(rows_ref[rows, :], cols_ref[:, lanes], preferred_element_type=F32)
                hi, lo = split2(jnp.exp2(jnp.minimum(power, 0.0)))
                hi_ref[rows, lanes] = hi
                lo_ref[rows, lanes] = lo
        if step > 0:
            both = total[:, :BLK] + total[:, BLK:]
            for h in range(STEP // BLK):
                part_ref[(step - 1) * (STEP // BLK) + h] = both[h * BLK : (h + 1) * BLK].T[:VEC]
    for step in range(steps):
        for copy in copies(step):
            copy.wait()


def make_tile(near, far, out):
    return pl.pallas_call(
        tile_kernel,
        in_specs=[vmem(), vmem(), vmem()],
        out_specs=[hbm(), hbm(), vmem()],
        out_shape=[
            pltpu.HBM((PTS, PTS), BF16),
            pltpu.HBM((PTS, PTS), BF16),
            shape(NB, VEC, BLK),
        ],
        scratch_shapes=[
            pltpu.VMEM((PTS, PTS), BF16),
            pltpu.VMEM((PTS, PTS), BF16),
            pltpu.VMEM((BLK, PTS), BF16),
            pltpu.VMEM((PTS, BLK), BF16),
            pltpu.VMEM((PTS, 2 * BLK), BF16),
            pltpu.SemaphoreType.DMA((2, PTS // STEP)),
        ],
        compiler_params=limit(40),
        name="kernel_tile",
    )(near, far, out)


def owner_kernel(got_ref, held_ref, gain_ref, nugget_ref, out_ref):
    total = got_ref[0]
    for b in range(1, NB):
        total += got_ref[b]
    applied = gain_ref[0] * total + nugget_ref[0] * held_ref[pl.ds(RHS, VEC), :]
    first = held_ref[pl.ds(0, RHS), :] - applied[:RHS]
    image = applied[RHS:]
    for b in range(NB):
        out_ref[b, pl.ds(0, RHS), :] = first
        out_ref[b, pl.ds(RHS, RITZ), :] = image


def at_owner(got, held, gain, nugget):
    return pl.pallas_call(
        owner_kernel,
        in_specs=[vmem(), vmem(), smem(), smem()],
        out_shape=shape(NB, VEC, BLK),
        compiler_params=limit(8),
        name="at_owner",
    )(got, held, gain, nugget)


def square_iota():
    return lax.broadcasted_iota(jnp.int32, (RITZ, RITZ), 0), lax.broadcasted_iota(jnp.int32, (RITZ, RITZ), 1)


def gram_kernel(vec_ref, pts_ref, out_ref, left_ref, right_ref):
    for b in range(NB):
        lanes = pl.ds(b * BLK, BLK)
        left_ref[:, lanes] = vec_ref[b]
        right_ref[pl.ds(0, RITZ), lanes] = pts_ref[b, FEAT:, :]
        right_ref[pl.ds(RITZ, RITZ), lanes] = vec_ref[b, RHS:, :]
    gram = lax.dot_general(left_ref[...], right_ref[...], NT, precision=HIGH, preferred_element_type=F32)
    coarse = gram[RHS:, :RITZ]
    coarse = 0.5 * (coarse + coarse.T)
    image = gram[RHS:, RITZ:]
    i, j = square_iota()
    packed = jnp.where(j >= i, coarse, image)
    diagonal = jnp.sum(jnp.where(i == j, image, 0.0), axis=0, keepdims=True)
    for b in range(NB // 2):
        out_ref[b, pl.ds(0, RHS), :] = gram[:RHS]
        out_ref[b, pl.ds(RHS, RITZ // 2), :] = jnp.concatenate([packed[: RITZ // 2], packed[RITZ // 2 :]], axis=1)
        out_ref[b, pl.ds(RHS + RITZ // 2, 1), :] = jnp.concatenate([diagonal, diagonal], axis=1)


def make_gram(vec, pts):
    return pl.pallas_call(
        gram_kernel,
        out_shape=shape(NB // 2, PACKED, BLK),
        scratch_shapes=[pltpu.VMEM((VEC, PTS), F32), pltpu.VMEM((2 * RITZ, PTS), F32)],
        compiler_params=limit(12),
        name="gram",
    )(vec, pts)


def inverse(matrix):
    i, j = square_iota()
    work = jnp.concatenate([matrix, jnp.where(i == j, 1.0, 0.0)], axis=1)
    row = lax.broadcasted_iota(jnp.int32, work.shape, 0)
    for k in range(0, RITZ, 2):
        col0 = jnp.broadcast_to(work[:, k : k + 1], work.shape)
        col1 = jnp.broadcast_to(work[:, k + 1 : k + 2], work.shape)
        a, b = col0[k : k + 1], col1[k : k + 1]
        c, d = col0[k + 1 : k + 2], col1[k + 1 : k + 2]
        top, low = work[k : k + 1], work[k + 1 : k + 2]
        scale = 1.0 / (a * d - b * c)
        new_top = (d * top - b * low) * scale
        new_low = (a * low - c * top) * scale
        work = work - (col0 * new_top + col1 * new_low)
        work = jnp.where(row == k, new_top, jnp.where(row == k + 1, new_low, work))
    return work[:, RITZ:]


def apply_kernel(hi_hbm, lo_hbm, vec_ref, pts_ref, out_ref, rows_ref, hi_ref, lo_ref, sem):
    copies = []
    for step in range(PTS // READ):
        lanes = pl.ds(step * READ, READ)
        copies.append(
            (
                pltpu.make_async_copy(hi_hbm.at[:, lanes], hi_ref.at[:, lanes], sem.at[0, step]),
                pltpu.make_async_copy(lo_hbm.at[:, lanes], lo_ref.at[:, lanes], sem.at[1, step]),
            )
        )
        for copy in copies[-1]:
            copy.start()
    for b in range(NB):
        lanes = pl.ds(b * BLK, BLK)
        first = vec_ref[b, :RHS, :]
        hi, lo = split2(
            jnp.concatenate([first, jnp.zeros_like(first), pts_ref[b, FEAT:, :], vec_ref[b, RHS:, :]], axis=0)
        )
        rows_ref[pl.ds(0, HALF), lanes] = hi
        rows_ref[pl.ds(HALF, HALF), lanes] = lo
    for step in range(PTS // READ):
        lanes = pl.ds(step * READ, READ)
        for copy in copies[step]:
            copy.wait()
        both = jnp.dot(rows_ref[...], hi_ref[:, lanes], preferred_element_type=F32)
        more = jnp.dot(rows_ref[pl.ds(0, HALF), :], lo_ref[:, lanes], preferred_element_type=F32)
        out_ref[:, lanes] = both[:HALF] + both[HALF:] + more


def apply_tile(hi, lo, vec, pts):
    return pl.pallas_call(
        apply_kernel,
        in_specs=[hbm(), hbm(), vmem(), vmem()],
        out_shape=shape(HALF, PTS),
        scratch_shapes=[
            pltpu.VMEM((2 * HALF, PTS), BF16),
            pltpu.VMEM((PTS, PTS), BF16),
            pltpu.VMEM((PTS, PTS), BF16),
            pltpu.SemaphoreType.DMA((2, PTS // READ)),
        ],
        compiler_params=limit(32),
        cost_estimate=pl.CostEstimate(flops=8 * HALF * PTS * PTS, bytes_accessed=4 * PTS * PTS, transcendentals=0),
        name="apply_tile",
    )(in_hbm(hi), in_hbm(lo), vec, pts)


def solve_kernel(gram_ref, more_ref, image_ref, vec_ref, pts_ref, held_ref, place_ref, part_ref, own_ref):
    gram = gram_ref[...] + more_ref[...]
    projected = gram[:RHS, :RITZ]
    first = gram[:RHS, RITZ:]
    square = jnp.concatenate([gram[RHS : RHS + RITZ // 2, :RITZ], gram[RHS : RHS + RITZ // 2, RITZ:]], axis=0)
    turned = square.T
    i, j = square_iota()
    coarse = jnp.where(j >= i, square, turned)
    image = jnp.where(j < i, square, jnp.where(j > i, turned, gram[RHS + RITZ // 2 :, :RITZ]))
    solve = inverse(coarse)
    amounts = lax.dot_general(projected, solve, NT, precision=HIGH, preferred_element_type=F32)
    against = first - jnp.dot(amounts, image, precision=HIGH, preferred_element_type=F32)
    turns = lax.dot_general(against, solve, NT, precision=HIGH, preferred_element_type=F32)
    zero = jnp.zeros_like(turns)
    coef = jnp.concatenate([turns, amounts], axis=1)
    value = image_ref[pl.ds(0, RHS), :] - jnp.dot(
        coef, image_ref[pl.ds(2 * RHS, 2 * RITZ), :], precision=HIGH, preferred_element_type=F32
    )
    for at in range(NB):
        half = (at // (NB // 2) + place_ref[1]) % 2
        part_ref[half * (NB // 2) + at % (NB // 2)] = value[:, at * BLK : (at + 1) * BLK]
    mine = place_ref[0]
    basis = jnp.concatenate([pts_ref[mine, FEAT:, :], vec_ref[mine, RHS:, :]], axis=0)
    wanted = jnp.concatenate(
        [coef, jnp.concatenate([zero, amounts], axis=1), jnp.concatenate([-amounts, zero], axis=1)], axis=0
    )
    base = vec_ref[mine, :RHS, :]
    base = jnp.concatenate([base, base, held_ref[pl.ds(RHS, RHS), :]], axis=0)
    own_ref[...] = base - jnp.dot(wanted, basis, precision=HIGH, preferred_element_type=F32)


def solve(gram, more, image, vec, pts, held, place):
    return pl.pallas_call(
        solve_kernel,
        in_specs=[vmem()] * 6 + [smem()],
        out_shape=[shape(NB, RHS, BLK), shape(3 * RHS, BLK)],
        compiler_params=limit(12),
        name="solve",
    )(gram, more, image, vec, pts, held, place)


def stats_kernel(got_ref, own_ref, gain_ref, nugget_ref, applied_ref, out_ref):
    total = got_ref[0]
    for b in range(1, NB):
        total += got_ref[b]
    direction = own_ref[pl.ds(0, RHS), :]
    residual = own_ref[pl.ds(RHS, RHS), :]
    applied = gain_ref[0] * total + nugget_ref[0] * direction
    applied_ref[...] = applied
    sums = jnp.concatenate(
        [
            jnp.sum(direction * applied, axis=1, keepdims=True),
            jnp.sum(residual * residual, axis=1, keepdims=True),
        ],
        axis=0,
    )
    sums = jnp.broadcast_to(sums, (2 * RHS, BLK)).T[:RHS]
    for b in range(WORLD // RHS):
        out_ref[pl.ds(b * RHS, RHS), :] = sums


def make_stats(got, own, gain, nugget):
    return pl.pallas_call(
        stats_kernel,
        in_specs=[vmem(), vmem(), smem(), smem()],
        out_shape=[shape(RHS, BLK), shape(WORLD, 2 * RHS)],
        compiler_params=limit(8),
        name="stats",
    )(got, own, gain, nugget)


def finish_kernel(got_ref, own_ref, applied_ref, solution_ref, residual_ref):
    sums = jnp.sum(got_ref[...], axis=0, keepdims=True)
    i = lax.broadcasted_iota(jnp.int32, (2 * RHS, 2 * RHS), 0)
    j = lax.broadcasted_iota(jnp.int32, (2 * RHS, 2 * RHS), 1)
    sums = jnp.sum(jnp.where(i == j, sums, 0.0), axis=1, keepdims=True)
    size = sums[RHS:] / sums[:RHS]
    solution_ref[...] = own_ref[pl.ds(2 * RHS, RHS), :] + size * own_ref[pl.ds(0, RHS), :]
    residual_ref[...] = own_ref[pl.ds(RHS, RHS), :] - size * applied_ref[...]


def finish(got, own, applied):
    return pl.pallas_call(
        finish_kernel,
        out_shape=[shape(RHS, BLK), shape(RHS, BLK)],
        compiler_params=limit(8),
        name="finish",
    )(got, own, applied)


def exchange(pieces, axis):
    return lax.all_to_all(pieces, axis, split_axis=0, concat_axis=0, tiled=True)


def other_core(array):
    return lax.ppermute(array, CORE, [(0, 1), (1, 0)])


def local(points, inv_scales, amplitude, noise_var, targets, initial, ritz_basis):
    near, pts, held = spread(points, inv_scales[None, :], initial, ritz_basis, targets)
    pts = exchange(pts, XY)
    near, pts = lax.optimization_barrier((near, pts))
    near = exchange(near, Z)
    far = other_core(near)
    hi, lo, part = make_tile(near, far, pts)

    vec = exchange(at_owner(exchange(part, XY), held, amplitude, noise_var), XY)
    gram = jnp.sum(exchange(make_gram(vec, pts), Z), axis=0)
    image = apply_tile(hi, lo, vec, pts)
    place = jnp.stack([lax.axis_index(XY), lax.axis_index(CORE)]).astype(jnp.int32)
    part, own = solve(gram, other_core(gram), image, vec, pts, held, place)
    applied, stats = make_stats(exchange(part, CZ), own, amplitude, noise_var)
    return tuple(finish(exchange(stats, EVERY), own, applied))


def solution(mesh):
    torus = Mesh(mesh.devices.reshape(4, 8, 4, 2), ("row_0", "row_1", "col_0", "col_1"))
    in_specs = (
        P(None, COL_ROW),
        P(),
        P(),
        P(),
        P(None, COL_ROW),
        P(None, COL_ROW),
        P(None, COL_ROW),
    )
    out_specs = (P(None, COL_ROW), P(None, COL_ROW))
    return jax.shard_map(local, mesh=torus, in_specs=in_specs, out_specs=out_specs, check_vma=False)
```

```python
import math

import jax
import jax.numpy as jnp
from jax import lax
from jax.experimental import pallas as pl
from jax.experimental.pallas import tpu as pltpu
from jax.sharding import Mesh
from jax.sharding import PartitionSpec as P

CORE = "col_1"
Z = "row_1"
XY = ("col_0", "row_0")
CZ = ("col_1", "row_1")
EVERY = ("col_0", "col_1", "row_0", "row_1")
COL_ROW = EVERY

FEAT = 16
RITZ = 64
RHS = 8
VEC = RHS + RITZ
BLK = 128
NB = 16
PTS = NB * BLK
STEP = 256
CHUNK = 256
READ = 512
HALF = 2 * RHS + 2 * RITZ
PACKED = RHS + RITZ // 2 + 1
WORLD = 256

HIGH = lax.Precision.HIGHEST
F32 = jnp.float32
BF16 = jnp.bfloat16
NT = (((1,), (1,)), ((), ()))


def split2(x):
    hi = x.astype(BF16)
    return hi, (x - hi.astype(F32)).astype(BF16)


def split3(x):
    hi = x.astype(BF16).astype(F32)
    rest = x - hi
    mid = rest.astype(BF16).astype(F32)
    return hi, mid, rest - mid


def features(x, swap):
    a, b, c = split3(x)
    n1, n2, n3 = split3(-0.5 * jnp.sum(x * x, axis=0, keepdims=True))
    row = lax.broadcasted_iota(jnp.int32, x.shape, 0)
    base = 3 if swap else 0
    norm = jnp.where(row == base, n1, jnp.where(row == base + 1, n2, jnp.where(row == base + 2, n3, 0.0)))
    one = 0 if swap else 3
    norm = jnp.where((row >= one) & (row < one + 3), 1.0, norm)
    zero = jnp.zeros_like(x)
    if swap:
        parts = [a, b, a, b, c, a, norm, zero]
    else:
        parts = [a, a, b, b, a, c, norm, zero]
    return jnp.concatenate(parts, axis=0)


def vmem():
    return pl.BlockSpec(memory_space=pltpu.VMEM)


def in_hbm(array):
    return pltpu.with_memory_space_constraint(array, pltpu.HBM)


def smem():
    return pl.BlockSpec(memory_space=pltpu.SMEM)


def shape(*dims):
    return jax.ShapeDtypeStruct(dims, F32)


def limit(mib):
    return pltpu.CompilerParams(vmem_limit_bytes=mib << 20)


def hbm():
    return pl.BlockSpec(memory_space=pltpu.HBM)


def spread_kernel(
    points_hbm, scale_hbm, initial_hbm, ritz_hbm, targets_hbm, near_ref, pts_ref, held_ref, points_ref, scale_ref, sem
):
    copies = [
        pltpu.make_async_copy(points_hbm, points_ref, sem.at[0]),
        pltpu.make_async_copy(scale_hbm, scale_ref, sem.at[1]),
        pltpu.make_async_copy(targets_hbm, held_ref.at[pl.ds(0, RHS)], sem.at[2]),
        pltpu.make_async_copy(initial_hbm, held_ref.at[pl.ds(RHS, RHS)], sem.at[3]),
        pltpu.make_async_copy(ritz_hbm, held_ref.at[pl.ds(2 * RHS, RITZ)], sem.at[4]),
    ]
    for copy in copies:
        copy.start()
    for copy in copies:
        copy.wait()
    scaled = points_ref[...] * (scale_ref[...].T * math.sqrt(math.log2(math.e)))
    for b in range(NB // 2):
        near_ref[b, pl.ds(0, FEAT), :] = scaled
        near_ref[b, pl.ds(FEAT, VEC), :] = held_ref[pl.ds(RHS, VEC), :]
    for b in range(NB):
        pts_ref[b, pl.ds(0, FEAT), :] = scaled
        pts_ref[b, pl.ds(FEAT, RITZ), :] = held_ref[pl.ds(2 * RHS, RITZ), :]


def spread(points, scales, initial, ritz, targets):
    return pl.pallas_call(
        spread_kernel,
        in_specs=[hbm()] * 5,
        out_specs=[vmem()] * 3,
        out_shape=[shape(NB // 2, FEAT + VEC, BLK), shape(NB, FEAT + RITZ, BLK), shape(RHS + VEC, BLK)],
        scratch_shapes=[
            pltpu.VMEM((FEAT, BLK), F32),
            pltpu.VMEM((1, FEAT), F32),
            pltpu.SemaphoreType.DMA((5,)),
        ],
        compiler_params=limit(8),
        name="spread",
    )(*map(in_hbm, (points, scales, initial, ritz, targets)))


def tile_kernel(
    near_ref, far_ref, out_ref, hi_hbm, lo_hbm, part_ref, hi_ref, lo_ref, cols_ref, rows_ref, vec_ref, sem
):
    for b in range(NB):
        src = near_ref if b < NB // 2 else far_ref
        at = b % (NB // 2)
        lanes = pl.ds(b * BLK, BLK)
        cols_ref[:, lanes] = features(src[at, :FEAT, :], False).astype(BF16)
        tall = jnp.concatenate([src[at, FEAT:, :], jnp.zeros((BLK - VEC, BLK), F32)], axis=0).T
        hi, lo = split2(tall)
        vec_ref[lanes, pl.ds(0, BLK)] = hi
        vec_ref[lanes, pl.ds(BLK, BLK)] = lo
        rows_ref[lanes, :] = features(out_ref[b, :FEAT, :], True).T.astype(BF16)

    def copies(step):
        rows = pl.ds(step * STEP, STEP)
        return (
            pltpu.make_async_copy(hi_ref.at[rows], hi_hbm.at[rows], sem.at[0, step]),
            pltpu.make_async_copy(lo_ref.at[rows], lo_hbm.at[rows], sem.at[1, step]),
        )

    steps = PTS // STEP
    for step in range(steps + 1):
        rows, before = pl.ds(step * STEP, STEP), pl.ds((step - 1) * STEP, STEP)
        if step > 0:
            for copy in copies(step - 1):
                copy.start()
        total = jnp.zeros((STEP, 2 * BLK), F32)
        for c in range(PTS // CHUNK):
            lanes = pl.ds(c * CHUNK, CHUNK)
            if step > 0:
                vec = vec_ref[lanes, :]
                total += jnp.dot(hi_ref[before, lanes], vec, preferred_element_type=F32)
                total += jnp.dot(lo_ref[before, lanes], vec, preferred_element_type=F32)
            if step < steps:
                power = jnp.dot(rows_ref[rows, :], cols_ref[:, lanes], preferred_element_type=F32)
                hi, lo = split2(jnp.exp2(jnp.minimum(power, 0.0)))
                hi_ref[rows, lanes] = hi
                lo_ref[rows, lanes] = lo
        if step > 0:
            both = total[:, :BLK] + total[:, BLK:]
            for h in range(STEP // BLK):
                part_ref[(step - 1) * (STEP // BLK) + h] = both[h * BLK : (h + 1) * BLK].T[:VEC]
    for step in range(steps):
        for copy in copies(step):
            copy.wait()


def make_tile(near, far, out):
    return pl.pallas_call(
        tile_kernel,
        in_specs=[vmem(), vmem(), vmem()],
        out_specs=[hbm(), hbm(), vmem()],
        out_shape=[
            pltpu.HBM((PTS, PTS), BF16),
            pltpu.HBM((PTS, PTS), BF16),
            shape(NB, VEC, BLK),
        ],
        scratch_shapes=[
            pltpu.VMEM((PTS, PTS), BF16),
            pltpu.VMEM((PTS, PTS), BF16),
            pltpu.VMEM((BLK, PTS), BF16),
            pltpu.VMEM((PTS, BLK), BF16),
            pltpu.VMEM((PTS, 2 * BLK), BF16),
            pltpu.SemaphoreType.DMA((2, PTS // STEP)),
        ],
        compiler_params=limit(40),
        name="kernel_tile",
    )(near, far, out)


def owner_kernel(got_ref, held_ref, gain_ref, nugget_ref, out_ref):
    total = got_ref[0]
    for b in range(1, NB):
        total += got_ref[b]
    applied = gain_ref[0] * total + nugget_ref[0] * held_ref[pl.ds(RHS, VEC), :]
    first = held_ref[pl.ds(0, RHS), :] - applied[:RHS]
    image = applied[RHS:]
    for b in range(NB):
        out_ref[b, pl.ds(0, RHS), :] = first
        out_ref[b, pl.ds(RHS, RITZ), :] = image


def at_owner(got, held, gain, nugget):
    return pl.pallas_call(
        owner_kernel,
        in_specs=[vmem(), vmem(), smem(), smem()],
        out_shape=shape(NB, VEC, BLK),
        compiler_params=limit(8),
        name="at_owner",
    )(got, held, gain, nugget)


def square_iota():
    return lax.broadcasted_iota(jnp.int32, (RITZ, RITZ), 0), lax.broadcasted_iota(jnp.int32, (RITZ, RITZ), 1)


def gram_kernel(vec_ref, pts_ref, out_ref, left_ref, right_ref):
    for b in range(NB):
        lanes = pl.ds(b * BLK, BLK)
        left_ref[:, lanes] = vec_ref[b]
        right_ref[pl.ds(0, RITZ), lanes] = pts_ref[b, FEAT:, :]
        right_ref[pl.ds(RITZ, RITZ), lanes] = vec_ref[b, RHS:, :]
    gram = lax.dot_general(left_ref[...], right_ref[...], NT, precision=HIGH, preferred_element_type=F32)
    coarse = gram[RHS:, :RITZ]
    coarse = 0.5 * (coarse + coarse.T)
    image = gram[RHS:, RITZ:]
    i, j = square_iota()
    packed = jnp.where(j >= i, coarse, image)
    diagonal = jnp.sum(jnp.where(i == j, image, 0.0), axis=0, keepdims=True)
    for b in range(NB // 2):
        out_ref[b, pl.ds(0, RHS), :] = gram[:RHS]
        out_ref[b, pl.ds(RHS, RITZ // 2), :] = jnp.concatenate([packed[: RITZ // 2], packed[RITZ // 2 :]], axis=1)
        out_ref[b, pl.ds(RHS + RITZ // 2, 1), :] = jnp.concatenate([diagonal, diagonal], axis=1)


def make_gram(vec, pts):
    return pl.pallas_call(
        gram_kernel,
        out_shape=shape(NB // 2, PACKED, BLK),
        scratch_shapes=[pltpu.VMEM((VEC, PTS), F32), pltpu.VMEM((2 * RITZ, PTS), F32)],
        compiler_params=limit(12),
        name="gram",
    )(vec, pts)


def inverse(matrix):
    i, j = square_iota()
    work = jnp.concatenate([matrix, jnp.where(i == j, 1.0, 0.0)], axis=1)
    row = lax.broadcasted_iota(jnp.int32, work.shape, 0)
    for k in range(0, RITZ, 2):
        col0 = jnp.broadcast_to(work[:, k : k + 1], work.shape)
        col1 = jnp.broadcast_to(work[:, k + 1 : k + 2], work.shape)
        a, b = col0[k : k + 1], col1[k : k + 1]
        c, d = col0[k + 1 : k + 2], col1[k + 1 : k + 2]
        top, low = work[k : k + 1], work[k + 1 : k + 2]
        scale = 1.0 / (a * d - b * c)
        new_top = (d * top - b * low) * scale
        new_low = (a * low - c * top) * scale
        work = work - (col0 * new_top + col1 * new_low)
        work = jnp.where(row == k, new_top, jnp.where(row == k + 1, new_low, work))
    return work[:, RITZ:]


def apply_kernel(hi_hbm, lo_hbm, vec_ref, pts_ref, out_ref, rows_ref, hi_ref, lo_ref, sem):
    copies = []
    for step in range(PTS // READ):
        lanes = pl.ds(step * READ, READ)
        copies.append(
            (
                pltpu.make_async_copy(hi_hbm.at[:, lanes], hi_ref.at[:, lanes], sem.at[0, step]),
                pltpu.make_async_copy(lo_hbm.at[:, lanes], lo_ref.at[:, lanes], sem.at[1, step]),
            )
        )
        for copy in copies[-1]:
            copy.start()
    for b in range(NB):
        lanes = pl.ds(b * BLK, BLK)
        first = vec_ref[b, :RHS, :]
        hi, lo = split2(
            jnp.concatenate([first, jnp.zeros_like(first), pts_ref[b, FEAT:, :], vec_ref[b, RHS:, :]], axis=0)
        )
        rows_ref[pl.ds(0, HALF), lanes] = hi
        rows_ref[pl.ds(HALF, HALF), lanes] = lo
    for step in range(PTS // READ):
        lanes = pl.ds(step * READ, READ)
        for copy in copies[step]:
            copy.wait()
        both = jnp.dot(rows_ref[...], hi_ref[:, lanes], preferred_element_type=F32)
        more = jnp.dot(rows_ref[pl.ds(0, HALF), :], lo_ref[:, lanes], preferred_element_type=F32)
        out_ref[:, lanes] = both[:HALF] + both[HALF:] + more


def apply_tile(hi, lo, vec, pts):
    return pl.pallas_call(
        apply_kernel,
        in_specs=[hbm(), hbm(), vmem(), vmem()],
        out_shape=shape(HALF, PTS),
        scratch_shapes=[
            pltpu.VMEM((2 * HALF, PTS), BF16),
            pltpu.VMEM((PTS, PTS), BF16),
            pltpu.VMEM((PTS, PTS), BF16),
            pltpu.SemaphoreType.DMA((2, PTS // READ)),
        ],
        compiler_params=limit(32),
        cost_estimate=pl.CostEstimate(flops=8 * HALF * PTS * PTS, bytes_accessed=4 * PTS * PTS, transcendentals=0),
        name="apply_tile",
    )(in_hbm(hi), in_hbm(lo), vec, pts)


def solve_kernel(gram_ref, more_ref, image_ref, vec_ref, pts_ref, held_ref, place_ref, part_ref, own_ref):
    gram = gram_ref[...] + more_ref[...]
    projected = gram[:RHS, :RITZ]
    first = gram[:RHS, RITZ:]
    square = jnp.concatenate([gram[RHS : RHS + RITZ // 2, :RITZ], gram[RHS : RHS + RITZ // 2, RITZ:]], axis=0)
    turned = square.T
    i, j = square_iota()
    coarse = jnp.where(j >= i, square, turned)
    image = jnp.where(j < i, square, jnp.where(j > i, turned, gram[RHS + RITZ // 2 :, :RITZ]))
    solve = inverse(coarse)
    amounts = lax.dot_general(projected, solve, NT, precision=HIGH, preferred_element_type=F32)
    against = first - jnp.dot(amounts, image, precision=HIGH, preferred_element_type=F32)
    turns = lax.dot_general(against, solve, NT, precision=HIGH, preferred_element_type=F32)
    zero = jnp.zeros_like(turns)
    coef = jnp.concatenate([turns, amounts], axis=1)
    value = image_ref[pl.ds(0, RHS), :] - jnp.dot(
        coef, image_ref[pl.ds(2 * RHS, 2 * RITZ), :], precision=HIGH, preferred_element_type=F32
    )
    for at in range(NB):
        half = (at // (NB // 2) + place_ref[1]) % 2
        part_ref[half * (NB // 2) + at % (NB // 2)] = value[:, at * BLK : (at + 1) * BLK]
    mine = place_ref[0]
    basis = jnp.concatenate([pts_ref[mine, FEAT:, :], vec_ref[mine, RHS:, :]], axis=0)
    wanted = jnp.concatenate(
        [coef, jnp.concatenate([zero, amounts], axis=1), jnp.concatenate([-amounts, zero], axis=1)], axis=0
    )
    base = vec_ref[mine, :RHS, :]
    base = jnp.concatenate([base, base, held_ref[pl.ds(RHS, RHS), :]], axis=0)
    own_ref[...] = base - jnp.dot(wanted, basis, precision=HIGH, preferred_element_type=F32)


def solve(gram, more, image, vec, pts, held, place):
    return pl.pallas_call(
        solve_kernel,
        in_specs=[vmem()] * 6 + [smem()],
        out_shape=[shape(NB, RHS, BLK), shape(3 * RHS, BLK)],
        compiler_params=limit(12),
        name="solve",
    )(gram, more, image, vec, pts, held, place)


def stats_kernel(got_ref, own_ref, gain_ref, nugget_ref, applied_ref, out_ref):
    total = got_ref[0]
    for b in range(1, NB):
        total += got_ref[b]
    direction = own_ref[pl.ds(0, RHS), :]
    residual = own_ref[pl.ds(RHS, RHS), :]
    applied = gain_ref[0] * total + nugget_ref[0] * direction
    applied_ref[...] = applied
    sums = jnp.concatenate(
        [
            jnp.sum(direction * applied, axis=1, keepdims=True),
            jnp.sum(residual * residual, axis=1, keepdims=True),
        ],
        axis=0,
    )
    sums = jnp.broadcast_to(sums, (2 * RHS, BLK)).T[:RHS]
    for b in range(WORLD // RHS):
        out_ref[pl.ds(b * RHS, RHS), :] = sums


def make_stats(got, own, gain, nugget):
    return pl.pallas_call(
        stats_kernel,
        in_specs=[vmem(), vmem(), smem(), smem()],
        out_shape=[shape(RHS, BLK), shape(WORLD, 2 * RHS)],
        compiler_params=limit(8),
        name="stats",
    )(got, own, gain, nugget)


def finish_kernel(got_ref, own_ref, applied_ref, solution_ref, residual_ref):
    sums = jnp.sum(got_ref[...], axis=0, keepdims=True)
    i = lax.broadcasted_iota(jnp.int32, (2 * RHS, 2 * RHS), 0)
    j = lax.broadcasted_iota(jnp.int32, (2 * RHS, 2 * RHS), 1)
    sums = jnp.sum(jnp.where(i == j, sums, 0.0), axis=1, keepdims=True)
    size = sums[RHS:] / sums[:RHS]
    solution_ref[...] = own_ref[pl.ds(2 * RHS, RHS), :] + size * own_ref[pl.ds(0, RHS), :]
    residual_ref[...] = own_ref[pl.ds(RHS, RHS), :] - size * applied_ref[...]


def finish(got, own, applied):
    return pl.pallas_call(
        finish_kernel,
        out_shape=[shape(RHS, BLK), shape(RHS, BLK)],
        compiler_params=limit(8),
        name="finish",
    )(got, own, applied)


def exchange(pieces, axis):
    return lax.all_to_all(pieces, axis, split_axis=0, concat_axis=0, tiled=True)


def other_core(array):
    return lax.ppermute(array, CORE, [(0, 1), (1, 0)])


def local(points, inv_scales, amplitude, noise_var, targets, initial, ritz_basis):
    near, pts, held = spread(points, inv_scales[None, :], initial, ritz_basis, targets)
    near = exchange(near, Z)
    near, pts = lax.optimization_barrier((near, pts))
    far = other_core(near)
    pts = exchange(pts, XY)
    hi, lo, part = make_tile(near, far, pts)

    vec = exchange(at_owner(exchange(part, XY), held, amplitude, noise_var), XY)
    gram = make_gram(vec, pts)
    vec, gram = lax.optimization_barrier((vec, gram))
    image = apply_tile(hi, lo, vec, pts)
    image, gram = lax.optimization_barrier((image, exchange(gram, Z)))
    gram = jnp.sum(gram, axis=0)
    place = jnp.stack([lax.axis_index(XY), lax.axis_index(CORE)]).astype(jnp.int32)
    part, own = solve(gram, other_core(gram), image, vec, pts, held, place)
    applied, stats = make_stats(exchange(part, CZ), own, amplitude, noise_var)
    return tuple(finish(exchange(stats, EVERY), own, applied))


def solution(mesh):
    torus = Mesh(mesh.devices.reshape(4, 8, 4, 2), ("row_0", "row_1", "col_0", "col_1"))
    in_specs = (
        P(None, COL_ROW),
        P(),
        P(),
        P(),
        P(None, COL_ROW),
        P(None, COL_ROW),
        P(None, COL_ROW),
    )
    out_specs = (P(None, COL_ROW), P(None, COL_ROW))
    return jax.shard_map(local, mesh=torus, in_specs=in_specs, out_specs=out_specs, check_vma=False)
```

```python
import math

import jax
import jax.numpy as jnp
from jax import lax
from jax.experimental import pallas as pl
from jax.experimental.pallas import tpu as pltpu
from jax.sharding import Mesh
from jax.sharding import PartitionSpec as P

CORE = "col_1"
Z = "row_1"
XY = ("col_0", "row_0")
CZ = ("col_1", "row_1")
EVERY = ("col_0", "col_1", "row_0", "row_1")
COL_ROW = EVERY

FEAT = 16
RITZ = 64
RHS = 8
VEC = RHS + RITZ
BLK = 128
NB = 16
PTS = NB * BLK
STEP = 256
CHUNK = 256
READ = 512
HALF = 2 * RHS + 2 * RITZ
PACKED = RHS + RITZ // 2 + 1
WORLD = 256

HIGH = lax.Precision.HIGHEST
F32 = jnp.float32
BF16 = jnp.bfloat16
NT = (((1,), (1,)), ((), ()))


def split2(x):
    hi = x.astype(BF16)
    return hi, (x - hi.astype(F32)).astype(BF16)


def split3(x):
    hi = x.astype(BF16).astype(F32)
    rest = x - hi
    mid = rest.astype(BF16).astype(F32)
    return hi, mid, rest - mid


def features(x, swap):
    a, b, c = split3(x)
    n1, n2, n3 = split3(-0.5 * jnp.sum(x * x, axis=0, keepdims=True))
    row = lax.broadcasted_iota(jnp.int32, x.shape, 0)
    base = 3 if swap else 0
    norm = jnp.where(row == base, n1, jnp.where(row == base + 1, n2, jnp.where(row == base + 2, n3, 0.0)))
    one = 0 if swap else 3
    norm = jnp.where((row >= one) & (row < one + 3), 1.0, norm)
    zero = jnp.zeros_like(x)
    if swap:
        parts = [a, b, a, b, c, a, norm, zero]
    else:
        parts = [a, a, b, b, a, c, norm, zero]
    return jnp.concatenate(parts, axis=0)


def vmem():
    return pl.BlockSpec(memory_space=pltpu.VMEM)


def in_hbm(array):
    return pltpu.with_memory_space_constraint(array, pltpu.HBM)


def smem():
    return pl.BlockSpec(memory_space=pltpu.SMEM)


def shape(*dims):
    return jax.ShapeDtypeStruct(dims, F32)


def limit(mib):
    return pltpu.CompilerParams(vmem_limit_bytes=mib << 20)


def hbm():
    return pl.BlockSpec(memory_space=pltpu.HBM)


def spread_kernel(
    points_hbm, scale_hbm, initial_hbm, ritz_hbm, targets_hbm, near_ref, pts_ref, held_ref, points_ref, scale_ref, sem
):
    copies = [
        pltpu.make_async_copy(points_hbm, points_ref, sem.at[0]),
        pltpu.make_async_copy(scale_hbm, scale_ref, sem.at[1]),
        pltpu.make_async_copy(targets_hbm, held_ref.at[pl.ds(0, RHS)], sem.at[2]),
        pltpu.make_async_copy(initial_hbm, held_ref.at[pl.ds(RHS, RHS)], sem.at[3]),
        pltpu.make_async_copy(ritz_hbm, held_ref.at[pl.ds(2 * RHS, RITZ)], sem.at[4]),
    ]
    for copy in copies:
        copy.start()
    for copy in copies:
        copy.wait()
    scaled = points_ref[...] * (scale_ref[...].T * math.sqrt(math.log2(math.e)))
    for b in range(NB // 2):
        near_ref[b, pl.ds(0, FEAT), :] = scaled
        near_ref[b, pl.ds(FEAT, VEC), :] = held_ref[pl.ds(RHS, VEC), :]
    pts_ref[0, pl.ds(0, FEAT), :] = scaled
    pts_ref[0, pl.ds(FEAT, RITZ), :] = held_ref[pl.ds(2 * RHS, RITZ), :]


def spread(points, scales, initial, ritz, targets):
    return pl.pallas_call(
        spread_kernel,
        in_specs=[hbm()] * 5,
        out_specs=[vmem()] * 3,
        out_shape=[shape(NB // 2, FEAT + VEC, BLK), shape(1, FEAT + RITZ, BLK), shape(RHS + VEC, BLK)],
        scratch_shapes=[
            pltpu.VMEM((FEAT, BLK), F32),
            pltpu.VMEM((1, FEAT), F32),
            pltpu.SemaphoreType.DMA((5,)),
        ],
        compiler_params=limit(8),
        name="spread",
    )(*map(in_hbm, (points, scales, initial, ritz, targets)))


def arrived(b, place_ref):
    side = 4
    return ((place_ref[1] - b % side + side) % side) * side + (place_ref[0] - b // side + side) % side


def tile_kernel(
    near_ref, far_ref, out_ref, place_ref, hi_hbm, lo_hbm, part_ref, hi_ref, lo_ref, cols_ref, rows_ref, vec_ref, sem
):
    for b in range(NB):
        src = near_ref if b < NB // 2 else far_ref
        at = b % (NB // 2)
        lanes = pl.ds(b * BLK, BLK)
        cols_ref[:, lanes] = features(src[at, :FEAT, :], False).astype(BF16)
        tall = jnp.concatenate([src[at, FEAT:, :], jnp.zeros((BLK - VEC, BLK), F32)], axis=0).T
        hi, lo = split2(tall)
        vec_ref[lanes, pl.ds(0, BLK)] = hi
        vec_ref[lanes, pl.ds(BLK, BLK)] = lo
        rows_ref[lanes, :] = features(out_ref[arrived(b, place_ref), :FEAT, :], True).T.astype(BF16)

    def copies(step):
        rows = pl.ds(step * STEP, STEP)
        return (
            pltpu.make_async_copy(hi_ref.at[rows], hi_hbm.at[rows], sem.at[0, step]),
            pltpu.make_async_copy(lo_ref.at[rows], lo_hbm.at[rows], sem.at[1, step]),
        )

    steps = PTS // STEP
    for step in range(steps + 1):
        rows, before = pl.ds(step * STEP, STEP), pl.ds((step - 1) * STEP, STEP)
        if step > 0:
            for copy in copies(step - 1):
                copy.start()
        total = jnp.zeros((STEP, 2 * BLK), F32)
        for c in range(PTS // CHUNK):
            lanes = pl.ds(c * CHUNK, CHUNK)
            if step > 0:
                vec = vec_ref[lanes, :]
                total += jnp.dot(hi_ref[before, lanes], vec, preferred_element_type=F32)
                total += jnp.dot(lo_ref[before, lanes], vec, preferred_element_type=F32)
            if step < steps:
                power = jnp.dot(rows_ref[rows, :], cols_ref[:, lanes], preferred_element_type=F32)
                hi, lo = split2(jnp.exp2(jnp.minimum(power, 0.0)))
                hi_ref[rows, lanes] = hi
                lo_ref[rows, lanes] = lo
        if step > 0:
            both = total[:, :BLK] + total[:, BLK:]
            for h in range(STEP // BLK):
                part_ref[(step - 1) * (STEP // BLK) + h] = both[h * BLK : (h + 1) * BLK].T[:VEC]
    for step in range(steps):
        for copy in copies(step):
            copy.wait()


def make_tile(near, far, out, place):
    return pl.pallas_call(
        tile_kernel,
        in_specs=[vmem(), vmem(), vmem(), smem()],
        out_specs=[hbm(), hbm(), vmem()],
        out_shape=[
            pltpu.HBM((PTS, PTS), BF16),
            pltpu.HBM((PTS, PTS), BF16),
            shape(NB, VEC, BLK),
        ],
        scratch_shapes=[
            pltpu.VMEM((PTS, PTS), BF16),
            pltpu.VMEM((PTS, PTS), BF16),
            pltpu.VMEM((BLK, PTS), BF16),
            pltpu.VMEM((PTS, BLK), BF16),
            pltpu.VMEM((PTS, 2 * BLK), BF16),
            pltpu.SemaphoreType.DMA((2, PTS // STEP)),
        ],
        compiler_params=limit(40),
        name="kernel_tile",
    )(near, far, out, place)


def owner_kernel(got_ref, held_ref, gain_ref, nugget_ref, out_ref):
    total = got_ref[0]
    for b in range(1, NB):
        total += got_ref[b]
    applied = gain_ref[0] * total + nugget_ref[0] * held_ref[pl.ds(RHS, VEC), :]
    first = held_ref[pl.ds(0, RHS), :] - applied[:RHS]
    image = applied[RHS:]
    for b in range(NB):
        out_ref[b, pl.ds(0, RHS), :] = first
        out_ref[b, pl.ds(RHS, RITZ), :] = image


def at_owner(got, held, gain, nugget):
    return pl.pallas_call(
        owner_kernel,
        in_specs=[vmem(), vmem(), smem(), smem()],
        out_shape=shape(NB, VEC, BLK),
        compiler_params=limit(8),
        name="at_owner",
    )(got, held, gain, nugget)


def square_iota():
    return lax.broadcasted_iota(jnp.int32, (RITZ, RITZ), 0), lax.broadcasted_iota(jnp.int32, (RITZ, RITZ), 1)


def gram_kernel(vec_ref, pts_ref, place_ref, out_ref, left_ref, right_ref):
    for b in range(NB):
        lanes = pl.ds(b * BLK, BLK)
        left_ref[:, lanes] = vec_ref[b]
        right_ref[pl.ds(0, RITZ), lanes] = pts_ref[arrived(b, place_ref), FEAT:, :]
        right_ref[pl.ds(RITZ, RITZ), lanes] = vec_ref[b, RHS:, :]
    gram = lax.dot_general(left_ref[...], right_ref[...], NT, precision=HIGH, preferred_element_type=F32)
    coarse = gram[RHS:, :RITZ]
    coarse = 0.5 * (coarse + coarse.T)
    image = gram[RHS:, RITZ:]
    i, j = square_iota()
    packed = jnp.where(j >= i, coarse, image)
    diagonal = jnp.sum(jnp.where(i == j, image, 0.0), axis=0, keepdims=True)
    for b in range(NB // 2):
        out_ref[b, pl.ds(0, RHS), :] = gram[:RHS]
        out_ref[b, pl.ds(RHS, RITZ // 2), :] = jnp.concatenate([packed[: RITZ // 2], packed[RITZ // 2 :]], axis=1)
        out_ref[b, pl.ds(RHS + RITZ // 2, 1), :] = jnp.concatenate([diagonal, diagonal], axis=1)


def make_gram(vec, pts, place):
    return pl.pallas_call(
        gram_kernel,
        in_specs=[vmem(), vmem(), smem()],
        out_shape=shape(NB // 2, PACKED, BLK),
        scratch_shapes=[pltpu.VMEM((VEC, PTS), F32), pltpu.VMEM((2 * RITZ, PTS), F32)],
        compiler_params=limit(12),
        name="gram",
    )(vec, pts, place)


def inverse(matrix):
    i, j = square_iota()
    work = jnp.concatenate([matrix, jnp.where(i == j, 1.0, 0.0)], axis=1)
    row = lax.broadcasted_iota(jnp.int32, work.shape, 0)
    for k in range(0, RITZ, 2):
        col0 = jnp.broadcast_to(work[:, k : k + 1], work.shape)
        col1 = jnp.broadcast_to(work[:, k + 1 : k + 2], work.shape)
        a, b = col0[k : k + 1], col1[k : k + 1]
        c, d = col0[k + 1 : k + 2], col1[k + 1 : k + 2]
        top, low = work[k : k + 1], work[k + 1 : k + 2]
        scale = 1.0 / (a * d - b * c)
        new_top = (d * top - b * low) * scale
        new_low = (a * low - c * top) * scale
        work = work - (col0 * new_top + col1 * new_low)
        work = jnp.where(row == k, new_top, jnp.where(row == k + 1, new_low, work))
    return work[:, RITZ:]


def apply_kernel(hi_hbm, lo_hbm, vec_ref, pts_ref, place_ref, out_ref, rows_ref, hi_ref, lo_ref, sem):
    copies = []
    for step in range(PTS // READ):
        lanes = pl.ds(step * READ, READ)
        copies.append(
            (
                pltpu.make_async_copy(hi_hbm.at[:, lanes], hi_ref.at[:, lanes], sem.at[0, step]),
                pltpu.make_async_copy(lo_hbm.at[:, lanes], lo_ref.at[:, lanes], sem.at[1, step]),
            )
        )
        for copy in copies[-1]:
            copy.start()
    for b in range(NB):
        lanes = pl.ds(b * BLK, BLK)
        first = vec_ref[b, :RHS, :]
        ritz = pts_ref[arrived(b, place_ref), FEAT:, :]
        hi, lo = split2(jnp.concatenate([first, jnp.zeros_like(first), ritz, vec_ref[b, RHS:, :]], axis=0))
        rows_ref[pl.ds(0, HALF), lanes] = hi
        rows_ref[pl.ds(HALF, HALF), lanes] = lo
    for step in range(PTS // READ):
        lanes = pl.ds(step * READ, READ)
        for copy in copies[step]:
            copy.wait()
        both = jnp.dot(rows_ref[...], hi_ref[:, lanes], preferred_element_type=F32)
        more = jnp.dot(rows_ref[pl.ds(0, HALF), :], lo_ref[:, lanes], preferred_element_type=F32)
        out_ref[:, lanes] = both[:HALF] + both[HALF:] + more


def apply_tile(hi, lo, vec, pts, place):
    return pl.pallas_call(
        apply_kernel,
        in_specs=[hbm(), hbm(), vmem(), vmem(), smem()],
        out_shape=shape(HALF, PTS),
        scratch_shapes=[
            pltpu.VMEM((2 * HALF, PTS), BF16),
            pltpu.VMEM((PTS, PTS), BF16),
            pltpu.VMEM((PTS, PTS), BF16),
            pltpu.SemaphoreType.DMA((2, PTS // READ)),
        ],
        compiler_params=limit(32),
        cost_estimate=pl.CostEstimate(flops=8 * HALF * PTS * PTS, bytes_accessed=4 * PTS * PTS, transcendentals=0),
        name="apply_tile",
    )(in_hbm(hi), in_hbm(lo), vec, pts, place)


def solve_kernel(gram_ref, more_ref, image_ref, vec_ref, held_ref, place_ref, part_ref, own_ref):
    gram = gram_ref[...] + more_ref[...]
    projected = gram[:RHS, :RITZ]
    first = gram[:RHS, RITZ:]
    square = jnp.concatenate([gram[RHS : RHS + RITZ // 2, :RITZ], gram[RHS : RHS + RITZ // 2, RITZ:]], axis=0)
    turned = square.T
    i, j = square_iota()
    coarse = jnp.where(j >= i, square, turned)
    image = jnp.where(j < i, square, jnp.where(j > i, turned, gram[RHS + RITZ // 2 :, :RITZ]))
    solve = inverse(coarse)
    amounts = lax.dot_general(projected, solve, NT, precision=HIGH, preferred_element_type=F32)
    against = first - jnp.dot(amounts, image, precision=HIGH, preferred_element_type=F32)
    turns = lax.dot_general(against, solve, NT, precision=HIGH, preferred_element_type=F32)
    zero = jnp.zeros_like(turns)
    coef = jnp.concatenate([turns, amounts], axis=1)
    value = image_ref[pl.ds(0, RHS), :] - jnp.dot(
        coef, image_ref[pl.ds(2 * RHS, 2 * RITZ), :], precision=HIGH, preferred_element_type=F32
    )
    for at in range(NB):
        half = (at // (NB // 2) + place_ref[2]) % 2
        part_ref[half * (NB // 2) + at % (NB // 2)] = value[:, at * BLK : (at + 1) * BLK]
    mine = place_ref[0] * 4 + place_ref[1]
    basis = jnp.concatenate([held_ref[pl.ds(2 * RHS, RITZ), :], vec_ref[mine, RHS:, :]], axis=0)
    wanted = jnp.concatenate(
        [coef, jnp.concatenate([zero, amounts], axis=1), jnp.concatenate([-amounts, zero], axis=1)], axis=0
    )
    base = vec_ref[mine, :RHS, :]
    base = jnp.concatenate([base, base, held_ref[pl.ds(RHS, RHS), :]], axis=0)
    own_ref[...] = base - jnp.dot(wanted, basis, precision=HIGH, preferred_element_type=F32)


def solve(gram, more, image, vec, held, place):
    return pl.pallas_call(
        solve_kernel,
        in_specs=[vmem()] * 5 + [smem()],
        out_shape=[shape(NB, RHS, BLK), shape(3 * RHS, BLK)],
        compiler_params=limit(12),
        name="solve",
    )(gram, more, image, vec, held, place)


def stats_kernel(got_ref, own_ref, gain_ref, nugget_ref, applied_ref, out_ref):
    total = got_ref[0]
    for b in range(1, NB):
        total += got_ref[b]
    direction = own_ref[pl.ds(0, RHS), :]
    residual = own_ref[pl.ds(RHS, RHS), :]
    applied = gain_ref[0] * total + nugget_ref[0] * direction
    applied_ref[...] = applied
    sums = jnp.concatenate(
        [
            jnp.sum(direction * applied, axis=1, keepdims=True),
            jnp.sum(residual * residual, axis=1, keepdims=True),
        ],
        axis=0,
    )
    sums = jnp.broadcast_to(sums, (2 * RHS, BLK)).T[:RHS]
    for b in range(WORLD // RHS):
        out_ref[pl.ds(b * RHS, RHS), :] = sums


def make_stats(got, own, gain, nugget):
    return pl.pallas_call(
        stats_kernel,
        in_specs=[vmem(), vmem(), smem(), smem()],
        out_shape=[shape(RHS, BLK), shape(WORLD, 2 * RHS)],
        compiler_params=limit(8),
        name="stats",
    )(got, own, gain, nugget)


def finish_kernel(got_ref, own_ref, applied_ref, solution_ref, residual_ref):
    sums = jnp.sum(got_ref[...], axis=0, keepdims=True)
    i = lax.broadcasted_iota(jnp.int32, (2 * RHS, 2 * RHS), 0)
    j = lax.broadcasted_iota(jnp.int32, (2 * RHS, 2 * RHS), 1)
    sums = jnp.sum(jnp.where(i == j, sums, 0.0), axis=1, keepdims=True)
    size = sums[RHS:] / sums[:RHS]
    solution_ref[...] = own_ref[pl.ds(2 * RHS, RHS), :] + size * own_ref[pl.ds(0, RHS), :]
    residual_ref[...] = own_ref[pl.ds(RHS, RHS), :] - size * applied_ref[...]


def finish(got, own, applied):
    return pl.pallas_call(
        finish_kernel,
        out_shape=[shape(RHS, BLK), shape(RHS, BLK)],
        compiler_params=limit(8),
        name="finish",
    )(got, own, applied)


def exchange(pieces, axis):
    return lax.all_to_all(pieces, axis, split_axis=0, concat_axis=0, tiled=True)


def shifted(array, axis):
    size = lax.axis_size(axis)
    return [array] + [lax.ppermute(array, axis, [(i, (i + k) % size) for i in range(size)]) for k in range(1, size)]


def other_core(array):
    return lax.ppermute(array, CORE, [(0, 1), (1, 0)])


def local(points, inv_scales, amplitude, noise_var, targets, initial, ritz_basis):
    near, pts, held = spread(points, inv_scales[None, :], initial, ritz_basis, targets)
    place = jnp.stack([lax.axis_index("col_0"), lax.axis_index("row_0"), lax.axis_index(CORE)]).astype(jnp.int32)
    near = exchange(near, Z)
    pts = jnp.concatenate(shifted(jnp.concatenate(shifted(pts, "col_0"), axis=0), "row_0"), axis=0)
    far = other_core(near)
    hi, lo, part = make_tile(near, far, pts, place)

    vec = exchange(at_owner(exchange(part, XY), held, amplitude, noise_var), XY)
    gram = make_gram(vec, pts, place)
    vec, gram = lax.optimization_barrier((vec, gram))
    image = apply_tile(hi, lo, vec, pts, place)
    image, gram = lax.optimization_barrier((image, exchange(gram, Z)))
    gram = jnp.sum(gram, axis=0)
    part, own = solve(gram, other_core(gram), image, vec, held, place)
    applied, stats = make_stats(exchange(part, CZ), own, amplitude, noise_var)
    return tuple(finish(exchange(stats, EVERY), own, applied))


def solution(mesh):
    torus = Mesh(mesh.devices.reshape(4, 8, 4, 2), ("row_0", "row_1", "col_0", "col_1"))
    in_specs = (
        P(None, COL_ROW),
        P(),
        P(),
        P(),
        P(None, COL_ROW),
        P(None, COL_ROW),
        P(None, COL_ROW),
    )
    out_specs = (P(None, COL_ROW), P(None, COL_ROW))
    return jax.shard_map(local, mesh=torus, in_specs=in_specs, out_specs=out_specs, check_vma=False)
```

```python
import math

import jax
import jax.numpy as jnp
from jax import lax
from jax.experimental import pallas as pl
from jax.experimental.pallas import tpu as pltpu
from jax.sharding import Mesh
from jax.sharding import PartitionSpec as P


CORE = "col_1"
Z = "row_1"
XY = ("row_0", "col_0")
CZ = ("col_1", "row_1")
EVERY = ("col_0", "col_1", "row_0", "row_1")
COL_ROW = EVERY

FEAT = 16
RITZ = 64
RHS = 8
VEC = RHS + RITZ
BLK = 128
NB = 16
PTS = NB * BLK
STEP = 256
CHUNK = 256
READ = 256
HALF = 2 * RHS + 2 * RITZ
PACKED = RHS + RITZ // 2 + 1
WORLD = 256

HIGH = lax.Precision.HIGHEST
F32 = jnp.float32
BF16 = jnp.bfloat16
NT = (((1,), (1,)), ((), ()))


def split2(x):
    hi = x.astype(BF16)
    return hi, (x - hi.astype(F32)).astype(BF16)


def split3(x):
    hi = x.astype(BF16).astype(F32)
    rest = x - hi
    mid = rest.astype(BF16).astype(F32)
    return hi, mid, rest - mid


def features(x, swap):
    a, b, c = split3(x)
    n1, n2, n3 = split3(-0.5 * jnp.sum(x * x, axis=0, keepdims=True))
    row = lax.broadcasted_iota(jnp.int32, x.shape, 0)
    base = 3 if swap else 0
    norm = jnp.where(row == base, n1, jnp.where(row == base + 1, n2, jnp.where(row == base + 2, n3, 0.0)))
    one = 0 if swap else 3
    norm = jnp.where((row >= one) & (row < one + 3), 1.0, norm)
    zero = jnp.zeros_like(x)
    if swap:
        parts = [a, b, a, b, c, a, norm, zero]
    else:
        parts = [a, a, b, b, a, c, norm, zero]
    return jnp.concatenate(parts, axis=0)


def vmem():
    return pl.BlockSpec(memory_space=pltpu.VMEM)


def in_hbm(array):
    return pltpu.with_memory_space_constraint(array, pltpu.HBM)


def smem():
    return pl.BlockSpec(memory_space=pltpu.SMEM)


def shape(*dims):
    return jax.ShapeDtypeStruct(dims, F32)


def limit(mib):
    return pltpu.CompilerParams(vmem_limit_bytes=mib << 20)


def hbm():
    return pl.BlockSpec(memory_space=pltpu.HBM)


def spread_kernel(
    points_hbm,
    scale_hbm,
    initial_hbm,
    ritz_hbm,
    targets_hbm,
    near_ref,
    pts_ref,
    ritz_ref,
    held_ref,
    points_ref,
    scale_ref,
    sem,
):
    copies = [
        pltpu.make_async_copy(points_hbm, points_ref, sem.at[0]),
        pltpu.make_async_copy(scale_hbm, scale_ref, sem.at[1]),
        pltpu.make_async_copy(targets_hbm, held_ref.at[pl.ds(0, RHS)], sem.at[2]),
        pltpu.make_async_copy(initial_hbm, held_ref.at[pl.ds(RHS, RHS)], sem.at[3]),
        pltpu.make_async_copy(ritz_hbm, held_ref.at[pl.ds(2 * RHS, RITZ)], sem.at[4]),
    ]
    for copy in copies:
        copy.start()
    for copy in copies:
        copy.wait()
    scaled = points_ref[...] * (scale_ref[...].T * math.sqrt(math.log2(math.e)))
    for b in range(NB // 2):
        near_ref[b, pl.ds(0, FEAT), :] = scaled
        near_ref[b, pl.ds(FEAT, VEC), :] = held_ref[pl.ds(RHS, VEC), :]
    pts_ref[...] = scaled
    ritz_ref[...] = held_ref[pl.ds(2 * RHS, RITZ), :]


def spread(points, scales, initial, ritz, targets):
    return pl.pallas_call(
        spread_kernel,
        in_specs=[hbm()] * 5,
        out_specs=[vmem()] * 4,
        out_shape=[
            shape(NB // 2, FEAT + VEC, BLK),
            shape(FEAT, BLK),
            shape(RITZ, BLK),
            shape(RHS + VEC, BLK),
        ],
        scratch_shapes=[
            pltpu.VMEM((FEAT, BLK), F32),
            pltpu.VMEM((1, FEAT), F32),
            pltpu.SemaphoreType.DMA((5,)),
        ],
        compiler_params=limit(8),
        name="spread",
    )(*map(in_hbm, (points, scales, initial, ritz, targets)))


def tile_kernel(
    near_ref, far_ref, out_ref, hi_hbm, lo_hbm, part_ref, hi_ref, lo_ref, cols_ref, rows_ref, vec_ref, sem
):
    for b in range(NB):
        src = near_ref if b < NB // 2 else far_ref
        at = b % (NB // 2)
        lanes = pl.ds(b * BLK, BLK)
        cols_ref[:, lanes] = features(src[at, :FEAT, :], False).astype(BF16)
        tall = jnp.concatenate([src[at, FEAT:, :], jnp.zeros((BLK - VEC, BLK), F32)], axis=0).T
        hi, lo = split2(tall)
        vec_ref[lanes, pl.ds(0, BLK)] = hi
        vec_ref[lanes, pl.ds(BLK, BLK)] = lo
        rows_ref[lanes, :] = features(out_ref[b], True).T.astype(BF16)

    def copies(step):
        rows = pl.ds(step * STEP, STEP)
        return (
            pltpu.make_async_copy(hi_ref.at[rows], hi_hbm.at[rows], sem.at[0, step]),
            pltpu.make_async_copy(lo_ref.at[rows], lo_hbm.at[rows], sem.at[1, step]),
        )

    steps = PTS // STEP
    for step in range(steps + 1):
        rows, before = pl.ds(step * STEP, STEP), pl.ds((step - 1) * STEP, STEP)
        if step > 0:
            for copy in copies(step - 1):
                copy.start()
        total = jnp.zeros((STEP, 2 * BLK), F32)
        for c in range(PTS // CHUNK):
            lanes = pl.ds(c * CHUNK, CHUNK)
            if step > 0:
                vec = vec_ref[lanes, :]
                total += jnp.dot(hi_ref[before, lanes], vec, preferred_element_type=F32)
                total += jnp.dot(lo_ref[before, lanes], vec, preferred_element_type=F32)
            if step < steps:
                power = jnp.dot(rows_ref[rows, :], cols_ref[:, lanes], preferred_element_type=F32)
                hi, lo = split2(jnp.exp2(jnp.minimum(power, 0.0)))
                hi_ref[rows, lanes] = hi
                lo_ref[rows, lanes] = lo
        if step > 0:
            both = total[:, :BLK] + total[:, BLK:]
            for h in range(STEP // BLK):
                part_ref[(step - 1) * (STEP // BLK) + h] = both[h * BLK : (h + 1) * BLK].T[:VEC]
    for step in range(steps):
        for copy in copies(step):
            copy.wait()


def make_tile(near, far, out):
    return pl.pallas_call(
        tile_kernel,
        in_specs=[vmem(), vmem(), vmem()],
        out_specs=[hbm(), hbm(), vmem()],
        out_shape=[
            pltpu.HBM((PTS, PTS), BF16),
            pltpu.HBM((PTS, PTS), BF16),
            shape(NB, VEC, BLK),
        ],
        scratch_shapes=[
            pltpu.VMEM((PTS, PTS), BF16),
            pltpu.VMEM((PTS, PTS), BF16),
            pltpu.VMEM((BLK, PTS), BF16),
            pltpu.VMEM((PTS, BLK), BF16),
            pltpu.VMEM((PTS, 2 * BLK), BF16),
            pltpu.SemaphoreType.DMA((2, PTS // STEP)),
        ],
        compiler_params=limit(40),
        name="kernel_tile",
    )(near, far, out)


def owner_kernel(got_ref, held_ref, gain_ref, nugget_ref, out_ref):
    total = got_ref[0]
    for b in range(1, NB):
        total += got_ref[b]
    applied = gain_ref[0] * total + nugget_ref[0] * held_ref[pl.ds(RHS, VEC), :]
    first = held_ref[pl.ds(0, RHS), :] - applied[:RHS]
    image = applied[RHS:]
    for b in range(NB):
        out_ref[b, pl.ds(0, RHS), :] = first
        out_ref[b, pl.ds(RHS, RITZ), :] = image


def at_owner(got, held, gain, nugget):
    return pl.pallas_call(
        owner_kernel,
        in_specs=[vmem(), vmem(), smem(), smem()],
        out_shape=shape(NB, VEC, BLK),
        compiler_params=limit(8),
        name="at_owner",
    )(got, held, gain, nugget)


def square_iota():
    return lax.broadcasted_iota(jnp.int32, (RITZ, RITZ), 0), lax.broadcasted_iota(jnp.int32, (RITZ, RITZ), 1)


def gram_kernel(vec_ref, ritz_ref, out_ref, left_ref, right_ref):
    for b in range(NB):
        lanes = pl.ds(b * BLK, BLK)
        left_ref[:, lanes] = vec_ref[b]
        right_ref[pl.ds(0, RITZ), lanes] = ritz_ref[b]
        right_ref[pl.ds(RITZ, RITZ), lanes] = vec_ref[b, RHS:, :]
    gram = lax.dot_general(left_ref[...], right_ref[...], NT, precision=HIGH, preferred_element_type=F32)
    coarse = gram[RHS:, :RITZ]
    coarse = 0.5 * (coarse + coarse.T)
    image = gram[RHS:, RITZ:]
    i, j = square_iota()
    packed = jnp.where(j >= i, coarse, image)
    diagonal = jnp.sum(jnp.where(i == j, image, 0.0), axis=0, keepdims=True)
    for b in range(NB // 2):
        out_ref[b, pl.ds(0, RHS), :] = gram[:RHS]
        out_ref[b, pl.ds(RHS, RITZ // 2), :] = jnp.concatenate([packed[: RITZ // 2], packed[RITZ // 2 :]], axis=1)
        out_ref[b, pl.ds(RHS + RITZ // 2, 1), :] = jnp.concatenate([diagonal, diagonal], axis=1)


def make_gram(vec, ritz):
    return pl.pallas_call(
        gram_kernel,
        out_shape=shape(NB // 2, PACKED, BLK),
        scratch_shapes=[pltpu.VMEM((VEC, PTS), F32), pltpu.VMEM((2 * RITZ, PTS), F32)],
        compiler_params=limit(12),
        name="gram",
    )(vec, ritz)


def inverse(matrix):
    full = (8, 2 * RITZ)
    i, j = square_iota()
    work = jnp.concatenate([matrix, jnp.where(i == j, 1.0, 0.0)], axis=1)
    work = [work[b : b + 8] for b in range(0, RITZ, 8)]
    sub = lax.broadcasted_iota(jnp.int32, full, 0)

    def pair(a, b, c, d, top, low):
        scale = 1.0 / (a * d - b * c)
        return (d * top - b * low) * scale, (a * low - c * top) * scale

    for k in range(0, RITZ, 4):
        at, row = k // 8, k % 8
        cols = [[jnp.broadcast_to(w[:, k + q : k + q + 1], full) for w in work] for q in range(4)]
        rows = [jnp.broadcast_to(work[at][row + q : row + q + 1], full) for q in range(4)]
        e = [[jnp.broadcast_to(cols[r][at][row + q : row + q + 1], full) for r in range(4)] for q in range(4)]
        r0, r1 = pair(e[0][0], e[0][1], e[1][0], e[1][1], rows[0], rows[1])
        f = [pair(e[0][0], e[0][1], e[1][0], e[1][1], e[0][r], e[1][r]) for r in (2, 3)]
        rows[2] = rows[2] - e[2][0] * r0 - e[2][1] * r1
        rows[3] = rows[3] - e[3][0] * r0 - e[3][1] * r1
        g = [[e[q][r] - e[q][0] * f[r - 2][0] - e[q][1] * f[r - 2][1] for r in (2, 3)] for q in (2, 3)]
        r2, r3 = pair(g[0][0], g[0][1], g[1][0], g[1][1], rows[2], rows[3])
        r0 = r0 - f[0][0] * r2 - f[1][0] * r3
        r1 = r1 - f[0][1] * r2 - f[1][1] * r3
        final = (r0, r1, r2, r3)
        work = [
            w - ((cols[0][b] * r0 + cols[1][b] * r1) + (cols[2][b] * r2 + cols[3][b] * r3))
            for b, w in enumerate(work)
        ]
        for q in range(4):
            work[at] = jnp.where(sub == row + q, final[q], work[at])
    return jnp.concatenate(work, axis=0)[:, RITZ:]


def apply_kernel(hi_hbm, lo_hbm, vec_ref, ritz_ref, out_ref, split_ref, rows_ref, hi_ref, lo_ref, sem):
    copies = []
    for step in range(PTS // READ):
        lanes = pl.ds(step * READ, READ)
        copies.append(
            (
                pltpu.make_async_copy(hi_hbm.at[:, lanes], hi_ref.at[:, lanes], sem.at[0, step]),
                pltpu.make_async_copy(lo_hbm.at[:, lanes], lo_ref.at[:, lanes], sem.at[1, step]),
            )
        )
        for copy in copies[-1]:
            copy.start()
    for b in range(NB):
        lanes = pl.ds(b * BLK, BLK)
        first = vec_ref[b, :RHS, :]
        hi, lo = split2(jnp.concatenate([first, jnp.zeros_like(first), ritz_ref[b], vec_ref[b, RHS:, :]], axis=0))
        rows_ref[pl.ds(0, HALF), lanes] = hi
        rows_ref[pl.ds(HALF, HALF), lanes] = lo
    for step in range(PTS // READ):
        lanes = pl.ds(step * READ, READ)
        for copy in copies[step]:
            copy.wait()
        both = jnp.dot(rows_ref[...], hi_ref[:, lanes], preferred_element_type=F32)
        more = jnp.dot(rows_ref[pl.ds(0, HALF), :], lo_ref[:, lanes], preferred_element_type=F32)
        value = both[:HALF] + both[HALF:] + more
        out_ref[:, lanes] = value[:RHS]
        for part, piece in enumerate(split3(value[2 * RHS :])):
            split_ref[pl.ds(part * 2 * RITZ, 2 * RITZ), lanes] = piece.astype(BF16)


def apply_tile(hi, lo, vec, ritz):
    return pl.pallas_call(
        apply_kernel,
        in_specs=[hbm(), hbm(), vmem(), vmem()],
        out_shape=[shape(RHS, PTS), jax.ShapeDtypeStruct((6 * RITZ, PTS), BF16)],
        scratch_shapes=[
            pltpu.VMEM((2 * HALF, PTS), BF16),
            pltpu.VMEM((PTS, PTS), BF16),
            pltpu.VMEM((PTS, PTS), BF16),
            pltpu.SemaphoreType.DMA((2, PTS // READ)),
        ],
        compiler_params=limit(32),
        cost_estimate=pl.CostEstimate(flops=8 * HALF * PTS * PTS, bytes_accessed=4 * PTS * PTS, transcendentals=0),
        name="apply_tile",
    )(in_hbm(hi), in_hbm(lo), vec, ritz)


def solve_kernel(gram_ref, more_ref, image_ref, split_ref, vec_ref, held_ref, place_ref, part_ref, own_ref):
    gram = gram_ref[...] + more_ref[...]
    projected = gram[:RHS, :RITZ]
    first = gram[:RHS, RITZ:]
    square = jnp.concatenate([gram[RHS : RHS + RITZ // 2, :RITZ], gram[RHS : RHS + RITZ // 2, RITZ:]], axis=0)
    turned = square.T
    i, j = square_iota()
    coarse = jnp.where(j >= i, square, turned)
    image = jnp.where(j < i, square, jnp.where(j > i, turned, gram[RHS + RITZ // 2 :, :RITZ]))
    solve = inverse(coarse)
    amounts = lax.dot_general(projected, solve, NT, precision=HIGH, preferred_element_type=F32)
    against = first - jnp.dot(amounts, image, precision=HIGH, preferred_element_type=F32)
    turns = lax.dot_general(against, solve, NT, precision=HIGH, preferred_element_type=F32)
    zero = jnp.zeros_like(turns)
    coef = jnp.concatenate([turns, amounts], axis=1)
    pieces = split3(coef)
    value = image_ref[...]
    for part, rows in ((2, 1), (1, 2), (0, 3)):
        left = jnp.concatenate(pieces[:rows], axis=0).astype(BF16)
        more = jnp.dot(left, split_ref[pl.ds(part * 2 * RITZ, 2 * RITZ), :], preferred_element_type=F32)
        for q in range(rows):
            value -= more[q * RHS : (q + 1) * RHS]
    for at in range(NB):
        half = (at // (NB // 2) + place_ref[2]) % 2
        part_ref[half * (NB // 2) + at % (NB // 2)] = value[:, at * BLK : (at + 1) * BLK]
    mine = place_ref[1] * 4 + place_ref[0]
    basis = jnp.concatenate([held_ref[pl.ds(2 * RHS, RITZ), :], vec_ref[mine, RHS:, :]], axis=0)
    wanted = jnp.concatenate(
        [coef, jnp.concatenate([zero, amounts], axis=1), jnp.concatenate([-amounts, zero], axis=1)], axis=0
    )
    base = vec_ref[mine, :RHS, :]
    base = jnp.concatenate([base, base, held_ref[pl.ds(RHS, RHS), :]], axis=0)
    own_ref[...] = base - jnp.dot(wanted, basis, precision=HIGH, preferred_element_type=F32)


def solve(gram, more, image, split, vec, held, place):
    return pl.pallas_call(
        solve_kernel,
        in_specs=[vmem()] * 6 + [smem()],
        out_shape=[shape(NB, RHS, BLK), shape(3 * RHS, BLK)],
        compiler_params=limit(12),
        name="solve",
    )(gram, more, image, split, vec, held, place)


def stats_kernel(got_ref, own_ref, gain_ref, nugget_ref, applied_ref, out_ref):
    total = got_ref[0]
    for b in range(1, NB):
        total += got_ref[b]
    direction = own_ref[pl.ds(0, RHS), :]
    residual = own_ref[pl.ds(RHS, RHS), :]
    applied = gain_ref[0] * total + nugget_ref[0] * direction
    applied_ref[...] = applied
    sums = jnp.concatenate(
        [
            jnp.sum(direction * applied, axis=1, keepdims=True),
            jnp.sum(residual * residual, axis=1, keepdims=True),
        ],
        axis=0,
    )
    sums = jnp.broadcast_to(sums, (2 * RHS, BLK)).T[:RHS]
    for b in range(WORLD // RHS):
        out_ref[pl.ds(b * RHS, RHS), :] = sums


def make_stats(got, own, gain, nugget):
    return pl.pallas_call(
        stats_kernel,
        in_specs=[vmem(), vmem(), smem(), smem()],
        out_shape=[shape(RHS, BLK), shape(WORLD, 2 * RHS)],
        compiler_params=limit(8),
        name="stats",
    )(got, own, gain, nugget)


def finish_kernel(got_ref, own_ref, applied_ref, solution_ref, residual_ref):
    sums = jnp.sum(got_ref[...], axis=0, keepdims=True)
    i = lax.broadcasted_iota(jnp.int32, (2 * RHS, 2 * RHS), 0)
    j = lax.broadcasted_iota(jnp.int32, (2 * RHS, 2 * RHS), 1)
    sums = jnp.sum(jnp.where(i == j, sums, 0.0), axis=1, keepdims=True)
    size = sums[RHS:] / sums[:RHS]
    solution_ref[...] = own_ref[pl.ds(2 * RHS, RHS), :] + size * own_ref[pl.ds(0, RHS), :]
    residual_ref[...] = own_ref[pl.ds(RHS, RHS), :] - size * applied_ref[...]


def finish(got, own, applied):
    return pl.pallas_call(
        finish_kernel,
        out_shape=[shape(RHS, BLK), shape(RHS, BLK)],
        compiler_params=limit(8),
        name="finish",
    )(got, own, applied)


def exchange(pieces, axis):
    return lax.all_to_all(pieces, axis, split_axis=0, concat_axis=0, tiled=True)


def all_around(array, axis):
    size, here = lax.axis_size(axis), lax.axis_index(axis)
    whole = jnp.zeros((size, *array.shape), array.dtype)
    for k in range(size):
        block = array if k == 0 else lax.ppermute(array, axis, [(i, (i + k) % size) for i in range(size)])
        whole = lax.dynamic_update_index_in_dim(whole, block, (here - k + size) % size, 0)
    return whole


def other_core(array):
    return lax.ppermute(array, CORE, [(0, 1), (1, 0)])


def local(points, inv_scales, amplitude, noise_var, targets, initial, ritz_basis):
    near, pts, ritz, held = spread(points, inv_scales[None, :], initial, ritz_basis, targets)
    place = jnp.stack([lax.axis_index("col_0"), lax.axis_index("row_0"), lax.axis_index(CORE)]).astype(jnp.int32)
    near = exchange(near, Z)
    pts = all_around(pts, "col_0")
    pts = all_around(pts, "row_0").reshape(NB, FEAT, BLK)
    far = other_core(near)
    hi, lo, part = make_tile(near, far, pts)

    part, ritz = lax.optimization_barrier((part, ritz))
    part = exchange(part, XY)
    ritz = all_around(ritz, "col_0")
    own = at_owner(part, held, amplitude, noise_var)
    own, ritz = lax.optimization_barrier((own, ritz))
    vec = exchange(own, XY)
    ritz = all_around(ritz, "row_0").reshape(NB, RITZ, BLK)
    gram = make_gram(vec, ritz)
    vec, gram = lax.optimization_barrier((vec, gram))
    image, split = apply_tile(hi, lo, vec, ritz)
    image, split, gram = lax.optimization_barrier((image, split, exchange(gram, Z)))
    gram = jnp.sum(gram, axis=0)
    part, own = solve(gram, other_core(gram), image, split, vec, held, place)
    applied, stats = make_stats(exchange(part, CZ), own, amplitude, noise_var)
    return tuple(finish(exchange(stats, EVERY), own, applied))


def solution(mesh):
    torus = Mesh(mesh.devices.reshape(4, 8, 4, 2), ("row_0", "row_1", "col_0", "col_1"))
    in_specs = (
        P(None, COL_ROW),
        P(),
        P(),
        P(),
        P(None, COL_ROW),
        P(None, COL_ROW),
        P(None, COL_ROW),
    )
    out_specs = (P(None, COL_ROW), P(None, COL_ROW))
    return jax.shard_map(local, mesh=torus, in_specs=in_specs, out_specs=out_specs, check_vma=False)
```

```python
import math

import jax
import jax.numpy as jnp
from jax import lax
from jax.experimental import pallas as pl
from jax.experimental.pallas import tpu as pltpu
from jax.sharding import Mesh
from jax.sharding import PartitionSpec as P


CORE = "col_1"
Z = "row_1"
XY = ("row_0", "col_0")
CZ = ("col_1", "row_1")
EVERY = ("col_0", "col_1", "row_0", "row_1")
COL_ROW = EVERY

FEAT = 16
RITZ = 64
RHS = 8
VEC = RHS + RITZ
BLK = 128
NB = 16
PTS = NB * BLK
STEP = 256
CHUNK = 256
READ = 512
HALF = 2 * RHS + 2 * RITZ
PACKED = RHS + RITZ // 2 + 1
WORLD = 256

HIGH = lax.Precision.HIGHEST
F32 = jnp.float32
BF16 = jnp.bfloat16
NT = (((1,), (1,)), ((), ()))


def split2(x):
    hi = x.astype(BF16)
    return hi, (x - hi.astype(F32)).astype(BF16)


def split3(x):
    hi = x.astype(BF16).astype(F32)
    rest = x - hi
    mid = rest.astype(BF16).astype(F32)
    return hi, mid, rest - mid


def features(x, swap):
    a, b, c = split3(x)
    n1, n2, n3 = split3(-0.5 * jnp.sum(x * x, axis=0, keepdims=True))
    row = lax.broadcasted_iota(jnp.int32, x.shape, 0)
    base = 3 if swap else 0
    norm = jnp.where(row == base, n1, jnp.where(row == base + 1, n2, jnp.where(row == base + 2, n3, 0.0)))
    one = 0 if swap else 3
    norm = jnp.where((row >= one) & (row < one + 3), 1.0, norm)
    zero = jnp.zeros_like(x)
    if swap:
        parts = [a, b, a, b, c, a, norm, zero]
    else:
        parts = [a, a, b, b, a, c, norm, zero]
    return jnp.concatenate(parts, axis=0)


def vmem():
    return pl.BlockSpec(memory_space=pltpu.VMEM)


def in_hbm(array):
    return pltpu.with_memory_space_constraint(array, pltpu.HBM)


def shape(*dims):
    return jax.ShapeDtypeStruct(dims, F32)


def limit(mib):
    return pltpu.CompilerParams(vmem_limit_bytes=mib << 20)


def hbm():
    return pl.BlockSpec(memory_space=pltpu.HBM)


def spread_kernel(
    points_hbm,
    scale_hbm,
    initial_hbm,
    ritz_hbm,
    targets_hbm,
    near_ref,
    pts_ref,
    held_ref,
    points_ref,
    scale_ref,
    sem,
):
    copies = [
        pltpu.make_async_copy(points_hbm, points_ref, sem.at[0]),
        pltpu.make_async_copy(scale_hbm, scale_ref, sem.at[1]),
        pltpu.make_async_copy(targets_hbm, held_ref.at[pl.ds(0, RHS)], sem.at[2]),
        pltpu.make_async_copy(initial_hbm, held_ref.at[pl.ds(RHS, RHS)], sem.at[3]),
        pltpu.make_async_copy(ritz_hbm, held_ref.at[pl.ds(2 * RHS, RITZ)], sem.at[4]),
    ]
    for copy in copies:
        copy.start()
    for copy in copies:
        copy.wait()
    scaled = points_ref[...] * (scale_ref[...].T * math.sqrt(math.log2(math.e)))
    for b in range(NB // 2):
        near_ref[b, pl.ds(0, FEAT), :] = scaled
        near_ref[b, pl.ds(FEAT, VEC), :] = held_ref[pl.ds(RHS, VEC), :]
    pts_ref[pl.ds(0, FEAT), :] = scaled
    pts_ref[pl.ds(FEAT, RITZ), :] = held_ref[pl.ds(2 * RHS, RITZ), :]


def spread(points, scales, initial, ritz, targets):
    return pl.pallas_call(
        spread_kernel,
        in_specs=[hbm()] * 5,
        out_specs=[vmem()] * 3,
        out_shape=[
            shape(NB // 2, FEAT + VEC, BLK),
            shape(FEAT + RITZ, BLK),
            shape(RHS + VEC, BLK),
        ],
        scratch_shapes=[
            pltpu.VMEM((FEAT, BLK), F32),
            pltpu.VMEM((1, FEAT), F32),
            pltpu.SemaphoreType.DMA((5,)),
        ],
        compiler_params=limit(8),
        name="spread",
    )(*map(in_hbm, (points, scales, initial, ritz, targets)))


def tile_kernel(
    near_ref, far_ref, out_ref, hi_hbm, lo_hbm, part_ref, hi_ref, lo_ref, cols_ref, rows_ref, vec_ref, sem
):
    for b in range(NB):
        src = near_ref if b < NB // 2 else far_ref
        at = b % (NB // 2)
        lanes = pl.ds(b * BLK, BLK)
        cols_ref[:, lanes] = features(src[at, :FEAT, :], False).astype(BF16)
        tall = jnp.concatenate([src[at, FEAT:, :], jnp.zeros((BLK - VEC, BLK), F32)], axis=0).T
        hi, lo = split2(tall)
        vec_ref[lanes, pl.ds(0, BLK)] = hi
        vec_ref[lanes, pl.ds(BLK, BLK)] = lo
        rows_ref[lanes, :] = features(out_ref[b, :FEAT, :], True).T.astype(BF16)

    def copies(step):
        rows = pl.ds(step * STEP, STEP)
        return (
            pltpu.make_async_copy(hi_ref.at[rows], hi_hbm.at[rows], sem.at[0, step]),
            pltpu.make_async_copy(lo_ref.at[rows], lo_hbm.at[rows], sem.at[1, step]),
        )

    steps = PTS // STEP
    for step in range(steps + 1):
        rows, before = pl.ds(step * STEP, STEP), pl.ds((step - 1) * STEP, STEP)
        if step > 0:
            for copy in copies(step - 1):
                copy.start()
        total = jnp.zeros((STEP, 2 * BLK), F32)
        for c in range(PTS // CHUNK):
            lanes = pl.ds(c * CHUNK, CHUNK)
            if step > 0:
                vec = vec_ref[lanes, :]
                total += jnp.dot(hi_ref[before, lanes], vec, preferred_element_type=F32)
                total += jnp.dot(lo_ref[before, lanes], vec, preferred_element_type=F32)
            if step < steps:
                power = jnp.dot(rows_ref[rows, :], cols_ref[:, lanes], preferred_element_type=F32)
                hi, lo = split2(jnp.exp2(jnp.minimum(power, 0.0)))
                hi_ref[rows, lanes] = hi
                lo_ref[rows, lanes] = lo
        if step > 0:
            both = total[:, :BLK] + total[:, BLK:]
            for h in range(STEP // BLK):
                part_ref[(step - 1) * (STEP // BLK) + h] = both[h * BLK : (h + 1) * BLK].T[:VEC]
    for step in range(steps):
        for copy in copies(step):
            copy.wait()


def make_tile(near, far, out):
    return pl.pallas_call(
        tile_kernel,
        in_specs=[vmem(), vmem(), vmem()],
        out_specs=[hbm(), hbm(), vmem()],
        out_shape=[
            pltpu.HBM((PTS, PTS), BF16),
            pltpu.HBM((PTS, PTS), BF16),
            shape(NB, VEC, BLK),
        ],
        scratch_shapes=[
            pltpu.VMEM((PTS, PTS), BF16),
            pltpu.VMEM((PTS, PTS), BF16),
            pltpu.VMEM((BLK, PTS), BF16),
            pltpu.VMEM((PTS, BLK), BF16),
            pltpu.VMEM((PTS, 2 * BLK), BF16),
            pltpu.SemaphoreType.DMA((2, PTS // STEP)),
        ],
        compiler_params=limit(40),
        name="kernel_tile",
    )(near, far, out)


def owner_kernel(got_ref, held_ref, scalars_ref, out_ref):
    total = got_ref[0]
    for b in range(1, NB):
        total += got_ref[b]
    gain, nugget = scalars_ref[pl.ds(0, 1), :], scalars_ref[pl.ds(1, 1), :]
    applied = gain * total + nugget * held_ref[pl.ds(RHS, VEC), :]
    first = held_ref[pl.ds(0, RHS), :] - applied[:RHS]
    image = applied[RHS:]
    for b in range(NB):
        out_ref[b, pl.ds(0, RHS), :] = first
        out_ref[b, pl.ds(RHS, RITZ), :] = image


def at_owner(got, held, scalars):
    return pl.pallas_call(
        owner_kernel,
        out_shape=shape(NB, VEC, BLK),
        compiler_params=limit(8),
        name="at_owner",
    )(got, held, scalars)


def square_iota():
    return lax.broadcasted_iota(jnp.int32, (RITZ, RITZ), 0), lax.broadcasted_iota(jnp.int32, (RITZ, RITZ), 1)


def gram_kernel(vec_ref, pts_ref, out_ref, left_ref, right_ref):
    for b in range(NB):
        lanes = pl.ds(b * BLK, BLK)
        left_ref[:, lanes] = vec_ref[b]
        right_ref[pl.ds(0, RITZ), lanes] = pts_ref[b, FEAT:, :]
        right_ref[pl.ds(RITZ, RITZ), lanes] = vec_ref[b, RHS:, :]
    gram = lax.dot_general(left_ref[...], right_ref[...], NT, precision=HIGH, preferred_element_type=F32)
    coarse = gram[RHS:, :RITZ]
    coarse = 0.5 * (coarse + coarse.T)
    image = gram[RHS:, RITZ:]
    i, j = square_iota()
    packed = jnp.where(j >= i, coarse, image)
    diagonal = jnp.sum(jnp.where(i == j, image, 0.0), axis=0, keepdims=True)
    for b in range(NB // 2):
        out_ref[b, pl.ds(0, RHS), :] = gram[:RHS]
        out_ref[b, pl.ds(RHS, RITZ // 2), :] = jnp.concatenate([packed[: RITZ // 2], packed[RITZ // 2 :]], axis=1)
        out_ref[b, pl.ds(RHS + RITZ // 2, 1), :] = jnp.concatenate([diagonal, diagonal], axis=1)


def make_gram(vec, pts):
    return pl.pallas_call(
        gram_kernel,
        out_shape=shape(NB // 2, PACKED, BLK),
        scratch_shapes=[pltpu.VMEM((VEC, PTS), F32), pltpu.VMEM((2 * RITZ, PTS), F32)],
        compiler_params=limit(12),
        name="gram",
    )(vec, pts)


def inverse(matrix):
    full = (8, 2 * RITZ)
    i, j = square_iota()
    work = jnp.concatenate([matrix, jnp.where(i == j, 1.0, 0.0)], axis=1)
    work = [work[b : b + 8] for b in range(0, RITZ, 8)]
    sub = lax.broadcasted_iota(jnp.int32, full, 0)

    def pair(a, b, c, d, top, low):
        scale = 1.0 / (a * d - b * c)
        return (d * top - b * low) * scale, (a * low - c * top) * scale

    for k in range(0, RITZ, 4):
        at, row = k // 8, k % 8
        cols = [[jnp.broadcast_to(w[:, k + q : k + q + 1], full) for w in work] for q in range(4)]
        rows = [jnp.broadcast_to(work[at][row + q : row + q + 1], full) for q in range(4)]
        e = [[jnp.broadcast_to(cols[r][at][row + q : row + q + 1], full) for r in range(4)] for q in range(4)]
        r0, r1 = pair(e[0][0], e[0][1], e[1][0], e[1][1], rows[0], rows[1])
        f = [pair(e[0][0], e[0][1], e[1][0], e[1][1], e[0][r], e[1][r]) for r in (2, 3)]
        rows[2] = rows[2] - e[2][0] * r0 - e[2][1] * r1
        rows[3] = rows[3] - e[3][0] * r0 - e[3][1] * r1
        g = [[e[q][r] - e[q][0] * f[r - 2][0] - e[q][1] * f[r - 2][1] for r in (2, 3)] for q in (2, 3)]
        r2, r3 = pair(g[0][0], g[0][1], g[1][0], g[1][1], rows[2], rows[3])
        r0 = r0 - f[0][0] * r2 - f[1][0] * r3
        r1 = r1 - f[0][1] * r2 - f[1][1] * r3
        final = (r0, r1, r2, r3)
        work = [
            w - ((cols[0][b] * r0 + cols[1][b] * r1) + (cols[2][b] * r2 + cols[3][b] * r3))
            for b, w in enumerate(work)
        ]
        for q in range(4):
            work[at] = jnp.where(sub == row + q, final[q], work[at])
    return jnp.concatenate(work, axis=0)[:, RITZ:]


def apply_kernel(hi_hbm, lo_hbm, vec_ref, pts_ref, out_ref, rows_ref, hi_ref, lo_ref, sem):
    copies = []
    for step in range(PTS // READ):
        lanes = pl.ds(step * READ, READ)
        copies.append(
            (
                pltpu.make_async_copy(hi_hbm.at[:, lanes], hi_ref.at[:, lanes], sem.at[0, step]),
                pltpu.make_async_copy(lo_hbm.at[:, lanes], lo_ref.at[:, lanes], sem.at[1, step]),
            )
        )
        for copy in copies[-1]:
            copy.start()
    for b in range(NB):
        lanes = pl.ds(b * BLK, BLK)
        first = vec_ref[b, :RHS, :]
        hi, lo = split2(
            jnp.concatenate([first, jnp.zeros_like(first), pts_ref[b, FEAT:, :], vec_ref[b, RHS:, :]], axis=0)
        )
        rows_ref[pl.ds(0, HALF), lanes] = hi
        rows_ref[pl.ds(HALF, HALF), lanes] = lo
    for step in range(PTS // READ):
        lanes = pl.ds(step * READ, READ)
        for copy in copies[step]:
            copy.wait()
        both = jnp.dot(rows_ref[...], hi_ref[:, lanes], preferred_element_type=F32)
        more = jnp.dot(rows_ref[pl.ds(0, HALF), :], lo_ref[:, lanes], preferred_element_type=F32)
        out_ref[:, lanes] = both[:HALF] + both[HALF:] + more


def apply_tile(hi, lo, vec, pts):
    return pl.pallas_call(
        apply_kernel,
        in_specs=[hbm(), hbm(), vmem(), vmem()],
        out_shape=shape(HALF, PTS),
        scratch_shapes=[
            pltpu.VMEM((2 * HALF, PTS), BF16),
            pltpu.VMEM((PTS, PTS), BF16),
            pltpu.VMEM((PTS, PTS), BF16),
            pltpu.SemaphoreType.DMA((2, PTS // READ)),
        ],
        compiler_params=limit(32),
        cost_estimate=pl.CostEstimate(flops=8 * HALF * PTS * PTS, bytes_accessed=4 * PTS * PTS, transcendentals=0),
        name="apply_tile",
    )(in_hbm(hi), in_hbm(lo), vec, pts)


def solve_kernel(gram_ref, more_ref, image_ref, vec_ref, held_ref, part_ref, own_ref):
    gram = gram_ref[...] + more_ref[...]
    projected = gram[:RHS, :RITZ]
    first = gram[:RHS, RITZ:]
    square = jnp.concatenate([gram[RHS : RHS + RITZ // 2, :RITZ], gram[RHS : RHS + RITZ // 2, RITZ:]], axis=0)
    turned = square.T
    i, j = square_iota()
    coarse = jnp.where(j >= i, square, turned)
    image = jnp.where(j < i, square, jnp.where(j > i, turned, gram[RHS + RITZ // 2 :, :RITZ]))
    solve = inverse(coarse)
    amounts = lax.dot_general(projected, solve, NT, precision=HIGH, preferred_element_type=F32)
    against = first - jnp.dot(amounts, image, precision=HIGH, preferred_element_type=F32)
    turns = lax.dot_general(against, solve, NT, precision=HIGH, preferred_element_type=F32)
    zero = jnp.zeros_like(turns)
    coef = jnp.concatenate([turns, amounts], axis=1)
    value = image_ref[pl.ds(0, RHS), :] - jnp.dot(
        coef, image_ref[pl.ds(2 * RHS, 2 * RITZ), :], precision=HIGH, preferred_element_type=F32
    )
    core = lax.axis_index(CORE)
    for at in range(NB):
        half = (at // (NB // 2) + core) % 2
        part_ref[half * (NB // 2) + at % (NB // 2)] = value[:, at * BLK : (at + 1) * BLK]
    mine = lax.axis_index("row_0") * 4 + lax.axis_index("col_0")
    basis = jnp.concatenate([held_ref[pl.ds(2 * RHS, RITZ), :], vec_ref[mine, RHS:, :]], axis=0)
    wanted = jnp.concatenate(
        [coef, jnp.concatenate([zero, amounts], axis=1), jnp.concatenate([-amounts, zero], axis=1)], axis=0
    )
    base = vec_ref[mine, :RHS, :]
    base = jnp.concatenate([base, base, held_ref[pl.ds(RHS, RHS), :]], axis=0)
    own_ref[...] = base - jnp.dot(wanted, basis, precision=HIGH, preferred_element_type=F32)


def solve(gram, more, image, vec, held):
    return pl.pallas_call(
        solve_kernel,
        out_shape=[shape(NB, RHS, BLK), shape(3 * RHS, BLK)],
        compiler_params=limit(12),
        name="solve",
    )(gram, more, image, vec, held)


def stats_kernel(got_ref, own_ref, scalars_ref, applied_ref, out_ref):
    total = got_ref[0]
    for b in range(1, NB):
        total += got_ref[b]
    direction = own_ref[pl.ds(0, RHS), :]
    residual = own_ref[pl.ds(RHS, RHS), :]
    applied = scalars_ref[pl.ds(0, 1), :] * total + scalars_ref[pl.ds(1, 1), :] * direction
    applied_ref[...] = applied
    sums = jnp.concatenate(
        [
            jnp.sum(direction * applied, axis=1, keepdims=True),
            jnp.sum(residual * residual, axis=1, keepdims=True),
        ],
        axis=0,
    )
    sums = jnp.broadcast_to(sums, (2 * RHS, BLK)).T[:RHS]
    for b in range(WORLD // RHS):
        out_ref[pl.ds(b * RHS, RHS), :] = sums


def make_stats(got, own, scalars):
    return pl.pallas_call(
        stats_kernel,
        out_shape=[shape(RHS, BLK), shape(WORLD, 2 * RHS)],
        compiler_params=limit(8),
        name="stats",
    )(got, own, scalars)


def finish_kernel(got_ref, own_ref, applied_ref, solution_ref, residual_ref):
    sums = jnp.sum(got_ref[...], axis=0, keepdims=True)
    i = lax.broadcasted_iota(jnp.int32, (2 * RHS, 2 * RHS), 0)
    j = lax.broadcasted_iota(jnp.int32, (2 * RHS, 2 * RHS), 1)
    sums = jnp.sum(jnp.where(i == j, sums, 0.0), axis=1, keepdims=True)
    size = sums[RHS:] / sums[:RHS]
    solution_ref[...] = own_ref[pl.ds(2 * RHS, RHS), :] + size * own_ref[pl.ds(0, RHS), :]
    residual_ref[...] = own_ref[pl.ds(RHS, RHS), :] - size * applied_ref[...]


def finish(got, own, applied):
    return pl.pallas_call(
        finish_kernel,
        out_shape=[shape(RHS, BLK), shape(RHS, BLK)],
        compiler_params=limit(8),
        name="finish",
    )(got, own, applied)


def exchange(pieces, axis):
    return lax.all_to_all(pieces, axis, split_axis=0, concat_axis=0, tiled=True)


def all_around(array, axis):
    size, here = lax.axis_size(axis), lax.axis_index(axis)
    whole = jnp.zeros((size, *array.shape), array.dtype)
    for k in range(size):
        block = array if k == 0 else lax.ppermute(array, axis, [(i, (i + k) % size) for i in range(size)])
        whole = lax.dynamic_update_index_in_dim(whole, block, (here - k + size) % size, 0)
    return whole


def other_core(array):
    return lax.ppermute(array, CORE, [(0, 1), (1, 0)])


def local(points, inv_scales, amplitude, noise_var, targets, initial, ritz_basis):
    near, pts, held = spread(points, inv_scales[None, :], initial, ritz_basis, targets)
    scalars = jnp.concatenate([amplitude, noise_var])
    scalars = jnp.broadcast_to(scalars[:, None], (2, BLK))
    near = exchange(near, Z)
    pts = all_around(pts, "col_0")
    pts = all_around(pts, "row_0").reshape(NB, FEAT + RITZ, BLK)
    near, scalars = lax.optimization_barrier((near, scalars))
    far = other_core(near)
    hi, lo, part = make_tile(near, far, pts)

    vec = exchange(at_owner(exchange(part, XY), held, scalars), XY)
    gram = make_gram(vec, pts)
    vec, gram = lax.optimization_barrier((vec, gram))
    image = apply_tile(hi, lo, vec, pts)
    image, gram = lax.optimization_barrier((image, exchange(gram, Z)))
    gram = jnp.sum(gram, axis=0)
    part, own = solve(gram, other_core(gram), image, vec, held)
    applied, stats = make_stats(exchange(part, CZ), own, scalars)
    return tuple(finish(exchange(stats, EVERY), own, applied))


def solution(mesh):
    torus = Mesh(mesh.devices.reshape(4, 8, 4, 2), ("row_0", "row_1", "col_0", "col_1"))
    in_specs = (
        P(None, COL_ROW),
        P(),
        P(),
        P(),
        P(None, COL_ROW),
        P(None, COL_ROW),
        P(None, COL_ROW),
    )
    out_specs = (P(None, COL_ROW), P(None, COL_ROW))
    return jax.shard_map(local, mesh=torus, in_specs=in_specs, out_specs=out_specs, check_vma=False)
```

```python
import math

import jax
import jax.numpy as jnp
from jax import lax
from jax.experimental import pallas as pl
from jax.experimental.pallas import tpu as pltpu
from jax.sharding import Mesh
from jax.sharding import PartitionSpec as P


CORE = "col_1"
Z = "row_1"
XY = ("row_0", "col_0")
CZ = ("col_1", "row_1")
EVERY = ("col_0", "col_1", "row_0", "row_1")
COL_ROW = EVERY

FEAT = 16
RITZ = 64
RHS = 8
VEC = RHS + RITZ
BLK = 128
NB = 16
PTS = NB * BLK
STEP = 256
CHUNK = 256
READ = 512
HALF = 2 * RHS + 2 * RITZ
PACKED = RHS + RITZ // 2 + 1
WORLD = 256

HIGH = lax.Precision.HIGHEST
F32 = jnp.float32
BF16 = jnp.bfloat16
NT = (((1,), (1,)), ((), ()))


def split2(x):
    hi = x.astype(BF16)
    return hi, (x - hi.astype(F32)).astype(BF16)


def split3(x):
    hi = x.astype(BF16).astype(F32)
    rest = x - hi
    mid = rest.astype(BF16).astype(F32)
    return hi, mid, rest - mid


def features(x, swap):
    a, b, c = split3(x)
    n1, n2, n3 = split3(-0.5 * jnp.sum(x * x, axis=0, keepdims=True))
    row = lax.broadcasted_iota(jnp.int32, x.shape, 0)
    base = 3 if swap else 0
    norm = jnp.where(row == base, n1, jnp.where(row == base + 1, n2, jnp.where(row == base + 2, n3, 0.0)))
    one = 0 if swap else 3
    norm = jnp.where((row >= one) & (row < one + 3), 1.0, norm)
    zero = jnp.zeros_like(x)
    if swap:
        parts = [a, b, a, b, c, a, norm, zero]
    else:
        parts = [a, a, b, b, a, c, norm, zero]
    return jnp.concatenate(parts, axis=0)


def vmem():
    return pl.BlockSpec(memory_space=pltpu.VMEM)


def in_hbm(array):
    return pltpu.with_memory_space_constraint(array, pltpu.HBM)


def shape(*dims):
    return jax.ShapeDtypeStruct(dims, F32)


def limit(mib):
    return pltpu.CompilerParams(vmem_limit_bytes=mib << 20)


def hbm():
    return pl.BlockSpec(memory_space=pltpu.HBM)


def spread_kernel(
    points_hbm,
    scale_hbm,
    initial_hbm,
    ritz_hbm,
    targets_hbm,
    near_ref,
    pts_ref,
    held_ref,
    points_ref,
    scale_ref,
    sem,
):
    copies = [
        pltpu.make_async_copy(points_hbm, points_ref, sem.at[0]),
        pltpu.make_async_copy(scale_hbm, scale_ref, sem.at[1]),
        pltpu.make_async_copy(targets_hbm, held_ref.at[pl.ds(0, RHS)], sem.at[2]),
        pltpu.make_async_copy(initial_hbm, held_ref.at[pl.ds(RHS, RHS)], sem.at[3]),
        pltpu.make_async_copy(ritz_hbm, held_ref.at[pl.ds(2 * RHS, RITZ)], sem.at[4]),
    ]
    for copy in copies:
        copy.start()
    for copy in copies:
        copy.wait()
    scaled = points_ref[...] * (scale_ref[...].T * math.sqrt(math.log2(math.e)))
    for b in range(NB // 2):
        near_ref[b, pl.ds(0, FEAT), :] = scaled
        near_ref[b, pl.ds(FEAT, VEC), :] = held_ref[pl.ds(RHS, VEC), :]
    pts_ref[pl.ds(0, FEAT), :] = scaled
    pts_ref[pl.ds(FEAT, RITZ), :] = held_ref[pl.ds(2 * RHS, RITZ), :]


def spread(points, scales, initial, ritz, targets):
    return pl.pallas_call(
        spread_kernel,
        in_specs=[hbm()] * 5,
        out_specs=[vmem()] * 3,
        out_shape=[
            shape(NB // 2, FEAT + VEC, BLK),
            shape(FEAT + RITZ, BLK),
            shape(RHS + VEC, BLK),
        ],
        scratch_shapes=[
            pltpu.VMEM((FEAT, BLK), F32),
            pltpu.VMEM((1, FEAT), F32),
            pltpu.SemaphoreType.DMA((5,)),
        ],
        compiler_params=limit(8),
        name="spread",
    )(*map(in_hbm, (points, scales, initial, ritz, targets)))


def tile_kernel(
    near_ref, far_ref, out_ref, mark_ref, hi_hbm, lo_hbm, part_ref, hi_ref, lo_ref, cols_ref, rows_ref, vec_ref, sem
):
    for b in range(NB):
        src = near_ref if b < NB // 2 else far_ref
        at = b % (NB // 2)
        lanes = pl.ds(b * BLK, BLK)
        cols_ref[:, lanes] = features(src[at, :FEAT, :], False).astype(BF16)
        tall = jnp.concatenate([src[at, FEAT:, :], jnp.zeros((BLK - VEC, BLK), F32)], axis=0).T
        hi, lo = split2(tall)
        vec_ref[lanes, pl.ds(0, BLK)] = hi
        vec_ref[lanes, pl.ds(BLK, BLK)] = lo
        rows_ref[lanes, :] = features(out_ref[b, :FEAT, :], True).T.astype(BF16)

    def copies(step):
        rows = pl.ds(step * STEP, STEP)
        return (
            pltpu.make_async_copy(hi_ref.at[rows], hi_hbm.at[rows], sem.at[0, step]),
            pltpu.make_async_copy(lo_ref.at[rows], lo_hbm.at[rows], sem.at[1, step]),
        )

    steps = PTS // STEP
    for step in range(steps + 1):
        rows, before = pl.ds(step * STEP, STEP), pl.ds((step - 1) * STEP, STEP)
        if step > 0:
            for copy in copies(step - 1):
                copy.start()
        total = jnp.zeros((STEP, 2 * BLK), F32)
        for c in range(PTS // CHUNK):
            lanes = pl.ds(c * CHUNK, CHUNK)
            if step > 0:
                vec = vec_ref[lanes, :]
                total += jnp.dot(hi_ref[before, lanes], vec, preferred_element_type=F32)
                total += jnp.dot(lo_ref[before, lanes], vec, preferred_element_type=F32)
            if step < steps:
                power = jnp.dot(rows_ref[rows, :], cols_ref[:, lanes], preferred_element_type=F32)
                hi, lo = split2(jnp.exp2(jnp.minimum(power, 0.0)))
                hi_ref[rows, lanes] = hi
                lo_ref[rows, lanes] = lo
        if step > 0:
            both = total[:, :BLK] + total[:, BLK:]
            for h in range(STEP // BLK):
                part_ref[(step - 1) * (STEP // BLK) + h] = both[h * BLK : (h + 1) * BLK].T[:VEC]
    for step in range(steps):
        for copy in copies(step):
            copy.wait()


def make_tile(near, far, out, mark):
    return pl.pallas_call(
        tile_kernel,
        in_specs=[vmem(), vmem(), vmem(), vmem()],
        out_specs=[hbm(), hbm(), vmem()],
        out_shape=[
            pltpu.HBM((PTS, PTS), BF16),
            pltpu.HBM((PTS, PTS), BF16),
            shape(NB, VEC, BLK),
        ],
        scratch_shapes=[
            pltpu.VMEM((PTS, PTS), BF16),
            pltpu.VMEM((PTS, PTS), BF16),
            pltpu.VMEM((BLK, PTS), BF16),
            pltpu.VMEM((PTS, BLK), BF16),
            pltpu.VMEM((PTS, 2 * BLK), BF16),
            pltpu.SemaphoreType.DMA((2, PTS // STEP)),
        ],
        compiler_params=limit(40),
        name="kernel_tile",
    )(near, far, out, mark)


def owner_kernel(got_ref, held_ref, scalars_ref, out_ref):
    total = got_ref[0]
    for b in range(1, NB):
        total += got_ref[b]
    gain, nugget = scalars_ref[pl.ds(0, 1), :], scalars_ref[pl.ds(1, 1), :]
    applied = gain * total + nugget * held_ref[pl.ds(RHS, VEC), :]
    first = held_ref[pl.ds(0, RHS), :] - applied[:RHS]
    image = applied[RHS:]
    for b in range(NB):
        out_ref[b, pl.ds(0, RHS), :] = first
        out_ref[b, pl.ds(RHS, RITZ), :] = image


def at_owner(got, held, scalars):
    return pl.pallas_call(
        owner_kernel,
        out_shape=shape(NB, VEC, BLK),
        compiler_params=limit(8),
        name="at_owner",
    )(got, held, scalars)


def square_iota():
    return lax.broadcasted_iota(jnp.int32, (RITZ, RITZ), 0), lax.broadcasted_iota(jnp.int32, (RITZ, RITZ), 1)


def gram_kernel(vec_ref, pts_ref, out_ref, left_ref, right_ref):
    for b in range(NB):
        lanes = pl.ds(b * BLK, BLK)
        left_ref[:, lanes] = vec_ref[b]
        right_ref[pl.ds(0, RITZ), lanes] = pts_ref[b, FEAT:, :]
        right_ref[pl.ds(RITZ, RITZ), lanes] = vec_ref[b, RHS:, :]
    gram = lax.dot_general(left_ref[...], right_ref[...], NT, precision=HIGH, preferred_element_type=F32)
    coarse = gram[RHS:, :RITZ]
    coarse = 0.5 * (coarse + coarse.T)
    image = gram[RHS:, RITZ:]
    i, j = square_iota()
    packed = jnp.where(j >= i, coarse, image)
    diagonal = jnp.sum(jnp.where(i == j, image, 0.0), axis=0, keepdims=True)
    for b in range(NB // 2):
        out_ref[b, pl.ds(0, RHS), :] = gram[:RHS]
        out_ref[b, pl.ds(RHS, RITZ // 2), :] = jnp.concatenate([packed[: RITZ // 2], packed[RITZ // 2 :]], axis=1)
        out_ref[b, pl.ds(RHS + RITZ // 2, 1), :] = jnp.concatenate([diagonal, diagonal], axis=1)


def make_gram(vec, pts):
    return pl.pallas_call(
        gram_kernel,
        out_shape=shape(NB // 2, PACKED, BLK),
        scratch_shapes=[pltpu.VMEM((VEC, PTS), F32), pltpu.VMEM((2 * RITZ, PTS), F32)],
        compiler_params=limit(12),
        name="gram",
    )(vec, pts)


def inverse(matrix):
    full = (8, 2 * RITZ)
    i, j = square_iota()
    work = jnp.concatenate([matrix, jnp.where(i == j, 1.0, 0.0)], axis=1)
    work = [work[b : b + 8] for b in range(0, RITZ, 8)]
    sub = lax.broadcasted_iota(jnp.int32, full, 0)

    def pair(a, b, c, d, top, low):
        scale = 1.0 / (a * d - b * c)
        return (d * top - b * low) * scale, (a * low - c * top) * scale

    for k in range(0, RITZ, 4):
        at, row = k // 8, k % 8
        cols = [[jnp.broadcast_to(w[:, k + q : k + q + 1], full) for w in work] for q in range(4)]
        rows = [jnp.broadcast_to(work[at][row + q : row + q + 1], full) for q in range(4)]
        e = [[jnp.broadcast_to(cols[r][at][row + q : row + q + 1], full) for r in range(4)] for q in range(4)]
        r0, r1 = pair(e[0][0], e[0][1], e[1][0], e[1][1], rows[0], rows[1])
        f = [pair(e[0][0], e[0][1], e[1][0], e[1][1], e[0][r], e[1][r]) for r in (2, 3)]
        rows[2] = rows[2] - e[2][0] * r0 - e[2][1] * r1
        rows[3] = rows[3] - e[3][0] * r0 - e[3][1] * r1
        g = [[e[q][r] - e[q][0] * f[r - 2][0] - e[q][1] * f[r - 2][1] for r in (2, 3)] for q in (2, 3)]
        r2, r3 = pair(g[0][0], g[0][1], g[1][0], g[1][1], rows[2], rows[3])
        r0 = r0 - f[0][0] * r2 - f[1][0] * r3
        r1 = r1 - f[0][1] * r2 - f[1][1] * r3
        final = (r0, r1, r2, r3)
        work = [
            w - ((cols[0][b] * r0 + cols[1][b] * r1) + (cols[2][b] * r2 + cols[3][b] * r3))
            for b, w in enumerate(work)
        ]
        for q in range(4):
            work[at] = jnp.where(sub == row + q, final[q], work[at])
    return jnp.concatenate(work, axis=0)[:, RITZ:]


def apply_kernel(hi_hbm, lo_hbm, vec_ref, pts_ref, out_ref, rows_ref, hi_ref, lo_ref, sem):
    copies = []
    for step in range(PTS // READ):
        lanes = pl.ds(step * READ, READ)
        copies.append(
            (
                pltpu.make_async_copy(hi_hbm.at[:, lanes], hi_ref.at[:, lanes], sem.at[0, step]),
                pltpu.make_async_copy(lo_hbm.at[:, lanes], lo_ref.at[:, lanes], sem.at[1, step]),
            )
        )
        for copy in copies[-1]:
            copy.start()
    for b in range(NB):
        lanes = pl.ds(b * BLK, BLK)
        first = vec_ref[b, :RHS, :]
        hi, lo = split2(
            jnp.concatenate([first, jnp.zeros_like(first), pts_ref[b, FEAT:, :], vec_ref[b, RHS:, :]], axis=0)
        )
        rows_ref[pl.ds(0, HALF), lanes] = hi
        rows_ref[pl.ds(HALF, HALF), lanes] = lo
    for step in range(PTS // READ):
        lanes = pl.ds(step * READ, READ)
        for copy in copies[step]:
            copy.wait()
        both = jnp.dot(rows_ref[...], hi_ref[:, lanes], preferred_element_type=F32)
        more = jnp.dot(rows_ref[pl.ds(0, HALF), :], lo_ref[:, lanes], preferred_element_type=F32)
        out_ref[:, lanes] = both[:HALF] + both[HALF:] + more


def apply_tile(hi, lo, vec, pts):
    return pl.pallas_call(
        apply_kernel,
        in_specs=[hbm(), hbm(), vmem(), vmem()],
        out_shape=shape(HALF, PTS),
        scratch_shapes=[
            pltpu.VMEM((2 * HALF, PTS), BF16),
            pltpu.VMEM((PTS, PTS), BF16),
            pltpu.VMEM((PTS, PTS), BF16),
            pltpu.SemaphoreType.DMA((2, PTS // READ)),
        ],
        compiler_params=limit(32),
        cost_estimate=pl.CostEstimate(flops=8 * HALF * PTS * PTS, bytes_accessed=4 * PTS * PTS, transcendentals=0),
        name="apply_tile",
    )(in_hbm(hi), in_hbm(lo), vec, pts)


def solve_kernel(gram_ref, more_ref, image_ref, vec_ref, held_ref, part_ref, own_ref):
    gram = gram_ref[...] + more_ref[...]
    projected = gram[:RHS, :RITZ]
    first = gram[:RHS, RITZ:]
    square = jnp.concatenate([gram[RHS : RHS + RITZ // 2, :RITZ], gram[RHS : RHS + RITZ // 2, RITZ:]], axis=0)
    turned = square.T
    i, j = square_iota()
    coarse = jnp.where(j >= i, square, turned)
    image = jnp.where(j < i, square, jnp.where(j > i, turned, gram[RHS + RITZ // 2 :, :RITZ]))
    solve = inverse(coarse)
    amounts = lax.dot_general(projected, solve, NT, precision=HIGH, preferred_element_type=F32)
    against = first - jnp.dot(amounts, image, precision=HIGH, preferred_element_type=F32)
    turns = lax.dot_general(against, solve, NT, precision=HIGH, preferred_element_type=F32)
    zero = jnp.zeros_like(turns)
    coef = jnp.concatenate([turns, amounts], axis=1)
    value = image_ref[pl.ds(0, RHS), :] - jnp.dot(
        coef, image_ref[pl.ds(2 * RHS, 2 * RITZ), :], precision=HIGH, preferred_element_type=F32
    )
    core = lax.axis_index(CORE)
    for at in range(NB):
        half = (at // (NB // 2) + core) % 2
        part_ref[half * (NB // 2) + at % (NB // 2)] = value[:, at * BLK : (at + 1) * BLK]
    mine = lax.axis_index("row_0") * 4 + lax.axis_index("col_0")
    basis = jnp.concatenate([held_ref[pl.ds(2 * RHS, RITZ), :], vec_ref[mine, RHS:, :]], axis=0)
    wanted = jnp.concatenate(
        [coef, jnp.concatenate([zero, amounts], axis=1), jnp.concatenate([-amounts, zero], axis=1)], axis=0
    )
    base = vec_ref[mine, :RHS, :]
    base = jnp.concatenate([base, base, held_ref[pl.ds(RHS, RHS), :]], axis=0)
    own_ref[...] = base - jnp.dot(wanted, basis, precision=HIGH, preferred_element_type=F32)


def solve(gram, more, image, vec, held):
    return pl.pallas_call(
        solve_kernel,
        out_shape=[shape(NB, RHS, BLK), shape(3 * RHS, BLK)],
        compiler_params=limit(12),
        name="solve",
    )(gram, more, image, vec, held)


def stats_kernel(got_ref, own_ref, scalars_ref, applied_ref, out_ref):
    total = got_ref[0]
    for b in range(1, NB):
        total += got_ref[b]
    direction = own_ref[pl.ds(0, RHS), :]
    residual = own_ref[pl.ds(RHS, RHS), :]
    applied = scalars_ref[pl.ds(0, 1), :] * total + scalars_ref[pl.ds(1, 1), :] * direction
    applied_ref[...] = applied
    sums = jnp.concatenate(
        [
            jnp.sum(direction * applied, axis=1, keepdims=True),
            jnp.sum(residual * residual, axis=1, keepdims=True),
        ],
        axis=0,
    )
    sums = jnp.broadcast_to(sums, (2 * RHS, BLK)).T[:RHS]
    for b in range(WORLD // RHS):
        out_ref[pl.ds(b * RHS, RHS), :] = sums


def make_stats(got, own, scalars):
    return pl.pallas_call(
        stats_kernel,
        out_shape=[shape(RHS, BLK), shape(WORLD, 2 * RHS)],
        compiler_params=limit(8),
        name="stats",
    )(got, own, scalars)


def finish_kernel(got_ref, own_ref, applied_ref, solution_ref, residual_ref):
    sums = jnp.sum(got_ref[...], axis=0, keepdims=True)
    i = lax.broadcasted_iota(jnp.int32, (2 * RHS, 2 * RHS), 0)
    j = lax.broadcasted_iota(jnp.int32, (2 * RHS, 2 * RHS), 1)
    sums = jnp.sum(jnp.where(i == j, sums, 0.0), axis=1, keepdims=True)
    size = sums[RHS:] / sums[:RHS]
    solution_ref[...] = own_ref[pl.ds(2 * RHS, RHS), :] + size * own_ref[pl.ds(0, RHS), :]
    residual_ref[...] = own_ref[pl.ds(RHS, RHS), :] - size * applied_ref[...]


def finish(got, own, applied):
    return pl.pallas_call(
        finish_kernel,
        out_shape=[shape(RHS, BLK), shape(RHS, BLK)],
        compiler_params=limit(8),
        name="finish",
    )(got, own, applied)


def exchange(pieces, axis):
    return lax.all_to_all(pieces, axis, split_axis=0, concat_axis=0, tiled=True)


def all_around(array, axis):
    size, here = lax.axis_size(axis), lax.axis_index(axis)
    whole = jnp.zeros((size, *array.shape), array.dtype)
    for k in range(size):
        block = array if k == 0 else lax.ppermute(array, axis, [(i, (i + k) % size) for i in range(size)])
        whole = lax.dynamic_update_index_in_dim(whole, block, (here - k + size) % size, 0)
    return whole


def other_core(array):
    return lax.ppermute(array, CORE, [(0, 1), (1, 0)])


def local(points, inv_scales, amplitude, noise_var, targets, initial, ritz_basis):
    near, pts, held = spread(points, inv_scales[None, :], initial, ritz_basis, targets)
    scalars = jnp.concatenate([amplitude, noise_var])
    scalars = jnp.broadcast_to(scalars[:, None], (2, BLK))
    pts = all_around(pts, "col_0")
    near = exchange(near, Z)
    pts = all_around(pts, "row_0").reshape(NB, FEAT + RITZ, BLK)
    near, scalars = lax.optimization_barrier((near, scalars))
    far = other_core(near)
    mark = near[0, :8] * 0.5
    hi, lo, part = make_tile(near, far, pts, mark)

    vec = exchange(at_owner(exchange(part, XY), held, scalars), XY)
    gram = make_gram(vec, pts)
    vec, gram = lax.optimization_barrier((vec, gram))
    image = apply_tile(hi, lo, vec, pts)
    image, gram = lax.optimization_barrier((image, exchange(gram, Z)))
    gram = jnp.sum(gram, axis=0)
    part, own = solve(gram, other_core(gram), image, vec, held)
    applied, stats = make_stats(exchange(part, CZ), own, scalars)
    return tuple(finish(exchange(stats, EVERY), own, applied))


def solution(mesh):
    torus = Mesh(mesh.devices.reshape(4, 8, 4, 2), ("row_0", "row_1", "col_0", "col_1"))
    in_specs = (
        P(None, COL_ROW),
        P(),
        P(),
        P(),
        P(None, COL_ROW),
        P(None, COL_ROW),
        P(None, COL_ROW),
    )
    out_specs = (P(None, COL_ROW), P(None, COL_ROW))
    return jax.shard_map(local, mesh=torus, in_specs=in_specs, out_specs=out_specs, check_vma=False)
```

```python
import math

import jax
import jax.numpy as jnp
from jax import lax
from jax.experimental import pallas as pl
from jax.experimental.pallas import tpu as pltpu
from jax.sharding import Mesh
from jax.sharding import PartitionSpec as P


CORE = "col_1"
Z = "row_1"
XY = ("row_0", "col_0")
CZ = ("col_1", "row_1")
EVERY = ("col_0", "col_1", "row_0", "row_1")
COL_ROW = EVERY

FEAT = 16
RITZ = 64
RHS = 8
VEC = RHS + RITZ
LEFT = VEC + 8
BLK = 128
NB = 16
PTS = NB * BLK
STEP = 256
CHUNK = 256
READ = 512
HALF = 2 * RHS + 2 * RITZ
PACKED = RHS + RITZ // 2 + 1
WORLD = 256

HIGH = lax.Precision.HIGHEST
F32 = jnp.float32
BF16 = jnp.bfloat16
NT = (((1,), (1,)), ((), ()))


def split2(x):
    hi = x.astype(BF16)
    return hi, (x - hi.astype(F32)).astype(BF16)


def split3(x):
    hi = x.astype(BF16).astype(F32)
    rest = x - hi
    mid = rest.astype(BF16).astype(F32)
    return hi, mid, rest - mid


def features(x, swap):
    a, b, c = split3(x)
    n1, n2, n3 = split3(-0.5 * jnp.sum(x * x, axis=0, keepdims=True))
    row = lax.broadcasted_iota(jnp.int32, x.shape, 0)
    base = 3 if swap else 0
    norm = jnp.where(row == base, n1, jnp.where(row == base + 1, n2, jnp.where(row == base + 2, n3, 0.0)))
    one = 0 if swap else 3
    norm = jnp.where((row >= one) & (row < one + 3), 1.0, norm)
    zero = jnp.zeros_like(x)
    if swap:
        parts = [a, b, a, b, c, a, norm, zero]
    else:
        parts = [a, a, b, b, a, c, norm, zero]
    return jnp.concatenate(parts, axis=0)


def vmem():
    return pl.BlockSpec(memory_space=pltpu.VMEM)


def in_hbm(array):
    return pltpu.with_memory_space_constraint(array, pltpu.HBM)


def shape(*dims):
    return jax.ShapeDtypeStruct(dims, F32)


def limit(mib):
    return pltpu.CompilerParams(vmem_limit_bytes=mib << 20)


def hbm():
    return pl.BlockSpec(memory_space=pltpu.HBM)


def spread_kernel(
    points_hbm,
    scale_hbm,
    initial_hbm,
    ritz_hbm,
    targets_hbm,
    near_ref,
    pts_ref,
    held_ref,
    points_ref,
    scale_ref,
    sem,
):
    copies = [
        pltpu.make_async_copy(points_hbm, points_ref, sem.at[0]),
        pltpu.make_async_copy(scale_hbm, scale_ref, sem.at[1]),
        pltpu.make_async_copy(targets_hbm, held_ref.at[pl.ds(0, RHS)], sem.at[2]),
        pltpu.make_async_copy(initial_hbm, held_ref.at[pl.ds(RHS, RHS)], sem.at[3]),
        pltpu.make_async_copy(ritz_hbm, held_ref.at[pl.ds(2 * RHS, RITZ)], sem.at[4]),
    ]
    for copy in copies:
        copy.start()
    for copy in copies:
        copy.wait()
    scaled = points_ref[...] * (scale_ref[...].T * math.sqrt(math.log2(math.e)))
    for b in range(NB // 2):
        near_ref[b, pl.ds(0, FEAT), :] = scaled
        near_ref[b, pl.ds(FEAT, VEC), :] = held_ref[pl.ds(RHS, VEC), :]
    pts_ref[pl.ds(0, FEAT), :] = scaled
    pts_ref[pl.ds(FEAT, RITZ), :] = held_ref[pl.ds(2 * RHS, RITZ), :]


def spread(points, scales, initial, ritz, targets):
    return pl.pallas_call(
        spread_kernel,
        in_specs=[hbm()] * 5,
        out_specs=[vmem()] * 3,
        out_shape=[
            shape(NB // 2, FEAT + VEC, BLK),
            shape(FEAT + RITZ, BLK),
            shape(RHS + VEC, BLK),
        ],
        scratch_shapes=[
            pltpu.VMEM((FEAT, BLK), F32),
            pltpu.VMEM((1, FEAT), F32),
            pltpu.SemaphoreType.DMA((5,)),
        ],
        compiler_params=limit(8),
        name="spread",
    )(*map(in_hbm, (points, scales, initial, ritz, targets)))


def tile_kernel(
    near_ref, far_ref, out_ref, mark_ref, hi_hbm, lo_hbm, part_ref, hi_ref, lo_ref, cols_ref, rows_ref, vec_ref, sem
):
    for b in range(NB):
        src = near_ref if b < NB // 2 else far_ref
        at = b % (NB // 2)
        lanes = pl.ds(b * BLK, BLK)
        cols_ref[:, lanes] = features(src[at, :FEAT, :], False).astype(BF16)
        tall = jnp.concatenate([src[at, FEAT:, :], jnp.zeros((BLK - VEC, BLK), F32)], axis=0).T
        hi, lo = split2(tall)
        vec_ref[lanes, pl.ds(0, BLK)] = hi
        vec_ref[lanes, pl.ds(BLK, BLK)] = lo
        rows_ref[lanes, :] = features(out_ref[b, :FEAT, :], True).T.astype(BF16)

    def copies(step):
        rows = pl.ds(step * STEP, STEP)
        return (
            pltpu.make_async_copy(hi_ref.at[rows], hi_hbm.at[rows], sem.at[0, step]),
            pltpu.make_async_copy(lo_ref.at[rows], lo_hbm.at[rows], sem.at[1, step]),
        )

    steps = PTS // STEP
    for step in range(steps + 1):
        rows, before = pl.ds(step * STEP, STEP), pl.ds((step - 1) * STEP, STEP)
        if step > 0:
            for copy in copies(step - 1):
                copy.start()
        total = jnp.zeros((STEP, 2 * BLK), F32)
        for c in range(PTS // CHUNK):
            lanes = pl.ds(c * CHUNK, CHUNK)
            if step > 0:
                vec = vec_ref[lanes, :]
                total += jnp.dot(hi_ref[before, lanes], vec, preferred_element_type=F32)
                total += jnp.dot(lo_ref[before, lanes], vec, preferred_element_type=F32)
            if step < steps:
                power = jnp.dot(rows_ref[rows, :], cols_ref[:, lanes], preferred_element_type=F32)
                hi, lo = split2(jnp.exp2(jnp.minimum(power, 0.0)))
                hi_ref[rows, lanes] = hi
                lo_ref[rows, lanes] = lo
        if step > 0:
            both = total[:, :BLK] + total[:, BLK:]
            for h in range(STEP // BLK):
                part_ref[(step - 1) * (STEP // BLK) + h] = both[h * BLK : (h + 1) * BLK].T[:VEC]
    for step in range(steps):
        for copy in copies(step):
            copy.wait()


def make_tile(near, far, out, mark):
    return pl.pallas_call(
        tile_kernel,
        in_specs=[vmem(), vmem(), vmem(), vmem()],
        out_specs=[hbm(), hbm(), vmem()],
        out_shape=[
            pltpu.HBM((PTS, PTS), BF16),
            pltpu.HBM((PTS, PTS), BF16),
            shape(NB, VEC, BLK),
        ],
        scratch_shapes=[
            pltpu.VMEM((PTS, PTS), BF16),
            pltpu.VMEM((PTS, PTS), BF16),
            pltpu.VMEM((BLK, PTS), BF16),
            pltpu.VMEM((PTS, BLK), BF16),
            pltpu.VMEM((PTS, 2 * BLK), BF16),
            pltpu.SemaphoreType.DMA((2, PTS // STEP)),
        ],
        compiler_params=limit(40),
        name="kernel_tile",
    )(near, far, out, mark)


def owner_kernel(got_ref, held_ref, scalars_ref, out_ref):
    total = got_ref[0]
    for b in range(1, NB):
        total += got_ref[b]
    gain, nugget = scalars_ref[pl.ds(0, 1), :], scalars_ref[pl.ds(1, 1), :]
    applied = gain * total + nugget * held_ref[pl.ds(RHS, VEC), :]
    first = held_ref[pl.ds(0, RHS), :] - applied[:RHS]
    image = applied[RHS:]
    for b in range(NB):
        out_ref[b, pl.ds(0, RHS), :] = first
        out_ref[b, pl.ds(RHS, RITZ), :] = image


def at_owner(got, held, scalars):
    return pl.pallas_call(
        owner_kernel,
        out_shape=shape(NB, VEC, BLK),
        compiler_params=limit(8),
        name="at_owner",
    )(got, held, scalars)


def square_iota():
    return lax.broadcasted_iota(jnp.int32, (RITZ, RITZ), 0), lax.broadcasted_iota(jnp.int32, (RITZ, RITZ), 1)


def gram_kernel(vec_ref, pts_ref, out_ref, left_ref, right_ref):
    for b in range(NB):
        lanes = pl.ds(b * BLK, BLK)
        pad = jnp.zeros((LEFT - VEC, BLK), F32)
        image = split3(vec_ref[b])
        basis = split3(pts_ref[b, FEAT:, :])
        for q in range(3):
            left_ref[pl.ds(q * LEFT, LEFT), lanes] = jnp.concatenate([image[q], pad], axis=0).astype(BF16)
            right_ref[pl.ds(q * 2 * RITZ, RITZ), lanes] = basis[q].astype(BF16)
            right_ref[pl.ds(q * 2 * RITZ + RITZ, RITZ), lanes] = image[q][RHS:].astype(BF16)
    gram = jnp.zeros((VEC, 2 * RITZ), F32)
    for q in (2, 1, 0):
        rows = 3 - q
        left = left_ref[pl.ds(0, rows * LEFT), :]
        right = right_ref[pl.ds(q * 2 * RITZ, 2 * RITZ), :]
        total = lax.dot_general(left, right, NT, preferred_element_type=F32)
        for r in range(rows - 1, -1, -1):
            gram += total[r * LEFT : r * LEFT + VEC]
    coarse = gram[RHS:, :RITZ]
    coarse = 0.5 * (coarse + coarse.T)
    image = gram[RHS:, RITZ:]
    i, j = square_iota()
    packed = jnp.where(j >= i, coarse, image)
    diagonal = jnp.sum(jnp.where(i == j, image, 0.0), axis=0, keepdims=True)
    for b in range(NB // 2):
        out_ref[b, pl.ds(0, RHS), :] = gram[:RHS]
        out_ref[b, pl.ds(RHS, RITZ // 2), :] = jnp.concatenate([packed[: RITZ // 2], packed[RITZ // 2 :]], axis=1)
        out_ref[b, pl.ds(RHS + RITZ // 2, 1), :] = jnp.concatenate([diagonal, diagonal], axis=1)


def make_gram(vec, pts):
    return pl.pallas_call(
        gram_kernel,
        out_shape=shape(NB // 2, PACKED, BLK),
        scratch_shapes=[pltpu.VMEM((3 * LEFT, PTS), BF16), pltpu.VMEM((6 * RITZ, PTS), BF16)],
        compiler_params=limit(12),
        name="gram",
    )(vec, pts)


def inverse(matrix):
    full = (8, 2 * RITZ)
    i, j = square_iota()
    work = jnp.concatenate([matrix, jnp.where(i == j, 1.0, 0.0)], axis=1)
    work = [work[b : b + 8] for b in range(0, RITZ, 8)]
    sub = lax.broadcasted_iota(jnp.int32, full, 0)

    def pair(a, b, c, d, top, low):
        scale = 1.0 / (a * d - b * c)
        return (d * top - b * low) * scale, (a * low - c * top) * scale

    for k in range(0, RITZ, 4):
        at, row = k // 8, k % 8
        cols = [[jnp.broadcast_to(w[:, k + q : k + q + 1], full) for w in work] for q in range(4)]
        rows = [jnp.broadcast_to(work[at][row + q : row + q + 1], full) for q in range(4)]
        e = [[jnp.broadcast_to(cols[r][at][row + q : row + q + 1], full) for r in range(4)] for q in range(4)]
        r0, r1 = pair(e[0][0], e[0][1], e[1][0], e[1][1], rows[0], rows[1])
        f = [pair(e[0][0], e[0][1], e[1][0], e[1][1], e[0][r], e[1][r]) for r in (2, 3)]
        rows[2] = rows[2] - e[2][0] * r0 - e[2][1] * r1
        rows[3] = rows[3] - e[3][0] * r0 - e[3][1] * r1
        g = [[e[q][r] - e[q][0] * f[r - 2][0] - e[q][1] * f[r - 2][1] for r in (2, 3)] for q in (2, 3)]
        r2, r3 = pair(g[0][0], g[0][1], g[1][0], g[1][1], rows[2], rows[3])
        r0 = r0 - f[0][0] * r2 - f[1][0] * r3
        r1 = r1 - f[0][1] * r2 - f[1][1] * r3
        final = (r0, r1, r2, r3)
        work = [
            w - ((cols[0][b] * r0 + cols[1][b] * r1) + (cols[2][b] * r2 + cols[3][b] * r3))
            for b, w in enumerate(work)
        ]
        for q in range(4):
            work[at] = jnp.where(sub == row + q, final[q], work[at])
    return jnp.concatenate(work, axis=0)[:, RITZ:]


def apply_kernel(hi_hbm, lo_hbm, vec_ref, pts_ref, out_ref, rows_ref, hi_ref, lo_ref, sem):
    copies = []
    for step in range(PTS // READ):
        lanes = pl.ds(step * READ, READ)
        copies.append(
            (
                pltpu.make_async_copy(hi_hbm.at[:, lanes], hi_ref.at[:, lanes], sem.at[0, step]),
                pltpu.make_async_copy(lo_hbm.at[:, lanes], lo_ref.at[:, lanes], sem.at[1, step]),
            )
        )
        for copy in copies[-1]:
            copy.start()
    for b in range(NB):
        lanes = pl.ds(b * BLK, BLK)
        first = vec_ref[b, :RHS, :]
        hi, lo = split2(
            jnp.concatenate([first, jnp.zeros_like(first), pts_ref[b, FEAT:, :], vec_ref[b, RHS:, :]], axis=0)
        )
        rows_ref[pl.ds(0, HALF), lanes] = hi
        rows_ref[pl.ds(HALF, HALF), lanes] = lo
    for step in range(PTS // READ):
        lanes = pl.ds(step * READ, READ)
        for copy in copies[step]:
            copy.wait()
        both = jnp.dot(rows_ref[...], hi_ref[:, lanes], preferred_element_type=F32)
        more = jnp.dot(rows_ref[pl.ds(0, HALF), :], lo_ref[:, lanes], preferred_element_type=F32)
        out_ref[:, lanes] = both[:HALF] + both[HALF:] + more


def apply_tile(hi, lo, vec, pts):
    return pl.pallas_call(
        apply_kernel,
        in_specs=[hbm(), hbm(), vmem(), vmem()],
        out_shape=shape(HALF, PTS),
        scratch_shapes=[
            pltpu.VMEM((2 * HALF, PTS), BF16),
            pltpu.VMEM((PTS, PTS), BF16),
            pltpu.VMEM((PTS, PTS), BF16),
            pltpu.SemaphoreType.DMA((2, PTS // READ)),
        ],
        compiler_params=limit(32),
        cost_estimate=pl.CostEstimate(flops=8 * HALF * PTS * PTS, bytes_accessed=4 * PTS * PTS, transcendentals=0),
        name="apply_tile",
    )(in_hbm(hi), in_hbm(lo), vec, pts)


def exact(left, right):
    return jnp.dot(left, right, precision=HIGH, preferred_element_type=F32)


def solve_kernel(gram_ref, more_ref, image_ref, vec_ref, held_ref, part_ref, own_ref):
    gram = gram_ref[...] + more_ref[...]
    projected = gram[:RHS, :RITZ]
    first = gram[:RHS, RITZ:]
    square = jnp.concatenate([gram[RHS : RHS + RITZ // 2, :RITZ], gram[RHS : RHS + RITZ // 2, RITZ:]], axis=0)
    turned = square.T
    i, j = square_iota()
    coarse = jnp.where(j >= i, square, turned)
    image = jnp.where(j < i, square, jnp.where(j > i, turned, gram[RHS + RITZ // 2 :, :RITZ]))
    solve = inverse(coarse)
    amounts = lax.dot_general(projected, solve, NT, precision=HIGH, preferred_element_type=F32)
    against = first - exact(amounts, image)
    turns = lax.dot_general(against, solve, NT, precision=HIGH, preferred_element_type=F32)
    value = image_ref[pl.ds(0, RHS), :] - exact(amounts, image_ref[pl.ds(2 * RHS + RITZ, RITZ), :])
    value = value - exact(turns, image_ref[pl.ds(2 * RHS, RITZ), :])
    core = lax.axis_index(CORE)
    for at in range(NB):
        half = (at // (NB // 2) + core) % 2
        part_ref[half * (NB // 2) + at % (NB // 2)] = value[:, at * BLK : (at + 1) * BLK]
    mine = lax.axis_index("row_0") * 4 + lax.axis_index("col_0")
    ritz = held_ref[pl.ds(2 * RHS, RITZ), :]
    residual = vec_ref[mine, :RHS, :] - exact(amounts, vec_ref[mine, RHS:, :])
    own_ref[pl.ds(0, RHS), :] = residual - exact(turns, ritz)
    own_ref[pl.ds(RHS, RHS), :] = residual
    own_ref[pl.ds(2 * RHS, RHS), :] = held_ref[pl.ds(RHS, RHS), :] + exact(amounts, ritz)


def solve(gram, more, image, vec, held):
    return pl.pallas_call(
        solve_kernel,
        out_shape=[shape(NB, RHS, BLK), shape(3 * RHS, BLK)],
        compiler_params=limit(12),
        name="solve",
    )(gram, more, image, vec, held)


def stats_kernel(got_ref, own_ref, scalars_ref, applied_ref, out_ref):
    total = got_ref[0]
    for b in range(1, NB):
        total += got_ref[b]
    direction = own_ref[pl.ds(0, RHS), :]
    residual = own_ref[pl.ds(RHS, RHS), :]
    applied = scalars_ref[pl.ds(0, 1), :] * total + scalars_ref[pl.ds(1, 1), :] * direction
    applied_ref[...] = applied
    sums = jnp.concatenate(
        [
            jnp.sum(direction * applied, axis=1, keepdims=True),
            jnp.sum(residual * residual, axis=1, keepdims=True),
        ],
        axis=0,
    )
    sums = jnp.broadcast_to(sums, (2 * RHS, BLK)).T[:RHS]
    for b in range(WORLD // RHS):
        out_ref[pl.ds(b * RHS, RHS), :] = sums


def make_stats(got, own, scalars):
    return pl.pallas_call(
        stats_kernel,
        out_shape=[shape(RHS, BLK), shape(WORLD, 2 * RHS)],
        compiler_params=limit(8),
        name="stats",
    )(got, own, scalars)


def finish_kernel(got_ref, own_ref, applied_ref, solution_ref, residual_ref):
    sums = jnp.sum(got_ref[...], axis=0, keepdims=True)
    i = lax.broadcasted_iota(jnp.int32, (2 * RHS, 2 * RHS), 0)
    j = lax.broadcasted_iota(jnp.int32, (2 * RHS, 2 * RHS), 1)
    sums = jnp.sum(jnp.where(i == j, sums, 0.0), axis=1, keepdims=True)
    size = sums[RHS:] / sums[:RHS]
    solution_ref[...] = own_ref[pl.ds(2 * RHS, RHS), :] + size * own_ref[pl.ds(0, RHS), :]
    residual_ref[...] = own_ref[pl.ds(RHS, RHS), :] - size * applied_ref[...]


def finish(got, own, applied):
    return pl.pallas_call(
        finish_kernel,
        out_shape=[shape(RHS, BLK), shape(RHS, BLK)],
        compiler_params=limit(8),
        name="finish",
    )(got, own, applied)


def exchange(pieces, axis):
    return lax.all_to_all(pieces, axis, split_axis=0, concat_axis=0, tiled=True)


def all_around(array, axis):
    size, here = lax.axis_size(axis), lax.axis_index(axis)
    whole = jnp.zeros((size, *array.shape), array.dtype)
    for k in range(size):
        block = array if k == 0 else lax.ppermute(array, axis, [(i, (i + k) % size) for i in range(size)])
        whole = lax.dynamic_update_index_in_dim(whole, block, (here - k + size) % size, 0)
    return whole


def other_core(array):
    return lax.ppermute(array, CORE, [(0, 1), (1, 0)])


def local(points, inv_scales, amplitude, noise_var, targets, initial, ritz_basis):
    near, pts, held = spread(points, inv_scales[None, :], initial, ritz_basis, targets)
    scalars = jnp.concatenate([amplitude, noise_var])
    scalars = jnp.broadcast_to(scalars[:, None], (2, BLK))
    pts = all_around(pts, "col_0")
    near = exchange(near, Z)
    pts = all_around(pts, "row_0").reshape(NB, FEAT + RITZ, BLK)
    near, scalars = lax.optimization_barrier((near, scalars))
    far = other_core(near)
    mark = near[0, :8] * 0.5
    hi, lo, part = make_tile(near, far, pts, mark)

    vec = exchange(at_owner(exchange(part, XY), held, scalars), XY)
    gram = make_gram(vec, pts)
    vec, gram = lax.optimization_barrier((vec, gram))
    image = apply_tile(hi, lo, vec, pts)
    image, gram = lax.optimization_barrier((image, exchange(gram, Z)))
    gram = jnp.sum(gram, axis=0)
    part, own = solve(gram, other_core(gram), image, vec, held)
    applied, stats = make_stats(exchange(part, CZ), own, scalars)
    return tuple(finish(exchange(stats, EVERY), own, applied))


def solution(mesh):
    torus = Mesh(mesh.devices.reshape(4, 8, 4, 2), ("row_0", "row_1", "col_0", "col_1"))
    in_specs = (
        P(None, COL_ROW),
        P(),
        P(),
        P(),
        P(None, COL_ROW),
        P(None, COL_ROW),
        P(None, COL_ROW),
    )
    out_specs = (P(None, COL_ROW), P(None, COL_ROW))
    return jax.shard_map(local, mesh=torus, in_specs=in_specs, out_specs=out_specs, check_vma=False)
```

```python
import math

import jax
import jax.numpy as jnp
from jax import lax
from jax.experimental import pallas as pl
from jax.experimental.pallas import tpu as pltpu
from jax.sharding import Mesh
from jax.sharding import PartitionSpec as P


CORE = "col_1"
Z = "row_1"
XY = ("row_0", "col_0")
CZ = ("col_1", "row_1")
EVERY = ("col_0", "col_1", "row_0", "row_1")
COL_ROW = EVERY

FEAT = 16
RITZ = 64
RHS = 8
VEC = RHS + RITZ
LEFT = VEC + 8
BLK = 128
NB = 16
PTS = NB * BLK
STEP = 256
CHUNK = 256
READ = 512
HALF = 2 * RHS + 2 * RITZ
PACKED = RHS + RITZ // 2 + 1
WORLD = 256

HIGH = lax.Precision.HIGHEST
F32 = jnp.float32
BF16 = jnp.bfloat16
NT = (((1,), (1,)), ((), ()))


def split2(x):
    hi = x.astype(BF16)
    return hi, (x - hi.astype(F32)).astype(BF16)


def split3(x):
    hi = x.astype(BF16).astype(F32)
    rest = x - hi
    mid = rest.astype(BF16).astype(F32)
    return hi, mid, rest - mid


def features(x, swap):
    a, b, c = split3(x)
    n1, n2, n3 = split3(-0.5 * jnp.sum(x * x, axis=0, keepdims=True))
    row = lax.broadcasted_iota(jnp.int32, x.shape, 0)
    base = 3 if swap else 0
    norm = jnp.where(row == base, n1, jnp.where(row == base + 1, n2, jnp.where(row == base + 2, n3, 0.0)))
    one = 0 if swap else 3
    norm = jnp.where((row >= one) & (row < one + 3), 1.0, norm)
    zero = jnp.zeros_like(x)
    if swap:
        parts = [a, b, a, b, c, a, norm, zero]
    else:
        parts = [a, a, b, b, a, c, norm, zero]
    return jnp.concatenate(parts, axis=0)


def vmem():
    return pl.BlockSpec(memory_space=pltpu.VMEM)


def in_hbm(array):
    return pltpu.with_memory_space_constraint(array, pltpu.HBM)


def shape(*dims):
    return jax.ShapeDtypeStruct(dims, F32)


def limit(mib):
    return pltpu.CompilerParams(vmem_limit_bytes=mib << 20)


def hbm():
    return pl.BlockSpec(memory_space=pltpu.HBM)


def spread_kernel(
    points_hbm,
    scale_hbm,
    initial_hbm,
    ritz_hbm,
    targets_hbm,
    near_ref,
    pts_ref,
    held_ref,
    points_ref,
    scale_ref,
    sem,
):
    copies = [
        pltpu.make_async_copy(points_hbm, points_ref, sem.at[0]),
        pltpu.make_async_copy(scale_hbm, scale_ref, sem.at[1]),
        pltpu.make_async_copy(targets_hbm, held_ref.at[pl.ds(0, RHS)], sem.at[2]),
        pltpu.make_async_copy(initial_hbm, held_ref.at[pl.ds(RHS, RHS)], sem.at[3]),
        pltpu.make_async_copy(ritz_hbm, held_ref.at[pl.ds(2 * RHS, RITZ)], sem.at[4]),
    ]
    for copy in copies:
        copy.start()
    for copy in copies:
        copy.wait()
    scaled = points_ref[...] * (scale_ref[...].T * math.sqrt(math.log2(math.e)))
    for b in range(NB // 2):
        near_ref[b, pl.ds(0, FEAT), :] = scaled
        near_ref[b, pl.ds(FEAT, VEC), :] = held_ref[pl.ds(RHS, VEC), :]
    pts_ref[pl.ds(0, FEAT), :] = scaled
    pts_ref[pl.ds(FEAT, RITZ), :] = held_ref[pl.ds(2 * RHS, RITZ), :]


def spread(points, scales, initial, ritz, targets):
    return pl.pallas_call(
        spread_kernel,
        in_specs=[hbm()] * 5,
        out_specs=[vmem()] * 3,
        out_shape=[
            shape(NB // 2, FEAT + VEC, BLK),
            shape(FEAT + RITZ, BLK),
            shape(RHS + VEC, BLK),
        ],
        scratch_shapes=[
            pltpu.VMEM((FEAT, BLK), F32),
            pltpu.VMEM((1, FEAT), F32),
            pltpu.SemaphoreType.DMA((5,)),
        ],
        compiler_params=limit(8),
        name="spread",
    )(*map(in_hbm, (points, scales, initial, ritz, targets)))


def tile_kernel(
    near_ref, far_ref, out_ref, mark_ref, hi_hbm, lo_hbm, part_ref, hi_ref, lo_ref, cols_ref, rows_ref, vec_ref, sem
):
    for b in range(NB):
        src = near_ref if b < NB // 2 else far_ref
        at = b % (NB // 2)
        lanes = pl.ds(b * BLK, BLK)
        cols_ref[:, lanes] = features(src[at, :FEAT, :], False).astype(BF16)
        pieces = [*split3(src[at, FEAT:, :]), jnp.zeros((2 * BLK - 3 * VEC, BLK), F32)]
        vec_ref[lanes, :] = jnp.concatenate(pieces, axis=0).T.astype(BF16)
        rows_ref[lanes, :] = features(out_ref[b, :FEAT, :], True).T.astype(BF16)

    def copies(step):
        rows = pl.ds(step * STEP, STEP)
        return (
            pltpu.make_async_copy(hi_ref.at[rows], hi_hbm.at[rows], sem.at[0, step]),
            pltpu.make_async_copy(lo_ref.at[rows], lo_hbm.at[rows], sem.at[1, step]),
        )

    steps = PTS // STEP
    for step in range(steps + 1):
        rows, before = pl.ds(step * STEP, STEP), pl.ds((step - 1) * STEP, STEP)
        if step > 0:
            for copy in copies(step - 1):
                copy.start()
        total = jnp.zeros((STEP, 2 * BLK), F32)
        for c in range(PTS // CHUNK):
            lanes = pl.ds(c * CHUNK, CHUNK)
            if step > 0:
                vec = vec_ref[lanes, :]
                total += jnp.dot(hi_ref[before, lanes], vec, preferred_element_type=F32)
                total += jnp.dot(lo_ref[before, lanes], vec, preferred_element_type=F32)
            if step < steps:
                power = jnp.dot(rows_ref[rows, :], cols_ref[:, lanes], preferred_element_type=F32)
                hi, lo = split2(jnp.exp2(jnp.minimum(power, 0.0)))
                hi_ref[rows, lanes] = hi
                lo_ref[rows, lanes] = lo
        if step > 0:
            for h in range(STEP // BLK):
                tall = total[h * BLK : (h + 1) * BLK].T
                part_ref[(step - 1) * (STEP // BLK) + h] = (
                    tall[:VEC] + tall[VEC : 2 * VEC] + tall[2 * VEC : 3 * VEC]
                )
    for step in range(steps):
        for copy in copies(step):
            copy.wait()


def make_tile(near, far, out, mark):
    return pl.pallas_call(
        tile_kernel,
        in_specs=[vmem(), vmem(), vmem(), vmem()],
        out_specs=[hbm(), hbm(), vmem()],
        out_shape=[
            pltpu.HBM((PTS, PTS), BF16),
            pltpu.HBM((PTS, PTS), BF16),
            shape(NB, VEC, BLK),
        ],
        scratch_shapes=[
            pltpu.VMEM((PTS, PTS), BF16),
            pltpu.VMEM((PTS, PTS), BF16),
            pltpu.VMEM((BLK, PTS), BF16),
            pltpu.VMEM((PTS, BLK), BF16),
            pltpu.VMEM((PTS, 2 * BLK), BF16),
            pltpu.SemaphoreType.DMA((2, PTS // STEP)),
        ],
        compiler_params=limit(40),
        name="kernel_tile",
    )(near, far, out, mark)


def owner_kernel(got_ref, held_ref, scalars_ref, out_ref):
    total = got_ref[0]
    for b in range(1, NB):
        total += got_ref[b]
    gain, nugget = scalars_ref[pl.ds(0, 1), :], scalars_ref[pl.ds(1, 1), :]
    applied = gain * total + nugget * held_ref[pl.ds(RHS, VEC), :]
    first = held_ref[pl.ds(0, RHS), :] - applied[:RHS]
    image = applied[RHS:]
    for b in range(NB):
        out_ref[b, pl.ds(0, RHS), :] = first
        out_ref[b, pl.ds(RHS, RITZ), :] = image


def at_owner(got, held, scalars):
    return pl.pallas_call(
        owner_kernel,
        out_shape=shape(NB, VEC, BLK),
        compiler_params=limit(8),
        name="at_owner",
    )(got, held, scalars)


def square_iota():
    return lax.broadcasted_iota(jnp.int32, (RITZ, RITZ), 0), lax.broadcasted_iota(jnp.int32, (RITZ, RITZ), 1)


def gram_kernel(vec_ref, pts_ref, out_ref, left_ref, right_ref):
    for b in range(NB):
        lanes = pl.ds(b * BLK, BLK)
        pad = jnp.zeros((LEFT - VEC, BLK), F32)
        image = split3(vec_ref[b])
        basis = split3(pts_ref[b, FEAT:, :])
        for q in range(3):
            left_ref[pl.ds(q * LEFT, LEFT), lanes] = jnp.concatenate([image[q], pad], axis=0).astype(BF16)
            right_ref[pl.ds(q * 2 * RITZ, RITZ), lanes] = basis[q].astype(BF16)
            right_ref[pl.ds(q * 2 * RITZ + RITZ, RITZ), lanes] = image[q][RHS:].astype(BF16)
    gram = jnp.zeros((VEC, 2 * RITZ), F32)
    for q in (2, 1, 0):
        rows = 3 - q
        left = left_ref[pl.ds(0, rows * LEFT), :]
        right = right_ref[pl.ds(q * 2 * RITZ, 2 * RITZ), :]
        total = lax.dot_general(left, right, NT, preferred_element_type=F32)
        for r in range(rows - 1, -1, -1):
            gram += total[r * LEFT : r * LEFT + VEC]
    coarse = gram[RHS:, :RITZ]
    coarse = 0.5 * (coarse + coarse.T)
    image = gram[RHS:, RITZ:]
    i, j = square_iota()
    packed = jnp.where(j >= i, coarse, image)
    diagonal = jnp.sum(jnp.where(i == j, image, 0.0), axis=0, keepdims=True)
    for b in range(NB // 2):
        out_ref[b, pl.ds(0, RHS), :] = gram[:RHS]
        out_ref[b, pl.ds(RHS, RITZ // 2), :] = jnp.concatenate([packed[: RITZ // 2], packed[RITZ // 2 :]], axis=1)
        out_ref[b, pl.ds(RHS + RITZ // 2, 1), :] = jnp.concatenate([diagonal, diagonal], axis=1)


def make_gram(vec, pts):
    return pl.pallas_call(
        gram_kernel,
        out_shape=shape(NB // 2, PACKED, BLK),
        scratch_shapes=[pltpu.VMEM((3 * LEFT, PTS), BF16), pltpu.VMEM((6 * RITZ, PTS), BF16)],
        compiler_params=limit(12),
        name="gram",
    )(vec, pts)


def inverse(matrix):
    full = (8, 2 * RITZ)
    i, j = square_iota()
    work = jnp.concatenate([matrix, jnp.where(i == j, 1.0, 0.0)], axis=1)
    work = [work[b : b + 8] for b in range(0, RITZ, 8)]
    sub = lax.broadcasted_iota(jnp.int32, full, 0)

    def pair(a, b, c, d, top, low):
        scale = 1.0 / (a * d - b * c)
        return (d * top - b * low) * scale, (a * low - c * top) * scale

    for k in range(0, RITZ, 4):
        at, row = k // 8, k % 8
        cols = [[jnp.broadcast_to(w[:, k + q : k + q + 1], full) for w in work] for q in range(4)]
        rows = [jnp.broadcast_to(work[at][row + q : row + q + 1], full) for q in range(4)]
        e = [[jnp.broadcast_to(cols[r][at][row + q : row + q + 1], full) for r in range(4)] for q in range(4)]
        r0, r1 = pair(e[0][0], e[0][1], e[1][0], e[1][1], rows[0], rows[1])
        f = [pair(e[0][0], e[0][1], e[1][0], e[1][1], e[0][r], e[1][r]) for r in (2, 3)]
        rows[2] = rows[2] - e[2][0] * r0 - e[2][1] * r1
        rows[3] = rows[3] - e[3][0] * r0 - e[3][1] * r1
        g = [[e[q][r] - e[q][0] * f[r - 2][0] - e[q][1] * f[r - 2][1] for r in (2, 3)] for q in (2, 3)]
        r2, r3 = pair(g[0][0], g[0][1], g[1][0], g[1][1], rows[2], rows[3])
        r0 = r0 - f[0][0] * r2 - f[1][0] * r3
        r1 = r1 - f[0][1] * r2 - f[1][1] * r3
        final = (r0, r1, r2, r3)
        work = [
            w - ((cols[0][b] * r0 + cols[1][b] * r1) + (cols[2][b] * r2 + cols[3][b] * r3))
            for b, w in enumerate(work)
        ]
        for q in range(4):
            work[at] = jnp.where(sub == row + q, final[q], work[at])
    return jnp.concatenate(work, axis=0)[:, RITZ:]


def apply_kernel(hi_hbm, lo_hbm, vec_ref, pts_ref, out_ref, rows_ref, hi_ref, lo_ref, sem):
    copies = []
    for step in range(PTS // READ):
        lanes = pl.ds(step * READ, READ)
        copies.append(
            (
                pltpu.make_async_copy(hi_hbm.at[:, lanes], hi_ref.at[:, lanes], sem.at[0, step]),
                pltpu.make_async_copy(lo_hbm.at[:, lanes], lo_ref.at[:, lanes], sem.at[1, step]),
            )
        )
        for copy in copies[-1]:
            copy.start()
    for b in range(NB):
        lanes = pl.ds(b * BLK, BLK)
        first = vec_ref[b, :RHS, :]
        rows = jnp.concatenate([first, jnp.zeros_like(first), pts_ref[b, FEAT:, :], vec_ref[b, RHS:, :]], axis=0)
        for q, piece in enumerate(split3(rows)):
            rows_ref[pl.ds(q * HALF, HALF), lanes] = piece.astype(BF16)
    for step in range(PTS // READ):
        lanes = pl.ds(step * READ, READ)
        for copy in copies[step]:
            copy.wait()
        both = jnp.dot(rows_ref[...], hi_ref[:, lanes], preferred_element_type=F32)
        more = jnp.dot(rows_ref[pl.ds(0, 2 * HALF), :], lo_ref[:, lanes], preferred_element_type=F32)
        both = both[: 2 * HALF] + more + jnp.concatenate([jnp.zeros_like(both[:HALF]), both[2 * HALF :]], axis=0)
        out_ref[:, lanes] = both[:HALF] + both[HALF:]


def apply_tile(hi, lo, vec, pts):
    return pl.pallas_call(
        apply_kernel,
        in_specs=[hbm(), hbm(), vmem(), vmem()],
        out_shape=shape(HALF, PTS),
        scratch_shapes=[
            pltpu.VMEM((3 * HALF, PTS), BF16),
            pltpu.VMEM((PTS, PTS), BF16),
            pltpu.VMEM((PTS, PTS), BF16),
            pltpu.SemaphoreType.DMA((2, PTS // READ)),
        ],
        compiler_params=limit(32),
        cost_estimate=pl.CostEstimate(flops=8 * HALF * PTS * PTS, bytes_accessed=4 * PTS * PTS, transcendentals=0),
        name="apply_tile",
    )(in_hbm(hi), in_hbm(lo), vec, pts)


def exact(left, right):
    return jnp.dot(left, right, precision=HIGH, preferred_element_type=F32)


def solve_kernel(gram_ref, more_ref, image_ref, vec_ref, held_ref, part_ref, own_ref):
    gram = gram_ref[...] + more_ref[...]
    projected = gram[:RHS, :RITZ]
    first = gram[:RHS, RITZ:]
    square = jnp.concatenate([gram[RHS : RHS + RITZ // 2, :RITZ], gram[RHS : RHS + RITZ // 2, RITZ:]], axis=0)
    turned = square.T
    i, j = square_iota()
    coarse = jnp.where(j >= i, square, turned)
    image = jnp.where(j < i, square, jnp.where(j > i, turned, gram[RHS + RITZ // 2 :, :RITZ]))
    solve = inverse(coarse)
    amounts = lax.dot_general(projected, solve, NT, precision=HIGH, preferred_element_type=F32)
    against = first - exact(amounts, image)
    turns = lax.dot_general(against, solve, NT, precision=HIGH, preferred_element_type=F32)
    value = image_ref[pl.ds(0, RHS), :] - exact(amounts, image_ref[pl.ds(2 * RHS + RITZ, RITZ), :])
    value = value - exact(turns, image_ref[pl.ds(2 * RHS, RITZ), :])
    core = lax.axis_index(CORE)
    for at in range(NB):
        half = (at // (NB // 2) + core) % 2
        part_ref[half * (NB // 2) + at % (NB // 2)] = value[:, at * BLK : (at + 1) * BLK]
    mine = lax.axis_index("row_0") * 4 + lax.axis_index("col_0")
    ritz = held_ref[pl.ds(2 * RHS, RITZ), :]
    residual = vec_ref[mine, :RHS, :] - exact(amounts, vec_ref[mine, RHS:, :])
    own_ref[pl.ds(0, RHS), :] = residual - exact(turns, ritz)
    own_ref[pl.ds(RHS, RHS), :] = residual
    own_ref[pl.ds(2 * RHS, RHS), :] = held_ref[pl.ds(RHS, RHS), :] + exact(amounts, ritz)


def solve(gram, more, image, vec, held):
    return pl.pallas_call(
        solve_kernel,
        out_shape=[shape(NB, RHS, BLK), shape(3 * RHS, BLK)],
        compiler_params=limit(12),
        name="solve",
    )(gram, more, image, vec, held)


def stats_kernel(got_ref, own_ref, scalars_ref, applied_ref, out_ref):
    total = got_ref[0]
    for b in range(1, NB):
        total += got_ref[b]
    direction = own_ref[pl.ds(0, RHS), :]
    residual = own_ref[pl.ds(RHS, RHS), :]
    applied = scalars_ref[pl.ds(0, 1), :] * total + scalars_ref[pl.ds(1, 1), :] * direction
    applied_ref[...] = applied
    sums = jnp.concatenate(
        [
            jnp.sum(direction * applied, axis=1, keepdims=True),
            jnp.sum(residual * residual, axis=1, keepdims=True),
        ],
        axis=0,
    )
    sums = jnp.broadcast_to(sums, (2 * RHS, BLK)).T[:RHS]
    for b in range(WORLD // RHS):
        out_ref[pl.ds(b * RHS, RHS), :] = sums


def make_stats(got, own, scalars):
    return pl.pallas_call(
        stats_kernel,
        out_shape=[shape(RHS, BLK), shape(WORLD, 2 * RHS)],
        compiler_params=limit(8),
        name="stats",
    )(got, own, scalars)


def finish_kernel(got_ref, own_ref, applied_ref, solution_ref, residual_ref):
    sums = jnp.sum(got_ref[...], axis=0, keepdims=True)
    i = lax.broadcasted_iota(jnp.int32, (2 * RHS, 2 * RHS), 0)
    j = lax.broadcasted_iota(jnp.int32, (2 * RHS, 2 * RHS), 1)
    sums = jnp.sum(jnp.where(i == j, sums, 0.0), axis=1, keepdims=True)
    size = sums[RHS:] / sums[:RHS]
    solution_ref[...] = own_ref[pl.ds(2 * RHS, RHS), :] + size * own_ref[pl.ds(0, RHS), :]
    residual_ref[...] = own_ref[pl.ds(RHS, RHS), :] - size * applied_ref[...]


def finish(got, own, applied):
    return pl.pallas_call(
        finish_kernel,
        out_shape=[shape(RHS, BLK), shape(RHS, BLK)],
        compiler_params=limit(8),
        name="finish",
    )(got, own, applied)


def exchange(pieces, axis):
    return lax.all_to_all(pieces, axis, split_axis=0, concat_axis=0, tiled=True)


def all_around(array, axis):
    size, here = lax.axis_size(axis), lax.axis_index(axis)
    whole = jnp.zeros((size, *array.shape), array.dtype)
    for k in range(size):
        block = array if k == 0 else lax.ppermute(array, axis, [(i, (i + k) % size) for i in range(size)])
        whole = lax.dynamic_update_index_in_dim(whole, block, (here - k + size) % size, 0)
    return whole


def other_core(array):
    return lax.ppermute(array, CORE, [(0, 1), (1, 0)])


def local(points, inv_scales, amplitude, noise_var, targets, initial, ritz_basis):
    near, pts, held = spread(points, inv_scales[None, :], initial, ritz_basis, targets)
    scalars = jnp.concatenate([amplitude, noise_var])
    scalars = jnp.broadcast_to(scalars[:, None], (2, BLK))
    pts = all_around(pts, "col_0")
    near = exchange(near, Z)
    pts = all_around(pts, "row_0").reshape(NB, FEAT + RITZ, BLK)
    near, scalars = lax.optimization_barrier((near, scalars))
    far = other_core(near)
    mark = near[0, :8] * 0.5
    hi, lo, part = make_tile(near, far, pts, mark)

    vec = exchange(at_owner(exchange(part, XY), held, scalars), XY)
    gram = make_gram(vec, pts)
    vec, gram = lax.optimization_barrier((vec, gram))
    image = apply_tile(hi, lo, vec, pts)
    image, gram = lax.optimization_barrier((image, exchange(gram, Z)))
    gram = jnp.sum(gram, axis=0)
    part, own = solve(gram, other_core(gram), image, vec, held)
    applied, stats = make_stats(exchange(part, CZ), own, scalars)
    return tuple(finish(exchange(stats, EVERY), own, applied))


def solution(mesh):
    torus = Mesh(mesh.devices.reshape(4, 8, 4, 2), ("row_0", "row_1", "col_0", "col_1"))
    in_specs = (
        P(None, COL_ROW),
        P(),
        P(),
        P(),
        P(None, COL_ROW),
        P(None, COL_ROW),
        P(None, COL_ROW),
    )
    out_specs = (P(None, COL_ROW), P(None, COL_ROW))
    return jax.shard_map(local, mesh=torus, in_specs=in_specs, out_specs=out_specs, check_vma=False)
```
